32 devices in a mesh: dp: 2 (over y), ctx: 4 (over z), tp: 4 (over x, core).
Axes of the slice: x: 2, y: 2, z: 4, core: 2. Of those that a mesh axis runs over, the one named last changes fastest.
Arguments:
- hidden_in: bfloat16 [8192, 2048], P(('dp', 'ctx')), may hold values from -6 to 6
- seq_lengths: int32 [2, 3], P('dp'), may hold values from 1024 to 2048, as said below
- pack_order: int32 [2, 3], P('dp'), may hold values from 0 to 2, each once within a row
- norm_gain: bfloat16 [2048], P('dp'), may hold values from 0.5 to 1.5
- in_x_weight: bfloat16 [2048, 4096], P('dp', 'tp'), may hold values from -0.125 to 0.125
- in_z_weight: bfloat16 [2048, 4096], P('dp', 'tp'), may hold values from -0.125 to 0.125
- conv_weight: bfloat16 [4, 4096], P(None, ('tp', 'dp')), may hold values from -3 to 3
- conv_bias: bfloat16 [4096], P(('tp', 'dp')), may hold values from -0.5 to 0.5
- x_weight: bfloat16 [4096, 160], P(('tp', 'dp')), may hold values from -0.09375 to 0.09375
- dt_weight: bfloat16 [128, 4096], P('dp', 'tp'), may hold values from -0.5 to 0.5
- dt_bias: bfloat16 [4096], P(('tp', 'dp')), may hold values from -9 to -2.296875
- a_log: bfloat16 [4096, 16], P(('tp', 'dp')), may hold values from 0 to 2.765625
- skip_weight: bfloat16 [4096], P(('tp', 'dp')), may hold values from 0.5 to 1.5
- out_weight: bfloat16 [4096, 2048], P('tp', 'dp'), may hold values from -0.09375 to 0.09375
- out_grad: bfloat16 [8192, 2048], P(('dp', 'ctx')), may hold values from -6 to 6
Outputs:
- out: bfloat16 [8192, 2048], P(('dp', 'ctx'))
- grad_input: bfloat16 [8192, 2048], P(('dp', 'ctx'))
- grad_norm_gain: float32 [2048], P('dp')
- grad_in_x: float32 [2048, 4096], P('dp', 'tp')
- grad_in_z: float32 [2048, 4096], P('dp', 'tp')
- grad_conv_weight: float32 [4, 4096], P(None, ('tp', 'dp'))
- grad_conv_bias: float32 [4096], P(('tp', 'dp'))
- grad_x_weight: float32 [4096, 160], P(('tp', 'dp'))
- grad_dt_weight: float32 [128, 4096], P('dp', 'tp')
- grad_dt_bias: float32 [4096], P(('tp', 'dp'))
- grad_a_log: float32 [4096, 16], P(('tp', 'dp'))
- grad_skip: float32 [4096], P(('tp', 'dp'))
- grad_out_weight: float32 [4096, 2048], P('tp', 'dp')
The draws below stay inside these ranges and needn't reach their ends.
Inputs may be any that keep to these rules, and one draw needn't show every extreme that they name: `seq_lengths`: in each group the 3 lengths sum to 4096; each is 1024 or more, and one is exactly 1024; some group has a sequence of the largest length. `pack_order`: each row is a permutation of 0 to 2.
All inputs are finite; a program needn't handle non-finite values.
Results may differ from the reference program's by a relative error of at most 0.012.
The reference program's roundings to bfloat16 on the way count: a program that leaves them out, or rounds other values in their place, can miss the bound.
Values may be sent and summed in bfloat16 or wider, within the bound.
A program may use at most 896 MiB of HBM per device.

```python
import math
import jax
import jax.numpy as jnp
from jax import lax

D = 2048
E = 4096
N = 16
R = 128
K = 4
ROW = 2048
LEN_MIN = 1024
MICRO = 2
SEQS = 3
GROUPS = 2
TOKENS = 8192


def draw_seq_lengths(key, part):
    surplus = MICRO * ROW - SEQS * LEN_MIN
    headroom = ROW - LEN_MIN
    low_end = max(0, surplus - headroom)
    high_end = min(surplus, headroom)
    first_key, second_key = jax.random.split(jax.random.fold_in(key, 11))
    middle = jax.random.randint(first_key, (GROUPS, 1), low_end, high_end + 1).astype(jnp.int32)
    middle = jnp.where(jnp.arange(GROUPS, dtype=jnp.int32)[:, None] == 0, high_end, middle).astype(jnp.int32)
    pieces = jnp.concatenate([jnp.zeros((GROUPS, 1), jnp.int32), middle, surplus - middle], axis=1)
    scores = jax.random.randint(second_key, (GROUPS, SEQS), 0, 1 << 20).astype(jnp.int32) * SEQS + jnp.arange(SEQS, dtype=jnp.int32)[None, :]
    arrangement = jnp.argsort(scores, axis=1).astype(jnp.int32)
    return (LEN_MIN + jnp.take_along_axis(pieces, arrangement, axis=1)).astype(jnp.int32)


def steps_of(key, shape, cuts, low, top_value):
    factor_of = 1.0
    for position, parts in cuts:
        draws = jax.random.uniform(jax.random.fold_in(jax.random.fold_in(key, 6), position), (parts,), jnp.float32, low / len(cuts), top_value / len(cuts))
        factor_of = factor_of * jnp.repeat(jnp.exp(draws), shape[position] // parts).reshape((-1,) + (1,) * (len(shape) - 1 - position))
    return factor_of


def noise(key, extent, width, most, cuts=(), held_as=jnp.bfloat16):
    loudness = steps_of(key, extent, cuts, -0.22, 0.18) if cuts else 1.0
    values = jax.random.normal(key, extent, jnp.float32) * width * loudness
    return jnp.minimum(jnp.maximum(values, -most), most).astype(held_as)


def setup_inputs(seed: int = 0) -> dict:
    key_list = jax.random.split(jax.random.key(seed), 16)
    hidden_in = noise(key_list[0], (TOKENS, D), 1.0, 6.0, ((0, 8),))
    seq_lengths = draw_seq_lengths(jax.random.fold_in(key_list[15], 71), 0)
    pack_order = jax.vmap(lambda own: jax.random.permutation(own, SEQS))(jax.random.split(key_list[2], GROUPS)).reshape((GROUPS, SEQS)).astype(jnp.int32)
    norm_gain = jnp.clip(1.0 + 0.1 * jax.random.normal(key_list[3], (D,), jnp.float32), 0.5, 1.5).astype(jnp.bfloat16)
    in_x_weight = noise(key_list[4], (D, E), D ** -0.5, 0.125, ((0, 2), (1, 4)))
    in_z_weight = noise(key_list[5], (D, E), D ** -0.5, 0.125, ((0, 2), (1, 4)))
    conv_weight = noise(key_list[6], (K, E), K ** -0.5, 3.0, ((1, 8),))
    conv_bias = jnp.clip(jax.random.uniform(key_list[7], (E,), jnp.float32, -0.5, 0.5) * steps_of(key_list[7], (E,), ((0, 8),), -0.4, 0.0), -0.5, 0.5).astype(jnp.bfloat16)
    x_weight = noise(key_list[8], (E, R + 2 * N), E ** -0.5, 0.09375, ((0, 8),))
    dt_weight = noise(key_list[9], (R, E), R ** -0.5, 0.5, ((0, 2), (1, 4)))
    dt_bias = jnp.clip(-9.0 + 6.703125 * jax.random.uniform(key_list[10], (E,), jnp.float32) ** steps_of(key_list[10], (E,), ((0, 8),), -0.2, 0.2), -9.0, -2.296875).astype(jnp.bfloat16)
    a_log = jnp.clip(2.765625 * jax.random.uniform(key_list[11], (E, N), jnp.float32) ** steps_of(key_list[11], (E, N), ((0, 8),), -0.2, 0.2), 0.0, 2.765625).astype(jnp.bfloat16)
    skip_weight = jnp.clip(0.5 + 1.0 * jax.random.uniform(key_list[12], (E,), jnp.float32) ** steps_of(key_list[12], (E,), ((0, 8),), -0.2, 0.2), 0.5, 1.5).astype(jnp.bfloat16)
    out_weight = noise(key_list[13], (E, D), E ** -0.5, 0.09375, ((0, 4), (1, 2)))
    out_grad = noise(key_list[14], (TOKENS, D), 1.0, 6.0, ((0, 8),))
    return dict(hidden_in=hidden_in, seq_lengths=seq_lengths, pack_order=pack_order, norm_gain=norm_gain, in_x_weight=in_x_weight, in_z_weight=in_z_weight, conv_weight=conv_weight, conv_bias=conv_bias, x_weight=x_weight, dt_weight=dt_weight, dt_bias=dt_bias, a_log=a_log, skip_weight=skip_weight, out_weight=out_weight, out_grad=out_grad)


@jax.custom_vjp
def low(v):
    return lax.optimization_barrier(v.astype(jnp.bfloat16)).astype(jnp.float32)

@jax.custom_vjp
def low_back(v):
    return v

def low_keep(v):
    return (low(v), None)

def low_pass(kept, grad):
    return (grad,)

def back_keep(v):
    return (v, None)

def back_low(kept, grad):
    return (low(grad),)
low.defvjp(low_keep, low_pass)
low_back.defvjp(back_keep, back_low)
EPSILON = 1e-05
PRECISE = lax.Precision.HIGHEST

def matmul_high(left, right):
    return jnp.dot(left, right, precision=PRECISE, preferred_element_type=jnp.float32)

def selective_scan(step_size, decay_rate, b_in, c_out, drive_in, keep_mask):
    length, channels = step_size.shape
    block_len = math.gcd(length, 64)
    block_count = length // block_len

    def run_block(carried, pieces):

        def token_step(inner_carry, token_row):
            state_now, rate_now = inner_carry
            step_t, b_t, c_t, drive_t, keep_t = token_row
            state_now = jnp.exp(step_t[:, None] * rate_now) * keep_t * state_now + (step_t * drive_t)[:, None] * b_t[None, :]
            return ((state_now, rate_now), lax.optimization_barrier(jnp.sum(state_now * c_t[None, :], axis=1)))
        return lax.scan(token_step, carried, pieces)
    shaped = tuple((one_array.reshape((block_count, block_len) + one_array.shape[1:]) for one_array in (step_size, b_in, c_out, drive_in, keep_mask)))
    initial = (jnp.zeros((channels, decay_rate.shape[1]), jnp.float32), decay_rate)
    final_carry, outputs = lax.scan(jax.checkpoint(run_block), initial, shaped)
    return outputs.reshape(length, channels)

def row_forward(rows_in, slot_row, weights):
    gain_vec, w_inx, w_inz, conv_taps, conv_shift, w_proj, w_step, step_bias, rate_log, skip_vec, w_out = weights
    length = rows_in.shape[0]
    inv_rms = lax.rsqrt(lax.optimization_barrier(jnp.mean(rows_in * rows_in, axis=1, keepdims=True)) + EPSILON)
    normed = low(rows_in * inv_rms * gain_vec)
    inner_x = low_back(low(matmul_high(normed, w_inx)))
    gate_z = low_back(matmul_high(normed, w_inz))
    padded = jnp.concatenate([jnp.zeros((K - 1, inner_x.shape[1]), jnp.float32), inner_x], axis=0)
    slot_pad = jnp.concatenate([jnp.full((K - 1,), -1, dtype=jnp.int32), slot_row.astype(jnp.int32)], axis=0)
    conv_pre = conv_shift[None, :]
    for tap_index in range(K):
        tap_valid = (slot_pad[tap_index:tap_index + length] == slot_row).astype(jnp.float32)
        conv_pre = conv_pre + conv_taps[tap_index] * padded[tap_index:tap_index + length] * tap_valid[:, None]
    activated = low(jax.nn.silu(conv_pre))
    projected = low_back(matmul_high(activated, w_proj))
    step_low = low(projected[:, :R])
    b_in = projected[:, R:R + N]
    c_out = projected[:, R + N:]
    step_pre = low_back(matmul_high(step_low, w_step) + step_bias)
    step_size = jax.nn.softplus(step_pre)
    decay_rate = -jnp.exp(rate_log)
    keep_mask = jnp.concatenate([jnp.zeros((1,), jnp.float32), (slot_row[1:] == slot_row[:-1]).astype(jnp.float32)])
    scan_out = selective_scan(step_size, decay_rate, b_in, c_out, activated, keep_mask) + skip_vec * activated
    gated_out = low(scan_out * jax.nn.silu(gate_z))
    return rows_in + matmul_high(gated_out, w_out)

def reference(hidden_in, seq_lengths, pack_order, norm_gain, in_x_weight, in_z_weight, conv_weight, conv_bias, x_weight, dt_weight, dt_bias, a_log, skip_weight, out_weight, out_grad):
    weights = tuple((one_array.astype(jnp.float32) for one_array in (norm_gain, in_x_weight, in_z_weight, conv_weight, conv_bias, x_weight, dt_weight, dt_bias, a_log, skip_weight, out_weight)))
    stream = MICRO * ROW
    ordered = jnp.take_along_axis(seq_lengths, pack_order, axis=1).astype(jnp.int32)
    nat_start = (jnp.cumsum(seq_lengths, axis=1) - seq_lengths).astype(jnp.int32)
    pack_start = (jnp.cumsum(ordered, axis=1) - ordered).astype(jnp.int32)
    positions = jnp.arange(stream, dtype=jnp.int32)
    slots_all = lax.optimization_barrier(jnp.sum((positions[None, :, None] >= pack_start[:, None, 1:]).astype(jnp.int32), axis=2)).astype(jnp.int32)
    sequence = jnp.take_along_axis(pack_order, slots_all, axis=1).astype(jnp.int32)
    groups_base = (jnp.arange(GROUPS, dtype=jnp.int32) * stream)[:, None]
    source = (jnp.take_along_axis(nat_start, sequence, axis=1) + positions[None, :] - jnp.take_along_axis(pack_start, slots_all, axis=1) + groups_base).reshape(-1).astype(jnp.int32)
    rows_in = hidden_in.astype(jnp.float32)[source].reshape(GROUPS * MICRO, ROW, D)
    rows_grad = out_grad.astype(jnp.float32)[source].reshape(GROUPS * MICRO, ROW, D)
    slot_rows = slots_all.reshape(GROUPS * MICRO, ROW)

    def one_row(running, pieces):
        row_in, row_grad, row_slots = pieces
        result, pull_back = jax.vjp(lambda rows_now, *params: row_forward(rows_now, row_slots, params), row_in, *weights)
        cotangents = pull_back(row_grad)
        running = tuple((summed + addition for summed, addition in zip(running, cotangents[1:])))
        return (running, (result.astype(jnp.bfloat16), cotangents[0].astype(jnp.bfloat16)))
    running_init = tuple((jnp.zeros_like(one_array) for one_array in weights))
    gradients, (out_rows, dx_rows) = lax.scan(one_row, running_init, (rows_in, rows_grad, slot_rows))
    out_full = jnp.zeros((TOKENS, D), jnp.bfloat16).at[source].set(out_rows.reshape(-1, D))
    dx_full = jnp.zeros((TOKENS, D), jnp.bfloat16).at[source].set(dx_rows.reshape(-1, D))
    return (out_full, dx_full, gradients[0], gradients[1], gradients[2], gradients[3], gradients[4], gradients[5], gradients[6], gradients[7], gradients[8], gradients[9], gradients[10])
```

```python
import jax
import jax.numpy as jnp
from jax import lax
from jax.experimental import pallas as pl
from jax.experimental.pallas import tpu as pltpu
from jax.sharding import PartitionSpec as P

N = 16
R = 128
K = 4
ROW = 2048
MICRO = 2
EPSILON = 1e-05

LANES = 128
SEGS = 8
FAR = 1e30
LOG2E = 1.4426950408889634
LN2 = 0.6931471805599453
F32 = jnp.float32
BF16 = jnp.bfloat16


def contract_last(left, right):
    return lax.dot_general(left, right, (((1,), (1,)), ((), ())), preferred_element_type=F32)


def contract_first(left, right):
    return lax.dot_general(left, right, (((0,), (0,)), ((), ())), preferred_element_type=F32)


def shifted(value, axis, steps):
    count = lax.axis_size(axis)
    leading, last = (max(0, -steps), min(count, count - steps))
    return lax.ppermute(value, axis, [(source, source + steps) for source in range(leading, last)])


def piece_starts(lengths, arrangement):
    count = lengths.shape[0]
    ids = jnp.arange(count, dtype=jnp.int32)
    ordered = jnp.sum(jnp.where(arrangement[:, None] == ids[None, :], lengths[None, :], 0), axis=1)
    nat_start = jnp.cumsum(lengths) - lengths
    pack_start = jnp.cumsum(ordered) - ordered
    rows = jnp.arange(1, MICRO, dtype=jnp.int32) * ROW
    slot = jnp.sum((rows[:, None] >= pack_start[None, 1:]).astype(jnp.int32), axis=1)
    in_slot = slot[:, None] == ids[None, :]
    sequence = jnp.sum(jnp.where(in_slot, arrangement[None, :], 0), axis=1)
    begun = jnp.sum(jnp.where(in_slot, pack_start[None, :], 0), axis=1)
    source = (
        jnp.sum(jnp.where(sequence[:, None] == ids[None, :], nat_start[None, :], 0), axis=1)
        + rows
        - begun
    )
    return jnp.concatenate([nat_start, source])


def exact_parts(value):
    high = value.astype(BF16)
    rest = value - high.astype(F32)
    mid = rest.astype(BF16)
    return high, mid, (rest - mid.astype(F32)).astype(BF16)


def spread_columns(table_ref, out_ref, extra_ref, turned_ref, groups, steps):
    rows_of = SEGS * steps
    row = lax.broadcasted_iota(jnp.int32, (2 * LANES, 2 * LANES), 0) % LANES
    side = lax.broadcasted_iota(jnp.int32, (2 * LANES, 2 * LANES), 1) // LANES
    for g in range(groups):

        def one(i, _):
            turned_ref[pl.ds(pl.multiple_of(i * SEGS, SEGS), SEGS), :] = table_ref[
                pl.ds(g * rows_of + i, SEGS, stride=steps), :
            ]
            return 0

        lax.fori_loop(0, steps, one, 0, unroll=8)
        high, mid, low = exact_parts(turned_ref[0:rows_of, :])
        most = jnp.concatenate([high, mid], axis=1)
        for n in range(0, 2 * N + 1, 2):
            pick = (row == n + side).astype(F32).astype(BF16)
            value = jnp.dot(most, pick, preferred_element_type=F32)
            value = value + jnp.dot(low, pick[:LANES], preferred_element_type=F32)
            first = value[:, :LANES].reshape(steps, SEGS, LANES)
            if n < 2 * N:
                out_ref[g * steps : (g + 1) * steps, n] = first
                out_ref[g * steps : (g + 1) * steps, n + 1] = value[:, LANES:].reshape(
                    steps, SEGS, LANES
                )
            else:
                extra_ref[g * steps : (g + 1) * steps] = first


def totals_kernel(
    groups,
    steps,
    step_ref,
    act_ref,
    dy_ref,
    rate_ref,
    table_ref,
    seg_s_ref,
    seg_h_ref,
    seg_c_ref,
    whole_ref,
    bc_s,
    keep_s,
    act_s,
):
    rows_of = SEGS * steps

    @pl.when(pl.program_id(0) == 0)
    def _():
        spread_columns(table_ref, bc_s, keep_s, act_s, groups, steps)

    act_s[...] = act_ref[...].astype(F32)
    half = N
    zero = jnp.zeros((SEGS, LANES), F32)
    for g in range(groups):
        for lo in range(0, N, half):
            rates = [
                jnp.broadcast_to(rate_ref[lo + n : lo + n + 1, :], (SEGS, LANES))
                for n in range(half)
            ]

            def one(i, carry):
                total, state, reach, back = carry
                state, reach, back = list(state), list(reach), list(back)
                at = pl.ds(g * rows_of + i, SEGS, stride=steps)
                step, act, dy = step_ref[at, :], act_s[at, :], dy_ref[at, :]
                gone = step + keep_s[g * steps + i]
                push = step * act
                for n in range(half):
                    decay = jnp.exp2(gone * rates[n])
                    state[n] = decay * state[n] + push * bc_s[g * steps + i, lo + n]
                    reach[n] = reach[n] * decay
                    back[n] = back[n] + reach[n] * (dy * bc_s[g * steps + i, N + lo + n])
                return (total + gone, tuple(state), tuple(reach), tuple(back))

            total, state, _, back = lax.fori_loop(
                0,
                steps,
                one,
                (zero, (zero,) * half, (jnp.ones((SEGS, LANES), F32),) * half, (zero,) * half),
                unroll=8,
            )
            if lo == 0:
                seg_s_ref[g * SEGS : (g + 1) * SEGS, :] = total
            for n in range(half):
                first = (g * N + lo + n) * SEGS
                seg_h_ref[first : first + SEGS, :] = state[n]
                seg_c_ref[first : first + SEGS, :] = back[n]
    rate = rate_ref[...]
    h = jnp.zeros((N, LANES), F32)
    c = jnp.zeros((N, LANES), F32)
    order = [(g, s) for g in range(groups) for s in range(SEGS)]
    gone = jnp.zeros((1, LANES), F32)
    for g, s in order:
        at = pl.ds(g * N * SEGS + s, N, stride=SEGS)
        spent = seg_s_ref[g * SEGS + s : g * SEGS + s + 1, :]
        h = jnp.exp2(rate * spent) * h + seg_h_ref[at, :]
        gone = gone + spent
    for g, s in order[::-1]:
        at = pl.ds(g * N * SEGS + s, N, stride=SEGS)
        spent = seg_s_ref[g * SEGS + s : g * SEGS + s + 1, :]
        c = jnp.exp2(rate * spent) * c + seg_c_ref[at, :]
    whole_ref[0:N, :] = h
    whole_ref[N : 2 * N, :] = c
    whole_ref[2 * N : 2 * N + SEGS, :] = jnp.broadcast_to(gone, (SEGS, LANES))


def grads_kernel(
    groups,
    steps,
    blocks,
    step_ref,
    act_ref,
    dy_ref,
    rate_ref,
    table_ref,
    seg_s_ref,
    seg_h_ref,
    seg_c_ref,
    h_in_ref,
    c_in_ref,
    y_ref,
    d_step_ref,
    d_act_ref,
    d_rate_ref,
    d_bc_ref,
    bc_s,
    keep_s,
    act_s,
    enter_h,
    enter_c,
    decay_s,
    prior_s,
    sum_b,
    sum_c,
):
    g, j = pl.program_id(0), pl.program_id(1)

    @pl.when(j == 0)
    def _():
        spread_columns(table_ref, bc_s, keep_s, act_s, 1, steps)
        sum_b[...] = jnp.zeros_like(sum_b)
        sum_c[...] = jnp.zeros_like(sum_c)

    rate = rate_ref[...]

    @pl.when(g == 0)
    def _():
        h = h_in_ref[...]
        c = c_in_ref[...]
        order = [(a, s) for a in range(groups) for s in range(SEGS)]
        for a, s in order:
            at = pl.ds(a * N * SEGS + s, N, stride=SEGS)
            spent = seg_s_ref[a * SEGS + s : a * SEGS + s + 1, :]
            enter_h.at[j][at, :] = h
            h = jnp.exp2(rate * spent) * h + seg_h_ref[at, :]
        for a, s in order[::-1]:
            at = pl.ds(a * N * SEGS + s, N, stride=SEGS)
            spent = seg_s_ref[a * SEGS + s : a * SEGS + s + 1, :]
            enter_c.at[j][at, :] = c
            c = jnp.exp2(rate * spent) * c + seg_c_ref[at, :]

    act_s[...] = act_ref[...].astype(F32)
    first = g * N * SEGS

    def rate_row(n):
        return jnp.broadcast_to(rate_ref[n : n + 1, :], (SEGS, LANES))

    def ahead(i, state):
        state = list(state)
        at = pl.ds(i, SEGS, stride=steps)
        step, act, dy = step_ref[at, :], act_s[at, :], dy_ref[at, :]
        gone = step + keep_s[i]
        push = step * act
        y = jnp.zeros((SEGS, LANES), F32)
        for n in range(N):
            decay = jnp.exp2(gone * rate_row(n))
            prior = decay * state[n]
            state[n] = prior + push * bc_s[i, n]
            decay_s[i, n] = decay
            prior_s[i, n] = prior
            y = y + state[n] * bc_s[i, N + n]
            sum_c[i, n] += state[n] * dy
        y_ref[at, :] = y
        return tuple(state)

    def enter(ref, n):
        return ref[j, pl.ds(pl.multiple_of(first + n * SEGS, SEGS), SEGS), :]

    lax.fori_loop(0, steps, ahead, tuple(enter(enter_h, n) for n in range(N)), unroll=8)

    def back(k, carry):
        i = steps - 1 - k
        carried, d_rate = list(carry[0]), list(carry[1])
        at = pl.ds(i, SEGS, stride=steps)
        step, act, dy = step_ref[at, :], act_s[at, :], dy_ref[at, :]
        push = step * act
        along = jnp.zeros((SEGS, LANES), F32)
        d_step = jnp.zeros((SEGS, LANES), F32)
        for n in range(N):
            grad = dy * bc_s[i, N + n] + carried[n]
            along = along + grad * bc_s[i, n]
            log_grad = grad * prior_s[i, n]
            d_step = d_step + log_grad * rate_row(n)
            d_rate[n] = d_rate[n] + log_grad * step
            carried[n] = grad * decay_s[i, n]
            sum_b[i, n] += grad * push
        d_step_ref[at, :] = d_step * LN2 + along * act
        d_act_ref[at, :] = along * step
        return (tuple(carried), tuple(d_rate))

    zero = jnp.zeros((SEGS, LANES), F32)
    _, d_rate = lax.fori_loop(
        0, steps, back, (tuple(enter(enter_c, n) for n in range(N)), (zero,) * N), unroll=8
    )
    for n in range(N):
        d_rate_ref[0, n : n + 1, :] = jnp.sum(d_rate[n], axis=0, keepdims=True)

    @pl.when(j == blocks - 1)
    def _():
        column = lax.broadcasted_iota(jnp.int32, (2 * LANES, LANES), 1)
        total = jnp.zeros((steps * SEGS, LANES), F32)
        for n in range(N):
            for ref, at in ((sum_b, n), (sum_c, N + n)):
                pick = (column == at).astype(F32).astype(BF16)
                value = exact_parts(ref[:, n].reshape(steps * SEGS, LANES))
                total = total + jnp.dot(
                    jnp.concatenate(value[:2], axis=1), pick, preferred_element_type=F32
                )
        act_s[...] = total

        def put(i, _):
            d_bc_ref[pl.ds(i, SEGS, stride=steps), :] = act_s[
                pl.ds(pl.multiple_of(i * SEGS, SEGS), SEGS), :
            ]
            return 0

        lax.fori_loop(0, steps, put, 0, unroll=8)


def scan_totals(step_size, activated, dy_scan, rate2, table, groups, begin, channels):
    length = step_size.shape[0]
    steps = length // (groups * SEGS)
    blocks = channels // LANES
    skip = begin // LANES
    body = lambda *refs: totals_kernel(groups, steps, *refs)
    tall = pl.BlockSpec((length, LANES), lambda j: (0, j + skip))
    rows = groups * N * SEGS
    return pl.pallas_call(
        body,
        grid=(blocks,),
        in_specs=[
            tall,
            tall,
            tall,
            pl.BlockSpec((N, LANES), lambda j: (0, j + skip)),
            pl.BlockSpec((length, LANES), lambda j: (0, 0)),
        ],
        out_specs=[
            pl.BlockSpec((groups * SEGS, LANES), lambda j: (0, j)),
            pl.BlockSpec((rows, LANES), lambda j: (0, j)),
            pl.BlockSpec((rows, LANES), lambda j: (0, j)),
            pl.BlockSpec((2 * N + SEGS, LANES), lambda j: (0, j)),
        ],
        out_shape=[
            jax.ShapeDtypeStruct((groups * SEGS, channels), F32),
            jax.ShapeDtypeStruct((rows, channels), F32),
            jax.ShapeDtypeStruct((rows, channels), F32),
            jax.ShapeDtypeStruct((2 * N + SEGS, channels), F32),
        ],
        scratch_shapes=[
            pltpu.VMEM((groups * steps, 2 * N, SEGS, LANES), F32),
            pltpu.VMEM((groups * steps, SEGS, LANES), F32),
            pltpu.VMEM((length, LANES), F32),
        ],
        compiler_params=pltpu.CompilerParams(
            dimension_semantics=("arbitrary",), vmem_limit_bytes=40 << 20
        ),
        cost_estimate=pl.CostEstimate(
            flops=length * channels * N * 6000,
            bytes_accessed=length * channels * 10,
            transcendentals=length * channels * N,
        ),
        name="scan_totals",
    )(step_size, activated, dy_scan, rate2, table)


def scan_grads(step_size, activated, dy_scan, rate2, table, segs, enter, groups, begin, channels):
    length = step_size.shape[0]
    steps = length // (groups * SEGS)
    blocks = channels // LANES
    skip = begin // LANES
    body = lambda *refs: grads_kernel(groups, steps, blocks, *refs)
    tall = pl.BlockSpec((length // groups, LANES), lambda g, j: (g, j + skip))
    short = pl.BlockSpec((length // groups, LANES), lambda g, j: (g, j))
    rows = groups * N * SEGS
    grid_spec = pl.GridSpec(
        grid=(groups, blocks),
        in_specs=[
            tall,
            tall,
            tall,
            pl.BlockSpec((N, LANES), lambda g, j: (0, j + skip)),
            pl.BlockSpec((length // groups, LANES), lambda g, j: (g, 0)),
            pl.BlockSpec((groups * SEGS, LANES), lambda g, j: (0, j)),
            pl.BlockSpec((rows, LANES), lambda g, j: (0, j)),
            pl.BlockSpec((rows, LANES), lambda g, j: (0, j)),
            pl.BlockSpec((N, LANES), lambda g, j: (0, j)),
            pl.BlockSpec((N, LANES), lambda g, j: (0, j)),
        ],
        out_specs=[
            short,
            short,
            short,
            pl.BlockSpec((1, N, LANES), lambda g, j: (g, 0, j)),
            pl.BlockSpec((length // groups, LANES), lambda g, j: (g, 0)),
        ],
        scratch_shapes=[
            pltpu.VMEM((steps, 2 * N, SEGS, LANES), F32),
            pltpu.VMEM((steps, SEGS, LANES), F32),
            pltpu.VMEM((length // groups, LANES), F32),
            pltpu.VMEM((blocks, rows, LANES), F32),
            pltpu.VMEM((blocks, rows, LANES), F32),
            pltpu.VMEM((steps, N, SEGS, LANES), F32),
            pltpu.VMEM((steps, N, SEGS, LANES), F32),
            pltpu.VMEM((steps, N, SEGS, LANES), F32),
            pltpu.VMEM((steps, N, SEGS, LANES), F32),
        ],
    )
    return pl.pallas_call(
        body,
        grid_spec=grid_spec,
        out_shape=[
            jax.ShapeDtypeStruct((length, channels), F32),
            jax.ShapeDtypeStruct((length, channels), F32),
            jax.ShapeDtypeStruct((length, channels), F32),
            jax.ShapeDtypeStruct((groups, N, channels), F32),
            jax.ShapeDtypeStruct((length, LANES), F32),
        ],
        compiler_params=pltpu.CompilerParams(
            dimension_semantics=("arbitrary", "arbitrary"), vmem_limit_bytes=48 << 20
        ),
        cost_estimate=pl.CostEstimate(
            flops=length * channels * N * 12000,
            bytes_accessed=length * channels * 22,
            transcendentals=length * channels * N,
        ),
        name="scan_grads",
    )(step_size, activated, dy_scan, rate2, table, *segs, *enter)


MESH = pl.DeviceIdType.MESH
CHUNK = 256


def finish_kernel(
    parts,
    gated_hbm,
    normed_hbm,
    d_gate_hbm,
    d_inner_hbm,
    w_inx_hbm,
    w_inz_hbm,
    x_hbm,
    dy_hbm,
    rms_ref,
    gain_ref,
    small_send_ref,
    small_keep_ref,
    sums_hbm,
    small_ref,
    grad_hbm,
    left,
    right,
    w_x,
    w_z,
    x_cols,
    y_out,
    y_in,
    a_in,
    b_in,
    line,
    first,
    total,
    core_out,
    core_in,
    kept,
    x_out,
    x_in,
    rows_x,
    rows_dy,
    final,
    gain_sum,
    gain_core,
    gain_x,
    gain_out,
    s_out,
    s_in,
    s_a,
    s_b,
    s_line,
    load_sem,
    w_sem,
    y_sem,
    a_sem,
    b_sem,
    c_sem,
    out_sem,
    tp_sem,
    gain_sem,
    final_sem,
    small_sem,
):
    rows, width = x_hbm.shape
    half = width // 2
    dp, z, tp = lax.axis_index("dp"), lax.axis_index("ctx"), lax.axis_index("tp")
    core, x_bit = tp % 2, tp // 2
    near, across, diagonal = tp + 1 - 2 * core, (tp + 2) % 4, 3 - tp
    ends = (z == 0) | (z == 3)
    middle = (z == 1) | (z == 2)
    inward, twin, outward = z // 2 + 1, 3 - z, (z // 2) * 3

    loads = [
        pltpu.make_async_copy(gated_hbm, left.at[0], load_sem.at[0]),
        pltpu.make_async_copy(dy_hbm.at[:, pl.ds(half, half)], right.at[1], load_sem.at[1]),
        pltpu.make_async_copy(dy_hbm.at[:, pl.ds(0, half)], right.at[0], load_sem.at[2]),
        pltpu.make_async_copy(normed_hbm.at[pl.ds(0, half), :], left.at[1], load_sem.at[3]),
        pltpu.make_async_copy(normed_hbm.at[pl.ds(half, half), :], left.at[2], load_sem.at[4]),
        pltpu.make_async_copy(d_gate_hbm, right.at[2], load_sem.at[5]),
        pltpu.make_async_copy(d_inner_hbm, right.at[3], load_sem.at[6]),
    ]
    quarter = rows // 4
    own_row = pl.multiple_of(core * (rows // 2) + x_bit * quarter, quarter)
    loads.append(pltpu.make_async_copy(x_hbm.at[pl.ds(own_row, quarter), :], rows_x, load_sem.at[7]))
    loads.append(pltpu.make_async_copy(dy_hbm.at[pl.ds(own_row, quarter), :], rows_dy, load_sem.at[8]))
    for load in loads:
        load.start()

    barrier = pltpu.get_barrier_semaphore()
    for peer in ({"tp": near}, {"tp": across}, {"tp": diagonal}, {"dp": 1 - dp}):
        pl.semaphore_signal(barrier, inc=1, device_id=peer, device_id_type=MESH)

    @pl.when(ends)
    def _():
        pl.semaphore_signal(barrier, inc=1, device_id={"ctx": inward}, device_id_type=MESH)
        pl.semaphore_wait(barrier, 5)

    @pl.when(middle)
    def _():
        pl.semaphore_signal(barrier, inc=1, device_id={"ctx": twin}, device_id_type=MESH)
        pl.semaphore_signal(barrier, inc=1, device_id={"ctx": outward}, device_id_type=MESH)
        pl.semaphore_wait(barrier, 6)

    def remote(source, target, sems, at, peer):
        return pltpu.make_async_remote_copy(
            src_ref=source,
            dst_ref=target,
            send_sem=sems.at[0, at],
            recv_sem=sems.at[1, at],
            device_id=peer,
            device_id_type=MESH,
        )

    per_weight = parts // 3

    def chunk(k):
        return k // per_weight, pl.multiple_of(k % per_weight * CHUNK, CHUNK)

    def product(slot_l, slot_r, column):
        return jnp.dot(
            left[slot_l], right[slot_r, :, pl.ds(column, CHUNK)], preferred_element_type=F32
        )

    def y_copy(k):
        return remote(y_out.at[k % 4], y_in.at[k % 6], y_sem, k, {"dp": 1 - dp})

    def a_copy(k):
        return remote(line.at[k % 4], a_in.at[k], a_sem, k, {"ctx": inward})

    def b_copy(k):
        return remote(line.at[k % 4], b_in.at[k % 4], b_sem, k, {"ctx": twin})

    def c_copy(k):
        w, column = chunk(k)
        return remote(
            total.at[k % 4], sums_hbm.at[w, :, pl.ds(column, CHUNK)], c_sem, k, {"ctx": outward}
        )

    def own_copy(k):
        w, column = chunk(k)
        return pltpu.make_async_copy(
            total.at[k % 4], sums_hbm.at[w, :, pl.ds(column, CHUNK)], out_sem.at[k]
        )

    def send_y(k):
        w, column = chunk(k)
        up = (w + 1) // 2

        @pl.when(k >= 4)
        def _():
            y_copy(k - 4).wait_send()

        y_out[k % 4] = product(2 * up, w + 1, column).astype(BF16)
        y_copy(k).start()

    def take_y(k):
        w, column = chunk(k)
        up = (w + 1) // 2
        value = product(up, w + up, column)
        y_copy(k).wait_recv()
        value = value + y_in[k % 6].astype(F32)

        @pl.when(ends)
        def _():
            @pl.when(k >= 4)
            def _():
                a_copy(k - 4).wait_send()

            line[k % 4] = value.astype(BF16)
            a_copy(k).start()

        @pl.when(middle)
        def _():
            first[k % 2] = value

    def take_a(k):
        @pl.when(middle)
        def _():
            @pl.when(k >= 4)
            def _():
                b_copy(k - 4).wait_send()

            a_copy(k).wait_recv()
            line[k % 4] = (first[k % 2] + a_in[k].astype(F32)).astype(BF16)
            b_copy(k).start()

    def take_b(k):
        @pl.when(middle)
        def _():
            @pl.when(k >= 4)
            def _():
                c_copy(k - 4).wait_send()
                own_copy(k - 4).wait()

            b_copy(k).wait_recv()
            total[k % 4] = (line[k % 4].astype(F32) + b_in[k % 4].astype(F32)).astype(BF16)
            c_copy(k).start()
            own_copy(k).start()

    def tick(k, _):
        @pl.when(k + 2 < parts)
        def _():
            send_y(k + 2)

        @pl.when((k >= 1) & (k < parts + 1))
        def _():
            take_a(k - 1)

        @pl.when(k < parts)
        def _():
            take_y(k)

        @pl.when((k >= 2) & (k < parts + 2))
        def _():
            take_b(k - 2)

        return 0

    def ticks(begin, end):
        lax.fori_loop(begin, end, tick, 0)

    for load in loads[:2]:
        load.wait()
    send_y(0)
    send_y(1)
    for load in loads[2:7]:
        load.wait()

    block = w_x.shape[0]
    send_row = pl.multiple_of((1 - core) * (rows // 2), rows // 2)
    keep_row = pl.multiple_of(core * (rows // 2), rows // 2)

    def columns(d, _):
        at = pl.multiple_of(d * block, block)
        copies = [
            pltpu.make_async_copy(w_inx_hbm.at[pl.ds(at, block), :], w_x, w_sem.at[0]),
            pltpu.make_async_copy(w_inz_hbm.at[pl.ds(at, block), :], w_z, w_sem.at[1]),
            pltpu.make_async_copy(x_hbm.at[:, pl.ds(at, block)], x_cols, w_sem.at[2]),
        ]
        for copy in copies:
            copy.start()
        for copy in copies:
            copy.wait()
        sums = jnp.zeros((SEGS, block), F32)
        for row, keep in ((send_row, False), (keep_row, True)):
            span = pl.ds(row, rows // 2)
            value = contract_last(right[3, span, :], w_x[...])
            value = value + contract_last(right[2, span, :], w_z[...])
            hat = x_cols[span, :].astype(F32) * rms_ref[span, :]
            sums = sums + jnp.sum((value * hat).reshape(rows // 2 // SEGS, SEGS, block), axis=0)
            if keep:
                kept[:, pl.ds(at, block)] = value
            else:
                core_out[:, pl.ds(at, block)] = value.astype(BF16)
        gain_sum[:, pl.ds(at, block)] = sums
        return 0

    lax.fori_loop(0, width // block, columns, 0)
    core_copy = remote(core_out, core_in, tp_sem, 0, {"tp": near})
    core_copy.start()
    gain_copy = remote(gain_sum, gain_core, gain_sem, 0, {"tp": near})
    gain_copy.start()

    ticks(0, 1)

    core_copy.wait_recv()
    give = pl.multiple_of((1 - x_bit) * quarter, quarter)
    have = pl.multiple_of(x_bit * quarter, quarter)
    x_out[...] = (
        kept[pl.ds(give, quarter), :] + core_in[pl.ds(give, quarter), :].astype(F32)
    ).astype(BF16)
    x_copy = remote(x_out, x_in, tp_sem, 1, {"tp": across})
    x_copy.start()
    gain_copy.wait_recv()
    gain_out[...] = gain_sum[...] + gain_core[...]
    gain_across = remote(gain_out, gain_x, gain_sem, 1, {"tp": across})
    gain_across.start()

    ticks(1, 2)

    small_rows = small_send_ref.shape[0]
    gain_across.wait_recv()
    both = gain_out[...] + gain_x[...]
    quarter_w = half // 2
    s_out[0:small_rows, :] = small_send_ref[...].astype(BF16)
    s_out[small_rows:, :] = jnp.concatenate(
        [both[:, half : half + quarter_w], both[:, half + quarter_w :]], axis=0
    ).astype(BF16)
    small_y = remote(s_out, s_in, small_sem, 0, {"dp": 1 - dp})
    small_y.start()

    ticks(2, 4)

    x_copy.wait_recv()
    r_own = rms_ref[pl.ds(own_row, quarter), :]
    d_normed = (
        kept[pl.ds(have, quarter), :]
        + core_in[pl.ds(have, quarter), :].astype(F32)
        + x_in[...].astype(F32)
    )
    hat = rows_x_wait(loads, rows_x) * r_own
    d_hat = d_normed * gain_ref[...]
    mean = jnp.sum(d_hat * hat, axis=1, keepdims=True) * (1.0 / width)
    final[...] = (rows_dy[...].astype(F32) + r_own * (d_hat - hat * mean)).astype(BF16)
    gathers = []
    for side in range(2):
        place = pl.multiple_of((dp + side - 2 * dp * side) * half, half)
        spot = grad_hbm.at[pl.ds(own_row, quarter), pl.ds(place, half)]
        source = final.at[:, pl.ds(side * half, half)]
        for p, peer in enumerate((near, across, diagonal)):
            gathers.append(remote(source, spot, final_sem, 2 * p + side, {"tp": peer}))
        local = pltpu.make_async_copy(source, spot, load_sem.at[9 + side])
        local.start()
        loads.append(local)
    for copy in gathers:
        copy.start()

    small_y.wait_recv()
    s_keep = jnp.concatenate(
        [
            small_keep_ref[...],
            both[:, :quarter_w],
            both[:, quarter_w:half],
        ],
        axis=0,
    ) + s_in[...].astype(F32)
    small_a = remote(s_line, s_a, small_sem, 1, {"ctx": inward})
    small_b = remote(s_line, s_b, small_sem, 2, {"ctx": twin})
    small_c = remote(small_ref, small_ref, small_sem, 3, {"ctx": outward})

    @pl.when(ends)
    def _():
        s_line[...] = s_keep.astype(BF16)
        small_a.start()

    @pl.when(middle)
    def _():
        small_a.wait_recv()
        s_line[...] = (s_keep + s_a[...].astype(F32)).astype(BF16)
        small_b.start()

    ticks(4, 6)

    @pl.when(middle)
    def _():
        small_b.wait_recv()
        small_ref[...] = (s_line[...].astype(F32) + s_b[...].astype(F32)).astype(BF16)
        small_c.start()

    ticks(6, parts + 2)

    for k in range(parts - 4, parts):
        y_copy(k).wait_send()

    @pl.when(ends)
    def _():
        for k in range(parts - 4, parts):
            a_copy(k).wait_send()
        for k in range(parts):
            c_copy(k).wait_recv()
        small_a.wait_send()
        small_c.wait_recv()

    @pl.when(middle)
    def _():
        for k in range(parts - 4, parts):
            b_copy(k).wait_send()
            c_copy(k).wait_send()
            own_copy(k).wait()
        small_b.wait_send()
        small_c.wait_send()

    core_copy.wait_send()
    x_copy.wait_send()
    gain_copy.wait_send()
    gain_across.wait_send()
    small_y.wait_send()
    for copy in gathers:
        copy.wait()
    for local in loads[9:]:
        local.wait()


def rows_x_wait(loads, ref):
    loads[7].wait()
    loads[8].wait()
    return ref[...].astype(F32)


def finish(gated, normed, d_gate, d_inner, w_inx, w_inz, x_all, dy_all, rms, gain, small_send, small_keep):
    rows, width = x_all.shape
    channels = w_inx.shape[1]
    parts = 3 * (channels // CHUNK)
    half = width // 2
    small = small_send.shape[0] + 2 * SEGS
    block = 512
    hbm = pl.BlockSpec(memory_space=pl.ANY)
    vmem = pl.BlockSpec(memory_space=pltpu.VMEM)
    dma = pltpu.SemaphoreType.DMA
    piece = (half, CHUNK)
    quarter = rows // 4
    return pl.pallas_call(
        lambda *refs: finish_kernel(parts, *refs),
        in_specs=[hbm] * 8 + [vmem] * 4,
        out_specs=[hbm, vmem, hbm],
        out_shape=[
            jax.ShapeDtypeStruct((3, half, channels), BF16),
            jax.ShapeDtypeStruct((small, small_send.shape[1]), BF16),
            jax.ShapeDtypeStruct((rows, width), BF16),
        ],
        scratch_shapes=[
            pltpu.VMEM((3, half, rows), BF16),
            pltpu.VMEM((4, rows, channels), BF16),
            pltpu.VMEM((block, channels), BF16),
            pltpu.VMEM((block, channels), BF16),
            pltpu.VMEM((rows, block), BF16),
            pltpu.VMEM((4,) + piece, BF16),
            pltpu.VMEM((6,) + piece, BF16),
            pltpu.VMEM((parts,) + piece, BF16),
            pltpu.VMEM((4,) + piece, BF16),
            pltpu.VMEM((4,) + piece, BF16),
            pltpu.VMEM((2,) + piece, F32),
            pltpu.VMEM((4,) + piece, BF16),
            pltpu.VMEM((rows // 2, width), BF16),
            pltpu.VMEM((rows // 2, width), BF16),
            pltpu.VMEM((rows // 2, width), F32),
            pltpu.VMEM((quarter, width), BF16),
            pltpu.VMEM((quarter, width), BF16),
            pltpu.VMEM((quarter, width), BF16),
            pltpu.VMEM((quarter, width), BF16),
            pltpu.VMEM((quarter, width), BF16),
            pltpu.VMEM((SEGS, width), F32),
            pltpu.VMEM((SEGS, width), F32),
            pltpu.VMEM((SEGS, width), F32),
            pltpu.VMEM((SEGS, width), F32),
            pltpu.VMEM((small, small_send.shape[1]), BF16),
            pltpu.VMEM((small, small_send.shape[1]), BF16),
            pltpu.VMEM((small, small_send.shape[1]), BF16),
            pltpu.VMEM((small, small_send.shape[1]), BF16),
            pltpu.VMEM((small, small_send.shape[1]), BF16),
            dma((11,)),
            dma((3,)),
            dma((2, parts)),
            dma((2, parts)),
            dma((2, parts)),
            dma((2, parts)),
            dma((parts,)),
            dma((2, 2)),
            dma((2, 2)),
            dma((2, 6)),
            dma((2, 4)),
        ],
        compiler_params=pltpu.CompilerParams(
            collective_id=0, has_side_effects=True, vmem_limit_bytes=63000 << 10
        ),
        cost_estimate=pl.CostEstimate(
            flops=150_000_000_000, bytes_accessed=60_000_000, transcendentals=0
        ),
        name="finish",
    )(gated, normed, d_gate, d_inner, w_inx, w_inz, x_all, dy_all, rms, gain, small_send, small_keep)


def swap_pairs(value, axis, distance):
    count = lax.axis_size(axis)
    return lax.ppermute(value, axis, [(i, i ^ distance) for i in range(count)])


def ordered(mine, other, bit, axis=0):
    return jnp.where(
        bit == 0,
        jnp.concatenate([mine, other], axis=axis),
        jnp.concatenate([other, mine], axis=axis),
    )


def half_of(value, index, axis=0):
    size = value.shape[axis] // 2
    return lax.dynamic_slice_in_dim(value, index * size, size, axis)


def tp_sum(value):
    distance = 1
    while distance < lax.axis_size("tp"):
        value = value + swap_pairs(value, "tp", distance)
        distance *= 2
    return value


def tp_scatter(value):
    index, distance = lax.axis_index("tp"), 1
    while distance < lax.axis_size("tp"):
        mine = (index // distance) % 2
        got = swap_pairs(half_of(value, 1 - mine).astype(BF16), "tp", distance)
        value = half_of(value, mine).astype(F32) + got.astype(F32)
        distance *= 2
    return value


def tp_rows():
    index, distance, at, size = lax.axis_index("tp"), 1, 0, lax.axis_size("tp")
    while distance < lax.axis_size("tp"):
        size //= 2
        at = at + (index // distance) % 2 * size
        distance *= 2
    return at


def per_device(
    hidden_in,
    seq_lengths,
    pack_order,
    norm_gain,
    in_x_weight,
    in_z_weight,
    conv_weight,
    conv_bias,
    x_weight,
    dt_weight,
    dt_bias,
    a_log,
    skip_weight,
    out_weight,
    out_grad,
):
    length, width = hidden_in.shape
    channels = in_x_weight.shape[1]
    tp_count, dp_count, ctx_count = (lax.axis_size(a) for a in ("tp", "dp", "ctx"))
    dp_index, ctx_index, tp_index = (lax.axis_index(a) for a in ("dp", "ctx", "tp"))
    paired = dp_count == 2
    half = width // dp_count
    groups, splits = 2, 1
    fused = paired and ctx_count == 4 and tp_count == 4 and half == channels == length

    def turned(value, axis):
        if not paired:
            return value
        return jnp.concatenate(
            [half_of(value, dp_index, axis), half_of(value, 1 - dp_index, axis)], axis=axis
        )

    def joined(value, axis):
        if not paired:
            return lax.all_gather(value, "dp", axis=axis, tiled=True)
        other = swap_pairs(value, "dp", 1)
        return jnp.where(
            dp_index == 0,
            jnp.concatenate([value, other], axis=axis),
            jnp.concatenate([other, value], axis=axis),
        )

    def weight(own, axis, after):
        if not paired:
            return lax.all_gather(own, "dp", axis=axis, tiled=True), None
        bit = ctx_index % 2
        piece = half_of(own, bit)
        if after is not None:
            piece, _ = lax.optimization_barrier((piece, after))
        near = swap_pairs(piece, "dp", 1)
        far = swap_pairs(near, "ctx", 1)
        return jnp.concatenate([own, ordered(near, far, bit)], axis=axis), near

    small = jnp.concatenate(
        [conv_weight, conv_bias[None], dt_bias[None], skip_weight[None], a_log.T], axis=0
    )
    small = joined(small, 1).astype(F32)
    gain_full = joined(norm_gain, 0).astype(F32)
    w_proj = joined(x_weight, 0)
    w_step = joined(dt_weight, 0)
    w_inx, sent = weight(in_x_weight, 0, small)
    w_inz, sent = weight(in_z_weight, 0, sent)
    w_out, sent = weight(out_weight, 1, sent)
    gain_full = turned(gain_full, 0)
    taps_full = small[:K]
    conv_shift, step_bias, skip_full = small[K], small[K + 1], small[K + 2]
    decay_rate = -jnp.exp(small[K + 3 :])

    starts = piece_starts(seq_lengths[0], pack_order[0])
    positions = ctx_index * length + jnp.arange(length, dtype=jnp.int32)

    def piece(at):
        return jnp.sum((at[:, None] >= starts[None, :]).astype(jnp.int32), axis=1)

    piece_now = piece(positions)
    masks = [(piece(positions - back) == piece_now).astype(F32) for back in (3, 2, 1)]
    blocked = (1.0 - masks[2]) * FAR

    rows_all = turned(hidden_in, 1)
    grad_all = turned(out_grad, 1)
    rows_in = rows_all.astype(F32)
    inv_rms = lax.rsqrt(jnp.mean(rows_in * rows_in, axis=1, keepdims=True) + EPSILON)
    normed = (rows_in * inv_rms * gain_full).astype(BF16)
    inner_x = jnp.dot(normed, w_inx, preferred_element_type=F32).astype(BF16)
    halo = shifted(inner_x[length - (K - 1) :], "ctx", 1)
    extended = jnp.concatenate([halo, inner_x], axis=0).astype(F32)
    conv_pre = conv_shift[None, :] + taps_full[K - 1] * extended[K - 1 :]
    for tap in range(K - 1):
        conv_pre = conv_pre + taps_full[tap] * extended[tap : tap + length] * masks[tap][:, None]
    activated = jax.nn.silu(conv_pre).astype(BF16)
    projected = tp_sum(jnp.dot(activated, w_proj, preferred_element_type=F32))
    gate_z = jnp.dot(normed, w_inz, preferred_element_type=F32)
    d_gated = contract_last(grad_all, w_out)
    gate_sig = jax.nn.sigmoid(gate_z)
    dy_scan = d_gated * gate_z * gate_sig

    step_low = projected[:, :R].astype(BF16)
    step_pre = jnp.dot(step_low, w_step, preferred_element_type=F32) + step_bias
    step_size = jax.nn.softplus(step_pre)
    table = jnp.concatenate(
        [
            projected[:, R:],
            blocked[:, None],
            jnp.zeros((length, LANES - 2 * N - 1), F32),
        ],
        axis=1,
    )
    rate2 = decay_rate * LOG2E
    share = channels // splits

    def entering(whole, rate):
        state, back, spent = whole[:N], whole[N : 2 * N], whole[2 * N : 2 * N + 1]
        h_in = jnp.zeros_like(state)
        c_in = jnp.zeros_like(back)
        below = jnp.zeros_like(spent)
        above = jnp.zeros_like(spent)
        distance = 1
        while distance < ctx_count:
            got = swap_pairs(jnp.concatenate([state, back, jnp.broadcast_to(spent, (8,) + spent.shape[1:])], axis=0), "ctx", distance)
            o_state, o_back, o_spent = got[:N], got[N : 2 * N], got[2 * N : 2 * N + 1]
            upper = (ctx_index // distance) % 2 == 1
            h_in = jnp.where(upper, jnp.exp2(rate * below) * o_state + h_in, h_in)
            c_in = jnp.where(upper, c_in, jnp.exp2(rate * above) * o_back + c_in)
            below = jnp.where(upper, below + o_spent, below)
            above = jnp.where(upper, above, above + o_spent)
            mine, other = jnp.exp2(rate * spent), jnp.exp2(rate * o_spent)
            state, back = (
                jnp.where(upper, mine * o_state + state, other * state + o_state),
                jnp.where(upper, o_back + other * back, back + mine * o_back),
            )
            spent = spent + o_spent
            distance *= 2
        return h_in, c_in

    totals = [
        scan_totals(step_size, activated, dy_scan, rate2, table, groups, k * share, share)
        for k in range(splits)
    ]
    drive_in = activated.astype(F32)

    def input_sum(cotangent):
        value = contract_first(normed, cotangent)
        if paired:
            value = turned(value, 0)
        value = lax.psum_scatter(value.astype(BF16), "dp", scatter_dimension=0, tiled=True)
        return lax.psum(value, "ctx").astype(F32)

    def output_sum(gated):
        value = contract_first(gated, grad_all)
        if paired:
            value = turned(value, 1)
        value = lax.psum_scatter(value.astype(BF16), "dp", scatter_dimension=1, tiled=True)
        return lax.psum(value, "ctx").astype(F32)

    branch, d_low = None, None
    gates, pres, acts, rates_d, gateds = [], [], [], [], []
    for k in range(splits):
        cut = slice(k * share, (k + 1) * share)
        seg_s, seg_h, seg_c, whole = totals[k]
        scan, d_step, d_act, d_rate, d_bc = scan_grads(
            step_size,
            activated,
            dy_scan,
            rate2,
            table,
            (seg_s, seg_h, seg_c),
            entering(whole, rate2[:, cut]),
            groups,
            k * share,
            share,
        )
        sig, z = gate_sig[:, cut], gate_z[:, cut]
        scan_out = scan + skip_full[cut] * drive_in[:, cut]
        gated = (scan_out * z * sig).astype(BF16)
        d_gate = (d_gated[:, cut] * scan_out * sig * (1.0 + z * (1.0 - sig))).astype(BF16)
        d_pre = (d_step * jax.nn.sigmoid(step_pre[:, cut])).astype(BF16)
        low = jnp.concatenate([contract_last(d_pre, w_step[:, cut]), d_bc[:, : 2 * N]], axis=1)
        product = jnp.dot(gated, w_out[cut], preferred_element_type=F32)
        gateds.append(gated)
        branch = product if branch is None else branch + product
        d_low = low if d_low is None else d_low + low
        gates.append(d_gate)
        pres.append(d_pre)
        acts.append(d_act)
        rates_d.append(d_rate)
    d_gate, d_pre, d_act, d_rate, gated_out = (
        jnp.concatenate(v, axis=-1) for v in (gates, pres, acts, rates_d, gateds)
    )
    d_proj = tp_sum(d_low).astype(BF16)

    quarter = length // tp_count
    own_row = tp_rows() * quarter
    own_in = lax.dynamic_slice_in_dim(rows_all, own_row, quarter, 0).astype(F32)
    own_grad = lax.dynamic_slice_in_dim(grad_all, own_row, quarter, 0).astype(F32)
    own_rms = lax.rsqrt(jnp.mean(own_in * own_in, axis=1, keepdims=True) + EPSILON)
    own_hat = own_in * own_rms

    def whole_rows(value):
        distance = tp_count // 2
        while distance >= 1:
            value = ordered(value, swap_pairs(value, "tp", distance), (tp_index // distance) % 2)
            distance //= 2
        if not paired:
            return value
        return ordered(value[:, :half], value[:, half:], dp_index, axis=1)

    out_natural = whole_rows((own_in + tp_scatter(branch)).astype(BF16))

    g_skip = jnp.sum(dy_scan * drive_in, axis=0)
    g_bias = jnp.sum(d_pre.astype(F32), axis=0)
    g_step = contract_first(step_low, d_pre)
    g_log = jnp.sum(d_rate, axis=0) * decay_rate

    g_proj = contract_first(d_proj, activated)
    d_total = d_act + dy_scan * skip_full + contract_last(d_proj, w_proj)
    conv_sig = jax.nn.sigmoid(conv_pre)
    d_conv = d_total * conv_sig * (1.0 + conv_pre * (1.0 - conv_sig))
    g_shift = jnp.sum(d_conv, axis=0)
    g_taps = jnp.stack(
        [
            jnp.sum(d_conv * masks[tap][:, None] * extended[tap : tap + length], axis=0)
            for tap in range(K - 1)
        ]
        + [jnp.sum(d_conv * extended[K - 1 :], axis=0)],
        axis=0,
    )
    d_extended = jnp.pad(d_conv * taps_full[K - 1], ((K - 1, 0), (0, 0)))
    for tap in range(K - 1):
        d_extended = d_extended + jnp.pad(
            d_conv * masks[tap][:, None] * taps_full[tap], ((tap, K - 1 - tap), (0, 0))
        )
    returned = shifted(d_extended[: K - 1], "ctx", -1)
    d_inner = (
        d_extended[K - 1 :] + jnp.pad(returned, ((length - (K - 1), 0), (0, 0)))
    ).astype(BF16)
    packed = jnp.concatenate(
        [g_taps, g_shift[None], g_bias[None], g_skip[None], g_log, g_proj], axis=0
    )
    if fused:

        def side(index):
            piece = half_of(packed, index, 1)
            steps = half_of(g_step, index)
            cut = piece.shape[1]
            rows = [piece, steps[:, :cut], steps[:, cut:]]
            count = sum(r.shape[0] for r in rows)
            rows.append(jnp.zeros((-count % 16, cut), F32))
            return jnp.concatenate(rows, axis=0)

        small_send, small_keep = side(1 - dp_index), side(dp_index)
        sums, small_sum, grad_natural = finish(
            gated_out.T,
            normed.T,
            d_gate,
            d_inner,
            w_inx,
            w_inz,
            rows_all,
            grad_all,
            inv_rms,
            gain_full[None],
            small_send,
            small_keep,
        )
        sums = sums.astype(F32)
        small_sum = small_sum.astype(F32)
        count, high, cut = packed.shape[0], g_step.shape[0] // 2, packed.shape[1] // 2
        at = small_send.shape[0]
        g_out, g_inz, g_inx = sums[0], sums[1], sums[2]
        g_gain = jnp.concatenate(
            [
                jnp.sum(small_sum[at : at + SEGS], axis=0),
                jnp.sum(small_sum[at + SEGS :], axis=0),
            ]
        )
        packed = small_sum[:count]
        g_step = jnp.concatenate(
            [small_sum[count : count + high], small_sum[count + high : count + 2 * high]], axis=1
        )
    else:
        g_inx, g_inz, g_out = input_sum(d_inner), input_sum(d_gate), output_sum(gated_out)
        d_normed = tp_scatter(contract_last(d_inner, w_inx) + contract_last(d_gate, w_inz))
        g_gain = jnp.sum(d_normed * own_hat, axis=0)
        d_hat = d_normed * gain_full
        d_rows = own_grad + own_rms * (
            d_hat - own_hat * jnp.mean(d_hat * own_hat, axis=1, keepdims=True)
        )
        grad_natural = whole_rows(d_rows.astype(BF16))
        g_gain = turned(lax.psum(g_gain, ("ctx", "tp")), 0)
        g_gain = lax.psum_scatter(g_gain, "dp", scatter_dimension=0, tiled=True)
        packed = lax.psum(lax.psum_scatter(packed, "dp", scatter_dimension=1, tiled=True), "ctx")
        g_step = lax.psum(lax.psum_scatter(g_step, "dp", scatter_dimension=0, tiled=True), "ctx")
    return (
        out_natural,
        grad_natural,
        g_gain,
        g_inx,
        g_inz,
        packed[:K],
        packed[K],
        packed[K + 3 + N :].T,
        g_step,
        packed[K + 1],
        packed[K + 3 : K + 3 + N].T,
        packed[K + 2],
        g_out,
    )


def solution(mesh):
    in_specs = (
        P(("dp", "ctx"), None),
        P("dp", None),
        P("dp", None),
        P("dp"),
        P("dp", "tp"),
        P("dp", "tp"),
        P(None, ("tp", "dp")),
        P(("tp", "dp")),
        P(("tp", "dp"), None),
        P("dp", "tp"),
        P(("tp", "dp")),
        P(("tp", "dp"), None),
        P(("tp", "dp")),
        P("tp", "dp"),
        P(("dp", "ctx"), None),
    )
    out_specs = (
        P(("dp", "ctx"), None),
        P(("dp", "ctx"), None),
        P("dp"),
        P("dp", "tp"),
        P("dp", "tp"),
        P(None, ("tp", "dp")),
        P(("tp", "dp")),
        P(("tp", "dp"), None),
        P("dp", "tp"),
        P(("tp", "dp")),
        P(("tp", "dp"), None),
        P(("tp", "dp")),
        P("tp", "dp"),
    )
    return jax.shard_map(
        per_device, mesh=mesh, in_specs=in_specs, out_specs=out_specs, check_vma=False
    )
```

```python
import jax
import jax.numpy as jnp
from jax import lax
from jax.experimental import pallas as pl
from jax.experimental.pallas import tpu as pltpu
from jax.sharding import PartitionSpec as P

N = 16
R = 128
K = 4
ROW = 2048
MICRO = 2
EPSILON = 1e-05

LANES = 128
SEGS = 8
FAR = 1e30
LOG2E = 1.4426950408889634
LN2 = 0.6931471805599453
F32 = jnp.float32
BF16 = jnp.bfloat16


def contract_last(left, right):
    return lax.dot_general(left, right, (((1,), (1,)), ((), ())), preferred_element_type=F32)


def contract_first(left, right):
    return lax.dot_general(left, right, (((0,), (0,)), ((), ())), preferred_element_type=F32)


def shifted(value, axis, steps):
    count = lax.axis_size(axis)
    leading, last = (max(0, -steps), min(count, count - steps))
    return lax.ppermute(value, axis, [(source, source + steps) for source in range(leading, last)])


def piece_starts(lengths, arrangement):
    count = lengths.shape[0]
    ids = jnp.arange(count, dtype=jnp.int32)
    ordered = jnp.sum(jnp.where(arrangement[:, None] == ids[None, :], lengths[None, :], 0), axis=1)
    nat_start = jnp.cumsum(lengths) - lengths
    pack_start = jnp.cumsum(ordered) - ordered
    rows = jnp.arange(1, MICRO, dtype=jnp.int32) * ROW
    slot = jnp.sum((rows[:, None] >= pack_start[None, 1:]).astype(jnp.int32), axis=1)
    in_slot = slot[:, None] == ids[None, :]
    sequence = jnp.sum(jnp.where(in_slot, arrangement[None, :], 0), axis=1)
    begun = jnp.sum(jnp.where(in_slot, pack_start[None, :], 0), axis=1)
    source = (
        jnp.sum(jnp.where(sequence[:, None] == ids[None, :], nat_start[None, :], 0), axis=1)
        + rows
        - begun
    )
    return jnp.concatenate([nat_start, source])


def exact_parts(value):
    high = value.astype(BF16)
    rest = value - high.astype(F32)
    mid = rest.astype(BF16)
    return high, mid, (rest - mid.astype(F32)).astype(BF16)


def spread_columns(table_ref, out_ref, extra_ref, turned_ref, groups, steps):
    rows_of = SEGS * steps
    row = lax.broadcasted_iota(jnp.int32, (2 * LANES, 2 * LANES), 0) % LANES
    side = lax.broadcasted_iota(jnp.int32, (2 * LANES, 2 * LANES), 1) // LANES
    for g in range(groups):

        def one(i, _):
            turned_ref[pl.ds(pl.multiple_of(i * SEGS, SEGS), SEGS), :] = table_ref[
                pl.ds(g * rows_of + i, SEGS, stride=steps), :
            ]
            return 0

        lax.fori_loop(0, steps, one, 0, unroll=8)
        high, mid, low = exact_parts(turned_ref[0:rows_of, :])
        most = jnp.concatenate([high, mid], axis=1)
        for n in range(0, 2 * N + 1, 2):
            pick = (row == n + side).astype(F32).astype(BF16)
            value = jnp.dot(most, pick, preferred_element_type=F32)
            value = value + jnp.dot(low, pick[:LANES], preferred_element_type=F32)
            first = value[:, :LANES].reshape(steps, SEGS, LANES)
            if n < 2 * N:
                out_ref[g * steps : (g + 1) * steps, n] = first
                out_ref[g * steps : (g + 1) * steps, n + 1] = value[:, LANES:].reshape(
                    steps, SEGS, LANES
                )
            else:
                extra_ref[g * steps : (g + 1) * steps] = first


def silu_rows(left_ref, gate_ref, out_ref):
    strip = 128

    def one(r, _):
        at = pl.ds(pl.multiple_of(r * strip, strip), strip)
        gate = gate_ref[at, :]
        out_ref[at, :] = left_ref[at, :] * gate * jax.nn.sigmoid(gate)
        return 0

    lax.fori_loop(0, out_ref.shape[0] // strip, one, 0)


def totals_kernel(
    groups,
    steps,
    step_ref,
    act_ref,
    d_gated_ref,
    gate_ref,
    rate_ref,
    table_ref,
    seg_s_ref,
    seg_h_ref,
    seg_c_ref,
    whole_ref,
    bc_s,
    keep_s,
    act_s,
    dy_s,
):
    rows_of = SEGS * steps

    @pl.when(pl.program_id(0) == 0)
    def _():
        spread_columns(table_ref, bc_s, keep_s, act_s, groups, steps)

    act_s[...] = act_ref[...].astype(F32)
    silu_rows(d_gated_ref, gate_ref, dy_s)
    half = N
    zero = jnp.zeros((SEGS, LANES), F32)
    for g in range(groups):
        for lo in range(0, N, half):
            rates = [
                jnp.broadcast_to(rate_ref[lo + n : lo + n + 1, :], (SEGS, LANES))
                for n in range(half)
            ]

            def one(i, carry):
                total, state, reach, back = carry
                state, reach, back = list(state), list(reach), list(back)
                at = pl.ds(g * rows_of + i, SEGS, stride=steps)
                step, act, dy = step_ref[at, :], act_s[at, :], dy_s[at, :]
                gone = step + keep_s[g * steps + i]
                push = step * act
                for n in range(half):
                    decay = jnp.exp2(gone * rates[n])
                    state[n] = decay * state[n] + push * bc_s[g * steps + i, lo + n]
                    reach[n] = reach[n] * decay
                    back[n] = back[n] + reach[n] * (dy * bc_s[g * steps + i, N + lo + n])
                return (total + gone, tuple(state), tuple(reach), tuple(back))

            total, state, _, back = lax.fori_loop(
                0,
                steps,
                one,
                (zero, (zero,) * half, (jnp.ones((SEGS, LANES), F32),) * half, (zero,) * half),
                unroll=8,
            )
            if lo == 0:
                seg_s_ref[g * SEGS : (g + 1) * SEGS, :] = total
            for n in range(half):
                first = (g * N + lo + n) * SEGS
                seg_h_ref[first : first + SEGS, :] = state[n]
                seg_c_ref[first : first + SEGS, :] = back[n]
    rate = rate_ref[...]
    h = jnp.zeros((N, LANES), F32)
    c = jnp.zeros((N, LANES), F32)
    order = [(g, s) for g in range(groups) for s in range(SEGS)]
    gone = jnp.zeros((1, LANES), F32)
    for g, s in order:
        at = pl.ds(g * N * SEGS + s, N, stride=SEGS)
        spent = seg_s_ref[g * SEGS + s : g * SEGS + s + 1, :]
        h = jnp.exp2(rate * spent) * h + seg_h_ref[at, :]
        gone = gone + spent
    for g, s in order[::-1]:
        at = pl.ds(g * N * SEGS + s, N, stride=SEGS)
        spent = seg_s_ref[g * SEGS + s : g * SEGS + s + 1, :]
        c = jnp.exp2(rate * spent) * c + seg_c_ref[at, :]
    whole_ref[0:N, :] = h
    whole_ref[N : 2 * N, :] = c
    whole_ref[2 * N : 2 * N + SEGS, :] = jnp.broadcast_to(gone, (SEGS, LANES))


def grads_kernel(
    groups,
    steps,
    blocks,
    step_ref,
    pre_ref,
    act_ref,
    d_gated_ref,
    gate_ref,
    skip_ref,
    rate_ref,
    table_ref,
    seg_s_ref,
    seg_h_ref,
    seg_c_ref,
    h_in_ref,
    c_in_ref,
    gated_t_ref,
    gated_ref,
    d_gate_ref,
    d_pre_ref,
    drive_ref,
    d_rate_ref,
    d_bc_ref,
    bc_s,
    keep_s,
    act_s,
    enter_h,
    enter_c,
    decay_s,
    prior_s,
    sum_b,
    sum_c,
    dy_s,
    y_s,
    d_step_s,
    d_act_s,
):
    g, j = pl.program_id(0), pl.program_id(1)

    @pl.when(j == 0)
    def _():
        spread_columns(table_ref, bc_s, keep_s, act_s, 1, steps)
        sum_b[...] = jnp.zeros_like(sum_b)
        sum_c[...] = jnp.zeros_like(sum_c)

    rate = rate_ref[...]

    @pl.when(g == 0)
    def _():
        h = h_in_ref[...]
        c = c_in_ref[...]
        order = [(a, s) for a in range(groups) for s in range(SEGS)]
        for a, s in order:
            at = pl.ds(a * N * SEGS + s, N, stride=SEGS)
            spent = seg_s_ref[a * SEGS + s : a * SEGS + s + 1, :]
            enter_h.at[j][at, :] = h
            h = jnp.exp2(rate * spent) * h + seg_h_ref[at, :]
        for a, s in order[::-1]:
            at = pl.ds(a * N * SEGS + s, N, stride=SEGS)
            spent = seg_s_ref[a * SEGS + s : a * SEGS + s + 1, :]
            enter_c.at[j][at, :] = c
            c = jnp.exp2(rate * spent) * c + seg_c_ref[at, :]

    act_s[...] = act_ref[...].astype(F32)
    silu_rows(d_gated_ref, gate_ref, dy_s)
    first = g * N * SEGS

    def rate_row(n):
        return jnp.broadcast_to(rate_ref[n : n + 1, :], (SEGS, LANES))

    def ahead(i, state):
        state = list(state)
        at = pl.ds(i, SEGS, stride=steps)
        step, act, dy = step_ref[at, :], act_s[at, :], dy_s[at, :]
        gone = step + keep_s[i]
        push = step * act
        y = jnp.zeros((SEGS, LANES), F32)
        for n in range(N):
            decay = jnp.exp2(gone * rate_row(n))
            prior = decay * state[n]
            state[n] = prior + push * bc_s[i, n]
            decay_s[i, n] = decay
            prior_s[i, n] = prior
            y = y + state[n] * bc_s[i, N + n]
            sum_c[i, n] += state[n] * dy
        y_s[at, :] = y
        return tuple(state)

    def enter(ref, n):
        return ref[j, pl.ds(pl.multiple_of(first + n * SEGS, SEGS), SEGS), :]

    lax.fori_loop(0, steps, ahead, tuple(enter(enter_h, n) for n in range(N)), unroll=8)

    def back(k, carry):
        i = steps - 1 - k
        carried, d_rate = list(carry[0]), list(carry[1])
        at = pl.ds(i, SEGS, stride=steps)
        step, act, dy = step_ref[at, :], act_s[at, :], dy_s[at, :]
        push = step * act
        along = jnp.zeros((SEGS, LANES), F32)
        d_step = jnp.zeros((SEGS, LANES), F32)
        for n in range(N):
            grad = dy * bc_s[i, N + n] + carried[n]
            along = along + grad * bc_s[i, n]
            log_grad = grad * prior_s[i, n]
            d_step = d_step + log_grad * rate_row(n)
            d_rate[n] = d_rate[n] + log_grad * step
            carried[n] = grad * decay_s[i, n]
            sum_b[i, n] += grad * push
        d_step_s[at, :] = d_step * LN2 + along * act
        d_act_s[at, :] = along * step
        return (tuple(carried), tuple(d_rate))

    zero = jnp.zeros((SEGS, LANES), F32)
    _, d_rate = lax.fori_loop(
        0, steps, back, (tuple(enter(enter_c, n) for n in range(N)), (zero,) * N), unroll=8
    )
    for n in range(N):
        d_rate_ref[0, n : n + 1, :] = jnp.sum(d_rate[n], axis=0, keepdims=True)

    strip = 64

    def close(r, sums):
        at = pl.ds(pl.multiple_of(r * strip, strip), strip)
        gate, d_gated, act, dy = gate_ref[at, :], d_gated_ref[at, :], act_s[at, :], dy_s[at, :]
        skip = skip_ref[...]
        sig = jax.nn.sigmoid(gate)
        scan_out = y_s[at, :] + skip * act
        gated = scan_out * gate * sig
        y_s[at, :] = gated
        gated_ref[at, :] = gated.astype(BF16)
        d_gate_ref[at, :] = (d_gated * scan_out * sig * (1.0 + gate * (1.0 - sig))).astype(BF16)
        d_pre = (d_step_s[at, :] * jax.nn.sigmoid(pre_ref[at, :])).astype(BF16)
        d_pre_ref[at, :] = d_pre
        drive_ref[at, :] = d_act_s[at, :] + dy * skip

        def fold(value):
            return jnp.sum(value.reshape(strip // SEGS, SEGS, LANES), axis=0)

        return sums[0] + fold(dy * act), sums[1] + fold(d_pre.astype(F32))

    g_skip, g_bias = lax.fori_loop(0, y_s.shape[0] // strip, close, (zero, zero))
    d_rate_ref[0, N : N + 1, :] = jnp.sum(g_skip, axis=0, keepdims=True)
    d_rate_ref[0, N + 1 : N + 2, :] = jnp.sum(g_bias, axis=0, keepdims=True)
    gated_t_ref[...] = y_s[...].T.astype(BF16)

    @pl.when(j == blocks - 1)
    def _():
        column = lax.broadcasted_iota(jnp.int32, (2 * LANES, LANES), 1)
        total = jnp.zeros((steps * SEGS, LANES), F32)
        for n in range(N):
            for ref, at in ((sum_b, n), (sum_c, N + n)):
                pick = (column == at).astype(F32).astype(BF16)
                value = exact_parts(ref[:, n].reshape(steps * SEGS, LANES))
                total = total + jnp.dot(
                    jnp.concatenate(value[:2], axis=1), pick, preferred_element_type=F32
                )
        act_s[...] = total

        def put(i, _):
            d_bc_ref[pl.ds(i, SEGS, stride=steps), :] = act_s[
                pl.ds(pl.multiple_of(i * SEGS, SEGS), SEGS), :
            ]
            return 0

        lax.fori_loop(0, steps, put, 0, unroll=8)


def scan_totals(step_size, activated, d_gated, gate_z, rate2, table, groups):
    length, channels = step_size.shape
    steps = length // (groups * SEGS)
    blocks = channels // LANES
    tall = pl.BlockSpec((length, LANES), lambda j: (0, j))
    rows = groups * N * SEGS
    return pl.pallas_call(
        lambda *refs: totals_kernel(groups, steps, *refs),
        grid=(blocks,),
        in_specs=[
            tall,
            tall,
            tall,
            tall,
            pl.BlockSpec((N, LANES), lambda j: (0, j)),
            pl.BlockSpec((length, LANES), lambda j: (0, 0)),
        ],
        out_specs=[
            pl.BlockSpec((groups * SEGS, LANES), lambda j: (0, j)),
            pl.BlockSpec((rows, LANES), lambda j: (0, j)),
            pl.BlockSpec((rows, LANES), lambda j: (0, j)),
            pl.BlockSpec((2 * N + SEGS, LANES), lambda j: (0, j)),
        ],
        out_shape=[
            jax.ShapeDtypeStruct((groups * SEGS, channels), F32),
            jax.ShapeDtypeStruct((rows, channels), F32),
            jax.ShapeDtypeStruct((rows, channels), F32),
            jax.ShapeDtypeStruct((2 * N + SEGS, channels), F32),
        ],
        scratch_shapes=[
            pltpu.VMEM((groups * steps, 2 * N, SEGS, LANES), F32),
            pltpu.VMEM((groups * steps, SEGS, LANES), F32),
            pltpu.VMEM((length, LANES), F32),
            pltpu.VMEM((length, LANES), F32),
        ],
        compiler_params=pltpu.CompilerParams(
            dimension_semantics=("arbitrary",), vmem_limit_bytes=40 << 20
        ),
        cost_estimate=pl.CostEstimate(
            flops=length * channels * N * 3000,
            bytes_accessed=length * channels * 14,
            transcendentals=length * channels * N,
        ),
        name="scan_totals",
    )(step_size, activated, d_gated, gate_z, rate2, table)


def scan_grads(
    step_size, step_pre, activated, d_gated, gate_z, skip, rate2, table, segs, enter, groups
):
    length, channels = step_size.shape
    steps = length // (groups * SEGS)
    blocks = channels // LANES
    share = length // groups
    tall = pl.BlockSpec((share, LANES), lambda g, j: (g, j))
    one = pl.BlockSpec((share, LANES), lambda g, j: (g, 0))
    rows = groups * N * SEGS

    def wide(height):
        return pl.BlockSpec((height, LANES), lambda g, j: (0, j))

    def shape(dtype, *dims):
        return jax.ShapeDtypeStruct(dims, dtype)

    grid_spec = pl.GridSpec(
        grid=(groups, blocks),
        in_specs=[tall] * 5
        + [wide(1), wide(N), one]
        + [wide(groups * SEGS), wide(rows), wide(rows), wide(N), wide(N)],
        out_specs=[pl.BlockSpec((LANES, share), lambda g, j: (j, g))]
        + [tall] * 4
        + [pl.BlockSpec((1, 3 * SEGS, LANES), lambda g, j: (g, 0, j)), one],
        scratch_shapes=[
            pltpu.VMEM((steps, 2 * N, SEGS, LANES), F32),
            pltpu.VMEM((steps, SEGS, LANES), F32),
            pltpu.VMEM((share, LANES), F32),
            pltpu.VMEM((blocks, rows, LANES), F32),
            pltpu.VMEM((blocks, rows, LANES), F32),
            pltpu.VMEM((steps, N, SEGS, LANES), F32),
            pltpu.VMEM((steps, N, SEGS, LANES), F32),
            pltpu.VMEM((steps, N, SEGS, LANES), F32),
            pltpu.VMEM((steps, N, SEGS, LANES), F32),
            pltpu.VMEM((share, LANES), F32),
            pltpu.VMEM((share, LANES), F32),
            pltpu.VMEM((share, LANES), F32),
            pltpu.VMEM((share, LANES), F32),
        ],
    )
    return pl.pallas_call(
        lambda *refs: grads_kernel(groups, steps, blocks, *refs),
        grid_spec=grid_spec,
        out_shape=[
            shape(BF16, channels, length),
            shape(BF16, length, channels),
            shape(BF16, length, channels),
            shape(BF16, length, channels),
            shape(F32, length, channels),
            shape(F32, groups, 3 * SEGS, channels),
            shape(F32, length, LANES),
        ],
        compiler_params=pltpu.CompilerParams(
            dimension_semantics=("arbitrary", "arbitrary"), vmem_limit_bytes=48 << 20
        ),
        cost_estimate=pl.CostEstimate(
            flops=length * channels * N * 6000,
            bytes_accessed=length * channels * 30,
            transcendentals=length * channels * N,
        ),
        name="scan_grads",
    )(step_size, step_pre, activated, d_gated, gate_z, skip, rate2, table, *segs, *enter)


MESH = pl.DeviceIdType.MESH
CHUNK = 128
AHEAD = 4
LAG = 2
WIDE = 256


def finish_kernel(
    parts,
    gated_t_hbm,
    gated_hbm,
    normed_hbm,
    d_gate_hbm,
    d_pre_hbm,
    drive_hbm,
    inner_hbm,
    halo_hbm,
    w_inx_hbm,
    w_inz_hbm,
    w_out_hbm,
    x_hbm,
    dy_hbm,
    rms_ref,
    gain_ref,
    masks_ref,
    taps_ref,
    w_step_ref,
    w_proj_ref,
    d_bc_ref,
    misc_ref,
    g_step_ref,
    sums_out,
    sums_z,
    sums_x,
    small_ref,
    out_hbm,
    grad_hbm,
    left,
    right,
    w_x,
    w_z,
    x_cols,
    y_out,
    y_in,
    a_in,
    b_in,
    line,
    first,
    total,
    core_out,
    core_in,
    kept,
    x_out,
    x_in,
    rows_x,
    rows_dy,
    final,
    passed,
    gain_sum,
    gain_core,
    gain_x,
    gain_out,
    s_out,
    s_in,
    s_a,
    s_b,
    s_line,
    p_out,
    p_in,
    q_out,
    q_in,
    turned_p,
    drive,
    inner_low,
    inner,
    active,
    pack,
    tail,
    halo_out,
    halo_in,
    load_sem,
    w_sem,
    y_sem,
    a_sem,
    b_sem,
    c_sem,
    out_sem,
    tp_sem,
    gain_sem,
    final_sem,
    small_sem,
    chain_sem,
    proj_sem,
    halo_sem,
):
    rows, width = x_hbm.shape
    half = width // 2
    dp, z, tp = lax.axis_index("dp"), lax.axis_index("ctx"), lax.axis_index("tp")
    core, x_bit = tp % 2, tp // 2
    near, across = tp + 1 - 2 * core, (tp + 2) % 4
    ends = (z == 0) | (z == 3)
    middle = (z == 1) | (z == 2)
    inward, twin, outward = z // 2 + 1, 3 - z, (z // 2) * 3

    def load(source, target, at):
        copy = pltpu.make_async_copy(source, target, load_sem.at[at])
        copy.start()
        return copy

    quarter = rows // 4
    own_row = pl.multiple_of(core * (rows // 2) + x_bit * quarter, quarter)
    got_pre = load(d_pre_hbm, right.at[3], 0)
    got_left = load(gated_t_hbm, left.at[0], 1)
    got_other = load(dy_hbm.at[:, pl.ds(half, half)], right.at[1], 2)
    others = [
        load(dy_hbm.at[:, pl.ds(0, half)], right.at[0], 3),
        load(normed_hbm.at[pl.ds(0, half), :], left.at[1], 4),
        load(normed_hbm.at[pl.ds(half, half), :], left.at[2], 5),
        load(d_gate_hbm, right.at[2], 6),
        load(x_hbm.at[pl.ds(own_row, quarter), :], rows_x, 7),
        load(dy_hbm.at[pl.ds(own_row, quarter), :], rows_dy, 8),
    ]

    barrier = pltpu.get_barrier_semaphore()
    for peer in ({"tp": near}, {"tp": across}, {"dp": 1 - dp}):
        pl.semaphore_signal(barrier, inc=1, device_id=peer, device_id_type=MESH)

    @pl.when(ends)
    def _():
        pl.semaphore_signal(barrier, inc=1, device_id={"ctx": inward}, device_id_type=MESH)
        pl.semaphore_wait(barrier, 4)

    @pl.when(middle)
    def _():
        pl.semaphore_signal(barrier, inc=1, device_id={"ctx": twin}, device_id_type=MESH)
        pl.semaphore_signal(barrier, inc=1, device_id={"ctx": outward}, device_id_type=MESH)
        pl.semaphore_wait(barrier, 5)

    def remote(source, target, sems, at, peer):
        return pltpu.make_async_remote_copy(
            src_ref=source,
            dst_ref=target,
            send_sem=sems.at[0, at],
            recv_sem=sems.at[1, at],
            device_id=peer,
            device_id_type=MESH,
        )

    per_weight = parts // 3

    def chunk(k):
        return k // per_weight, pl.multiple_of(k % per_weight * CHUNK, CHUNK)

    def product(slot_l, slot_r, column):
        return jnp.dot(
            left[slot_l], right[slot_r, :, pl.ds(column, CHUNK)], preferred_element_type=F32
        )

    def y_copy(k):
        return remote(y_out.at[k % 6], y_in.at[k % 8], y_sem, k, {"dp": 1 - dp})

    def a_copy(k):
        return remote(line.at[k % 4], a_in.at[k % 10], a_sem, k, {"ctx": inward})

    def b_copy(k):
        return remote(line.at[k % 4], b_in.at[k % 4], b_sem, k, {"ctx": twin})

    sums = (sums_out, sums_z, sums_x)

    def far_copy(k, ref):
        spot = ref.at[:, pl.ds(chunk(k)[1], CHUNK)]
        return remote(total.at[k % 4], spot, c_sem, k, {"ctx": outward})

    def own_copy(k, ref):
        spot = ref.at[:, pl.ds(chunk(k)[1], CHUNK)]
        return pltpu.make_async_copy(total.at[k % 4], spot, out_sem.at[k])

    def give_c(k, start):
        for w, ref in enumerate(sums):

            @pl.when(k // per_weight == w)
            def _():
                far, own = far_copy(k, ref), own_copy(k, ref)
                if start:
                    far.start()
                    own.start()
                else:
                    far.wait_send()
                    own.wait()

    def wait_c(k):
        far_copy(k, sums_out).wait_recv()

    def send_y(k):
        w, column = chunk(k)
        up = (w + 1) // 2

        @pl.when(k >= 6)
        def _():
            y_copy(k - 6).wait_send()

        y_out[k % 6] = product(2 * up, w + 1, column).astype(BF16)
        y_copy(k).start()

    def take_y(k):
        w, column = chunk(k)
        up = (w + 1) // 2
        value = product(up, w + up, column)
        y_copy(k).wait_recv()
        value = value + y_in[k % 8].astype(F32)

        @pl.when(ends)
        def _():
            @pl.when(k >= 4)
            def _():
                a_copy(k - 4).wait_send()

            @pl.when(k >= 10)
            def _():
                wait_c(k - 10)

            line[k % 4] = value.astype(BF16)
            a_copy(k).start()

        @pl.when(middle)
        def _():
            first[k % 2] = value

    def take_a(k):
        @pl.when(middle)
        def _():
            @pl.when(k >= 4)
            def _():
                b_copy(k - 4).wait_send()

            a_copy(k).wait_recv()
            line[k % 4] = (first[k % 2] + a_in[k % 10].astype(F32)).astype(BF16)
            b_copy(k).start()

    def take_b(k):
        @pl.when(middle)
        def _():
            @pl.when(k >= 4)
            def _():
                give_c(k - 4, False)

            b_copy(k).wait_recv()
            total[k % 4] = (line[k % 4].astype(F32) + b_in[k % 4].astype(F32)).astype(BF16)
            give_c(k, True)

    def tick(k, _):
        @pl.when((k >= 2 * LAG) & (k < parts + 2 * LAG))
        def _():
            take_b(k - 2 * LAG)

        @pl.when((k >= LAG) & (k < parts + LAG))
        def _():
            take_a(k - LAG)

        @pl.when(k < parts)
        def _():
            take_y(k)

        @pl.when(k + AHEAD < parts)
        def _():
            send_y(k + AHEAD)

        return 0

    def ticks(begin, end):
        lax.fori_loop(begin, end, tick, 0)

    got_pre.wait()
    p_out[:, :LANES] = contract_last(right[3], w_step_ref[...]).astype(BF16)
    p_out[:, LANES:] = d_bc_ref[...].astype(BF16)
    p_copy = remote(p_out, p_in, proj_sem, 0, {"tp": near})
    p_copy.start()
    got_gated = load(gated_hbm, right.at[3], 0)
    got_left.wait()
    got_other.wait()
    for k in range(AHEAD):
        send_y(k)
    p_copy.wait_recv()
    q_out[...] = (p_out[...].astype(F32) + p_in[...].astype(F32)).astype(BF16)
    q_copy = remote(q_out, q_in, proj_sem, 1, {"tp": across})
    q_copy.start()

    block = w_x.shape[0]
    send_row = pl.multiple_of((1 - core) * (rows // 2), rows // 2)
    keep_row = pl.multiple_of(core * (rows // 2), rows // 2)
    give = pl.multiple_of((1 - x_bit) * quarter, quarter)
    have = pl.multiple_of(x_bit * quarter, quarter)

    got_gated.wait()

    def out_columns(d, _):
        at = pl.multiple_of(d * block, block)
        copy = pltpu.make_async_copy(w_out_hbm.at[:, pl.ds(at, block)], x_cols, w_sem.at[0])
        copy.start()
        copy.wait()
        core_out[:, pl.ds(at, block)] = jnp.dot(
            right[3, pl.ds(send_row, rows // 2), :], x_cols[...], preferred_element_type=F32
        ).astype(BF16)
        kept[:, pl.ds(at, block)] = jnp.dot(
            right[3, pl.ds(keep_row, rows // 2), :], x_cols[...], preferred_element_type=F32
        ).astype(BF16)
        return 0

    lax.fori_loop(0, width // block, out_columns, 0)
    core_copy = remote(core_out, core_in, tp_sem, 0, {"tp": near})
    core_copy.start()

    def chain_loads(q):
        at = pl.ds(q * WIDE, WIDE)
        return (
            pltpu.make_async_copy(
                drive_hbm.at[:, at], drive.at[pl.ds(SEGS, rows), :], chain_sem.at[0]
            ),
            pltpu.make_async_copy(
                inner_hbm.at[:, at], inner_low.at[pl.ds(2 * SEGS, rows), :], chain_sem.at[1]
            ),
            pltpu.make_async_copy(
                halo_hbm.at[:, at], inner_low.at[pl.ds(0, 2 * SEGS), :], chain_sem.at[2]
            ),
        )

    for copy in chain_loads(0):
        copy.start()
    for copy in others:
        copy.wait()

    ticks(0, 2)

    core_copy.wait_recv()

    def to_across():
        x_out[...] = (
            kept[pl.ds(give, quarter), :].astype(F32) + core_in[pl.ds(give, quarter), :].astype(F32)
        ).astype(BF16)

    to_across()
    x_copy = remote(x_out, x_in, tp_sem, 1, {"tp": across})
    x_copy.start()

    q_copy.wait_recv()
    projected = q_out[...].astype(F32) + q_in[...].astype(F32)
    p_copy.wait_send()
    p_out[...] = projected.astype(BF16)
    turned_p[...] = projected.T.astype(BF16)

    zeros = jnp.zeros((SEGS, WIDE), F32)
    strip = 64
    pad = 2 * SEGS
    drive[0:SEGS, :] = zeros
    drive[rows + SEGS :, :] = zeros

    def chain(q):
        cut = slice(q * WIDE, (q + 1) * WIDE)
        for copy in chain_loads(q):
            copy.wait()
        inner[...] = inner_low[...].astype(F32)
        taps = [taps_ref[i : i + 1, cut] for i in range(K + 1)]

        def down(r, sums):
            at = pl.multiple_of(r * strip, strip)
            mask = masks_ref[pl.ds(at + SEGS, strip), :]
            valid = [mask[:, i : i + 1] for i in range(K - 1)]
            near_rows = inner[pl.ds(at, strip + pad), :]
            moved = [near_rows[pad - (K - 1) + i :][:strip] for i in range(K)]
            moved = [moved[i] * valid[i] for i in range(K - 1)] + moved[K - 1 :]
            pre = taps[K] + taps[K - 1] * moved[K - 1]
            for i in range(K - 1):
                pre = pre + taps[i] * moved[i]
            sig = jax.nn.sigmoid(pre)
            active[pl.ds(at, strip), :] = (pre * sig).astype(BF16)
            whole = drive[pl.ds(at + SEGS, strip), :] + contract_last(
                p_out[pl.ds(at, strip), :], w_proj_ref[cut, :]
            )
            grad = whole * sig * (1.0 + pre * (1.0 - sig))
            drive[pl.ds(at + SEGS, strip), :] = grad

            def fold(value):
                return jnp.sum(value.reshape(strip // SEGS, SEGS, WIDE), axis=0)

            terms = [grad * m for m in moved] + [grad]
            return tuple(s + fold(t) for s, t in zip(sums, terms))

        sums_q = lax.fori_loop(0, rows // strip, down, (zeros,) * (K + 1))
        for i in range(K + 1):
            pack[i : i + 1, cut] = jnp.sum(sums_q[i], axis=0, keepdims=True)

        def spread(base, size):
            grads = drive[pl.ds(base + SEGS, size + SEGS), :]
            mask = masks_ref[pl.ds(base + SEGS, size + SEGS), :]
            value = grads[:size] * taps[K - 1]
            for back in range(1, K):
                valid = grads * mask[:, K - 1 - back : K - back]
                value = value + valid[back : back + size] * taps[K - 1 - back]
            return value

        def up(r, _):
            at = pl.multiple_of(r * strip, strip)
            right[3, pl.ds(at, strip), cut] = spread(at, strip).astype(BF16)
            return 0

        lax.fori_loop(0, rows // strip, up, 0)
        tail[:, cut] = spread(rows - pad, pad)
        halo_out[:, cut] = spread(-SEGS, SEGS)
        pack[4 * SEGS : 4 * SEGS + R + 2 * N, cut] = jnp.dot(
            turned_p[...], active[...], preferred_element_type=F32
        )[: R + 2 * N]

    for q in range(rows // WIDE):
        chain(q)
        if q + 1 < rows // WIDE:
            for copy in chain_loads(q + 1):
                copy.start()
            ticks(2 * q + 2, 2 * q + 4)
    halo_copy = remote(halo_out, halo_in, halo_sem, 0, {"ctx": jnp.maximum(z - 1, 0)})

    @pl.when(z > 0)
    def _():
        halo_copy.start()

    ticks(8, 10)

    def gather(ref, source, base):
        copies = []
        for side in range(2):
            place = pl.multiple_of((dp + side - 2 * dp * side) * half, half)
            spot = ref.at[pl.ds(own_row, quarter), pl.ds(place, half)]
            piece = source.at[:, pl.ds(side * half, half)]
            for p, peer in enumerate((across, near)):
                copies.append(remote(piece, spot, final_sem, base + 2 * p + side, {"tp": peer}))
            copies.append(pltpu.make_async_copy(piece, spot, load_sem.at[9 + base // 2 + side]))
        for copy in copies:
            copy.start()
        return copies

    def forward(ref, copies, base):
        copies[0].wait_recv()
        copies[3].wait_recv()
        row = pl.multiple_of(core * (rows // 2) + (1 - x_bit) * quarter, quarter)
        spot = ref.at[pl.ds(row, quarter), :]
        fetch = pltpu.make_async_copy(spot, passed, load_sem.at[15])
        fetch.start()
        fetch.wait()
        copy = remote(passed, spot, final_sem, base + 4, {"tp": near})
        copy.start()
        return copy

    def finished(copies, last):
        for k, copy in enumerate(copies):
            if k in (0, 3):
                copy.wait_send()
            else:
                copy.wait()
        last.wait()

    x_copy.wait_recv()

    def summed_rows():
        return (
            kept[pl.ds(have, quarter), :].astype(F32)
            + core_in[pl.ds(have, quarter), :].astype(F32)
            + x_in[...].astype(F32)
        )

    final[...] = (rows_x[...].astype(F32) + summed_rows()).astype(BF16)
    out_copies = gather(out_hbm, final, 0)

    @pl.when(z < 3)
    def _():
        halo_copy.wait_recv()
        tail[SEGS:, :] = tail[SEGS:, :] + halo_in[...]

    right[3, rows - pad :, :] = tail[...].astype(BF16)

    ticks(10, 12)

    core_copy.wait_send()
    x_copy.wait_send()

    def columns(d, _):
        at = pl.multiple_of(d * block, block)
        copies = [
            pltpu.make_async_copy(w_inx_hbm.at[pl.ds(at, block), :], w_x, w_sem.at[0]),
            pltpu.make_async_copy(w_inz_hbm.at[pl.ds(at, block), :], w_z, w_sem.at[1]),
            pltpu.make_async_copy(x_hbm.at[:, pl.ds(at, block)], x_cols, w_sem.at[2]),
        ]
        for copy in copies:
            copy.start()
        for copy in copies:
            copy.wait()
        sums_d = jnp.zeros((SEGS, block), F32)
        for row, keep in ((send_row, False), (keep_row, True)):
            span = pl.ds(row, rows // 2)
            value = contract_last(right[3, span, :], w_x[...])
            value = value + contract_last(right[2, span, :], w_z[...])
            hat = x_cols[span, :].astype(F32) * rms_ref[span, :]
            sums_d = sums_d + jnp.sum(
                (value * hat).reshape(rows // 2 // SEGS, SEGS, block), axis=0
            )
            target = kept if keep else core_out
            target[:, pl.ds(at, block)] = value.astype(BF16)
        gain_sum[:, pl.ds(at, block)] = sums_d
        return 0

    lax.fori_loop(0, width // block, columns, 0)
    gain_copy = remote(gain_sum, gain_core, gain_sem, 0, {"tp": near})
    gain_copy.start()
    gain_copy.wait_recv()
    core_again = remote(core_out, core_in, tp_sem, 2, {"tp": near})
    core_again.start()
    gain_out[...] = gain_sum[...] + gain_core[...]
    gain_across = remote(gain_out, gain_x, gain_sem, 1, {"tp": across})
    gain_across.start()

    ticks(12, 14)

    core_again.wait_recv()
    to_across()
    gain_across.wait_recv()
    x_again = remote(x_out, x_in, tp_sem, 3, {"tp": across})
    x_again.start()

    ticks(14, 16)

    both = gain_out[...] + gain_x[...]
    fine = half // 2
    steps_half = g_step_ref.shape[0] // 2
    base = 4 * SEGS + R + 2 * N
    pack[K + 1 : SEGS, :] = jnp.zeros((SEGS - K - 1, 2 * fine), F32)
    pack[SEGS : 4 * SEGS, :] = misc_ref[...]

    def small_rows(index, lanes):
        column = pl.multiple_of(index * fine, fine)
        row = pl.multiple_of(index * steps_half, steps_half)
        return jnp.concatenate(
            [
                pack[:, pl.ds(column, fine)],
                g_step_ref[pl.ds(row, steps_half), :fine],
                g_step_ref[pl.ds(row, steps_half), fine:],
                both[:, lanes : lanes + fine],
                both[:, lanes + fine : lanes + 2 * fine],
            ],
            axis=0,
        )

    s_out[...] = small_rows(1 - dp, half).astype(BF16)
    small_y = remote(s_out, s_in, small_sem, 0, {"dp": 1 - dp})
    small_y.start()
    out_last = forward(out_hbm, out_copies, 0)

    ticks(16, 18)

    x_again.wait_recv()
    r_own = rms_ref[pl.ds(own_row, quarter), :]
    d_normed = summed_rows()
    hat = rows_x[...].astype(F32) * r_own
    d_hat = d_normed * gain_ref[...]
    mean = jnp.sum(d_hat * hat, axis=1, keepdims=True) * (1.0 / width)
    rows_dy[...] = (rows_dy[...].astype(F32) + r_own * (d_hat - hat * mean)).astype(BF16)
    grad_copies = gather(grad_hbm, rows_dy, 6)

    ticks(18, 20)

    small_y.wait_recv()
    s_keep = small_rows(dp, 0) + s_in[...].astype(F32)
    small_a = remote(s_line, s_a, small_sem, 1, {"ctx": inward})
    small_b = remote(s_line, s_b, small_sem, 2, {"ctx": twin})
    small_c = remote(small_ref, small_ref, small_sem, 3, {"ctx": outward})

    @pl.when(ends)
    def _():
        s_line[...] = s_keep.astype(BF16)
        small_a.start()

    @pl.when(middle)
    def _():
        small_a.wait_recv()
        s_line[...] = (s_keep + s_a[...].astype(F32)).astype(BF16)
        small_b.start()

    ticks(20, 22)

    finished(out_copies, out_last)
    grad_last = forward(grad_hbm, grad_copies, 6)

    @pl.when(middle)
    def _():
        small_b.wait_recv()
        small_ref[...] = (s_line[...].astype(F32) + s_b[...].astype(F32)).astype(BF16)
        small_c.start()

    ticks(22, parts + 2 * LAG)

    for k in range(parts - 6, parts):
        y_copy(k).wait_send()

    @pl.when(ends)
    def _():
        for k in range(parts - 4, parts):
            a_copy(k).wait_send()
        for k in range(parts - 10, parts):
            wait_c(k)
        small_a.wait_send()
        small_c.wait_recv()

    @pl.when(middle)
    def _():
        for k in range(parts - 4, parts):
            b_copy(k).wait_send()
            far_copy(k, sums_x).wait_send()
            own_copy(k, sums_x).wait()
        small_b.wait_send()
        small_c.wait_send()

    @pl.when(z > 0)
    def _():
        halo_copy.wait_send()

    q_copy.wait_send()
    core_again.wait_send()
    x_again.wait_send()
    gain_copy.wait_send()
    gain_across.wait_send()
    small_y.wait_send()
    finished(grad_copies, grad_last)


def finish(
    gated_t, gated, normed_t, d_gate, d_pre, drive, inner, halo, w_inx, w_inz, w_out, x_all, dy_all,
    rms, gain, masks, taps, w_step, w_proj, d_bc, misc, g_step,
):
    rows, width = x_all.shape
    channels = w_inx.shape[1]
    parts = 3 * (channels // CHUNK)
    half = width // 2
    small = 4 * SEGS + R + 2 * N + g_step.shape[0] + 2 * SEGS
    fine = half // 2
    block = 512
    hbm = pl.BlockSpec(memory_space=pl.ANY)
    vmem = pl.BlockSpec(memory_space=pltpu.VMEM)
    dma = pltpu.SemaphoreType.DMA
    piece = (half, CHUNK)
    quarter = rows // 4

    def low(*shape):
        return pltpu.VMEM(shape, BF16)

    def full(*shape):
        return pltpu.VMEM(shape, F32)

    return pl.pallas_call(
        lambda *refs: finish_kernel(parts, *refs),
        in_specs=[hbm] * 13 + [vmem] * 9,
        out_specs=[hbm, hbm, hbm, vmem, hbm, hbm],
        out_shape=[jax.ShapeDtypeStruct((half, channels), BF16)] * 3
        + [
            jax.ShapeDtypeStruct((small, fine), BF16),
            jax.ShapeDtypeStruct((rows, width), BF16),
            jax.ShapeDtypeStruct((rows, width), BF16),
        ],
        scratch_shapes=[
            low(3, half, rows),
            low(4, rows, channels),
            low(block, channels),
            low(block, channels),
            low(rows, block),
            low(6, *piece),
            low(8, *piece),
            low(10, *piece),
            low(4, *piece),
            low(4, *piece),
            full(2, *piece),
            low(4, *piece),
            low(rows // 2, width),
            low(rows // 2, width),
            low(rows // 2, width),
            low(quarter, width),
            low(quarter, width),
            low(quarter, width),
            low(quarter, width),
            low(quarter, width),
            low(quarter, width),
            full(SEGS, width),
            full(SEGS, width),
            full(SEGS, width),
            full(SEGS, width),
            low(small, fine),
            low(small, fine),
            low(small, fine),
            low(small, fine),
            low(small, fine),
            low(rows, 2 * LANES),
            low(rows, 2 * LANES),
            low(rows, 2 * LANES),
            low(rows, 2 * LANES),
            low(2 * LANES, rows),
            full(rows + 2 * SEGS, WIDE),
            low(rows + 2 * SEGS, WIDE),
            full(rows + 2 * SEGS, WIDE),
            low(rows, WIDE),
            full(4 * SEGS + R + 2 * N, channels),
            full(2 * SEGS, channels),
            full(SEGS, channels),
            full(SEGS, channels),
            dma((16,)),
            dma((3,)),
            dma((2, parts)),
            dma((2, parts)),
            dma((2, parts)),
            dma((2, parts)),
            dma((parts,)),
            dma((2, 4)),
            dma((2, 2)),
            dma((2, 11)),
            dma((2, 4)),
            dma((3,)),
            dma((2, 2)),
            dma((2, 1)),
        ],
        compiler_params=pltpu.CompilerParams(
            collective_id=0, has_side_effects=True, vmem_limit_bytes=63900 << 10
        ),
        cost_estimate=pl.CostEstimate(
            flops=200_000_000_000, bytes_accessed=60_000_000, transcendentals=0
        ),
        name="finish",
    )(
        gated_t, gated, normed_t, d_gate, d_pre, drive, inner, halo, w_inx, w_inz, w_out, x_all, dy_all,
        rms, gain, masks, taps, w_step, w_proj, d_bc, misc, g_step,
    )


def swap_pairs(value, axis, distance):
    count = lax.axis_size(axis)
    return lax.ppermute(value, axis, [(i, i ^ distance) for i in range(count)])


def ordered(mine, other, bit, axis=0):
    return jnp.where(
        bit == 0,
        jnp.concatenate([mine, other], axis=axis),
        jnp.concatenate([other, mine], axis=axis),
    )


def half_of(value, index, axis=0):
    size = value.shape[axis] // 2
    return lax.dynamic_slice_in_dim(value, index * size, size, axis)


def tp_sum(value):
    distance = 1
    while distance < lax.axis_size("tp"):
        value = value + swap_pairs(value, "tp", distance)
        distance *= 2
    return value


def tp_scatter(value):
    index, distance = lax.axis_index("tp"), 1
    while distance < lax.axis_size("tp"):
        mine = (index // distance) % 2
        got = swap_pairs(half_of(value, 1 - mine).astype(BF16), "tp", distance)
        value = half_of(value, mine).astype(F32) + got.astype(F32)
        distance *= 2
    return value


def tp_rows():
    index, distance, at, size = lax.axis_index("tp"), 1, 0, lax.axis_size("tp")
    while distance < lax.axis_size("tp"):
        size //= 2
        at = at + (index // distance) % 2 * size
        distance *= 2
    return at


def per_device(
    hidden_in,
    seq_lengths,
    pack_order,
    norm_gain,
    in_x_weight,
    in_z_weight,
    conv_weight,
    conv_bias,
    x_weight,
    dt_weight,
    dt_bias,
    a_log,
    skip_weight,
    out_weight,
    out_grad,
):
    length, width = hidden_in.shape
    channels = in_x_weight.shape[1]
    tp_count, dp_count, ctx_count = (lax.axis_size(a) for a in ("tp", "dp", "ctx"))
    dp_index, ctx_index, tp_index = (lax.axis_index(a) for a in ("dp", "ctx", "tp"))
    paired = dp_count == 2
    half = width // dp_count
    groups = 2
    fused = paired and ctx_count == 4 and tp_count == 4 and half == channels == length

    def turned(value, axis):
        if not paired:
            return value
        return jnp.concatenate(
            [half_of(value, dp_index, axis), half_of(value, 1 - dp_index, axis)], axis=axis
        )

    def joined(value, axis):
        if not paired:
            return lax.all_gather(value, "dp", axis=axis, tiled=True)
        other = swap_pairs(value, "dp", 1)
        return jnp.where(
            dp_index == 0,
            jnp.concatenate([value, other], axis=axis),
            jnp.concatenate([other, value], axis=axis),
        )

    def weight(own, axis, after):
        if not paired:
            return lax.all_gather(own, "dp", axis=axis, tiled=True), None
        bit = ctx_index % 2
        piece = half_of(own, bit)
        if after is not None:
            piece, _ = lax.optimization_barrier((piece, after))
        near = swap_pairs(piece, "dp", 1)
        far = swap_pairs(near, "ctx", 1)
        return jnp.concatenate([own, ordered(near, far, bit)], axis=axis), near

    small = jnp.concatenate(
        [conv_weight, conv_bias[None], dt_bias[None], skip_weight[None], a_log.T], axis=0
    )
    small = joined(small, 1).astype(F32)
    gain_full = joined(norm_gain, 0).astype(F32)
    w_proj = joined(x_weight, 0)
    w_step = joined(dt_weight, 0)
    w_inx, sent = weight(in_x_weight, 0, None)
    w_inz, sent = weight(in_z_weight, 0, sent)
    w_out, sent = weight(out_weight, 1, sent)
    gain_full = turned(gain_full, 0)
    taps_full = small[:K]
    conv_shift, step_bias, skip_full = small[K], small[K + 1], small[K + 2]
    decay_rate = -jnp.exp(small[K + 3 :])

    starts = piece_starts(seq_lengths[0], pack_order[0])
    positions = ctx_index * length + jnp.arange(length, dtype=jnp.int32)

    def piece(at):
        return jnp.sum((at[:, None] >= starts[None, :]).astype(jnp.int32), axis=1)

    piece_now = piece(positions)
    masks = [(piece(positions - back) == piece_now).astype(F32) for back in (3, 2, 1)]
    blocked = (1.0 - masks[2]) * FAR

    rows_all = turned(hidden_in, 1)
    grad_all = turned(out_grad, 1)
    rows_in = rows_all.astype(F32)
    inv_rms = lax.rsqrt(jnp.mean(rows_in * rows_in, axis=1, keepdims=True) + EPSILON)
    normed = (rows_in * inv_rms * gain_full).astype(BF16)
    inner_x = jnp.dot(normed, w_inx, preferred_element_type=F32).astype(BF16)
    halo = shifted(inner_x[length - (K - 1) :], "ctx", 1)
    extended = jnp.concatenate([halo, inner_x], axis=0).astype(F32)
    conv_pre = conv_shift[None, :] + taps_full[K - 1] * extended[K - 1 :]
    for tap in range(K - 1):
        conv_pre = conv_pre + taps_full[tap] * extended[tap : tap + length] * masks[tap][:, None]
    activated = jax.nn.silu(conv_pre).astype(BF16)
    projected = tp_sum(jnp.dot(activated, w_proj, preferred_element_type=F32))
    gate_z = jnp.dot(normed, w_inz, preferred_element_type=F32)
    d_gated = contract_last(grad_all, w_out)

    step_low = projected[:, :R].astype(BF16)
    step_pre = jnp.dot(step_low, w_step, preferred_element_type=F32) + step_bias
    step_size = jax.nn.softplus(step_pre)
    table = jnp.concatenate(
        [
            projected[:, R:],
            blocked[:, None],
            jnp.zeros((length, LANES - 2 * N - 1), F32),
        ],
        axis=1,
    )
    rate2 = decay_rate * LOG2E

    def entering(whole, rate):
        state, back, spent = whole[:N], whole[N : 2 * N], whole[2 * N : 2 * N + 1]
        h_in = jnp.zeros_like(state)
        c_in = jnp.zeros_like(back)
        below = jnp.zeros_like(spent)
        above = jnp.zeros_like(spent)
        distance = 1
        while distance < ctx_count:
            got = swap_pairs(jnp.concatenate([state, back, jnp.broadcast_to(spent, (8,) + spent.shape[1:])], axis=0), "ctx", distance)
            o_state, o_back, o_spent = got[:N], got[N : 2 * N], got[2 * N : 2 * N + 1]
            upper = (ctx_index // distance) % 2 == 1
            h_in = jnp.where(upper, jnp.exp2(rate * below) * o_state + h_in, h_in)
            c_in = jnp.where(upper, c_in, jnp.exp2(rate * above) * o_back + c_in)
            below = jnp.where(upper, below + o_spent, below)
            above = jnp.where(upper, above, above + o_spent)
            mine, other = jnp.exp2(rate * spent), jnp.exp2(rate * o_spent)
            state, back = (
                jnp.where(upper, mine * o_state + state, other * state + o_state),
                jnp.where(upper, o_back + other * back, back + mine * o_back),
            )
            spent = spent + o_spent
            distance *= 2
        return h_in, c_in

    *segs, whole = scan_totals(step_size, activated, d_gated, gate_z, rate2, table, groups)
    gated_t, gated, d_gate, d_pre, d_drive, rates_d, d_bc = scan_grads(
        step_size,
        step_pre,
        activated,
        d_gated,
        gate_z,
        skip_full[None],
        rate2,
        table,
        segs,
        entering(whole, rate2),
        groups,
    )
    rates_d = jnp.sum(rates_d, axis=0)
    g_log, g_skip, g_bias = rates_d[:N] * decay_rate, rates_d[N], rates_d[N + 1]
    g_step = contract_first(step_low, d_pre)

    def input_sum(cotangent):
        value = contract_first(normed, cotangent)
        if paired:
            value = turned(value, 0)
        value = lax.psum_scatter(value.astype(BF16), "dp", scatter_dimension=0, tiled=True)
        return lax.psum(value, "ctx").astype(F32)

    def output_sum(gated):
        value = contract_first(gated, grad_all)
        if paired:
            value = turned(value, 1)
        value = lax.psum_scatter(value.astype(BF16), "dp", scatter_dimension=1, tiled=True)
        return lax.psum(value, "ctx").astype(F32)

    if fused:
        padded = jnp.pad(jnp.stack(masks, axis=1), ((SEGS, SEGS), (0, 1)))
        before = jnp.pad(halo, ((2 * SEGS - (K - 1), 0), (0, 0)))
        taps = jnp.pad(jnp.concatenate([taps_full, conv_shift[None]]), ((0, SEGS - K - 1), (0, 0)))
        misc = jnp.pad(
            jnp.concatenate([g_bias[None], g_skip[None], g_log]), ((0, 3 * SEGS - N - 2), (0, 0))
        )
        s_out, s_z, s_x, small_sum, out_natural, grad_natural = finish(
            gated_t,
            gated,
            normed.T,
            d_gate,
            d_pre,
            d_drive,
            inner_x,
            before,
            w_inx,
            w_inz,
            w_out,
            rows_all,
            grad_all,
            inv_rms,
            gain_full[None],
            padded,
            taps,
            w_step,
            jnp.pad(w_proj, ((0, 0), (0, 2 * LANES - R - 2 * N))),
            d_bc,
            misc,
            g_step,
        )
        small_sum = small_sum.astype(F32)
        steps_half = g_step.shape[0] // 2
        at = 4 * SEGS + R + 2 * N
        end = at + 2 * steps_half
        return (
            out_natural,
            grad_natural,
            jnp.concatenate(
                [
                    jnp.sum(small_sum[end : end + SEGS], axis=0),
                    jnp.sum(small_sum[end + SEGS :], axis=0),
                ]
            ),
            s_x.astype(F32),
            s_z.astype(F32),
            small_sum[:K],
            small_sum[K],
            small_sum[4 * SEGS : at].T,
            jnp.concatenate(
                [small_sum[at : at + steps_half], small_sum[at + steps_half : end]], axis=1
            ),
            small_sum[SEGS],
            small_sum[SEGS + 2 : SEGS + 2 + N].T,
            small_sum[SEGS + 1],
            s_out.astype(F32),
        )

    branch = jnp.dot(gated, w_out, preferred_element_type=F32)
    d_proj = tp_sum(
        jnp.concatenate([contract_last(d_pre, w_step), d_bc[:, : 2 * N]], axis=1)
    ).astype(BF16)

    quarter = length // tp_count
    own_row = tp_rows() * quarter
    own_in = lax.dynamic_slice_in_dim(rows_all, own_row, quarter, 0).astype(F32)
    own_grad = lax.dynamic_slice_in_dim(grad_all, own_row, quarter, 0).astype(F32)
    own_rms = lax.rsqrt(jnp.mean(own_in * own_in, axis=1, keepdims=True) + EPSILON)
    own_hat = own_in * own_rms

    def whole_rows(value):
        distance = tp_count // 2
        while distance >= 1:
            value = ordered(value, swap_pairs(value, "tp", distance), (tp_index // distance) % 2)
            distance //= 2
        if not paired:
            return value
        return ordered(value[:, :half], value[:, half:], dp_index, axis=1)

    out_natural = whole_rows((own_in + tp_scatter(branch)).astype(BF16))

    g_proj = contract_first(d_proj, activated)
    d_total = d_drive + contract_last(d_proj, w_proj)
    conv_sig = jax.nn.sigmoid(conv_pre)
    d_conv = d_total * conv_sig * (1.0 + conv_pre * (1.0 - conv_sig))
    g_shift = jnp.sum(d_conv, axis=0)
    g_taps = jnp.stack(
        [
            jnp.sum(d_conv * masks[tap][:, None] * extended[tap : tap + length], axis=0)
            for tap in range(K - 1)
        ]
        + [jnp.sum(d_conv * extended[K - 1 :], axis=0)],
        axis=0,
    )
    d_extended = jnp.pad(d_conv * taps_full[K - 1], ((K - 1, 0), (0, 0)))
    for tap in range(K - 1):
        d_extended = d_extended + jnp.pad(
            d_conv * masks[tap][:, None] * taps_full[tap], ((tap, K - 1 - tap), (0, 0))
        )
    returned = shifted(d_extended[: K - 1], "ctx", -1)
    d_inner = (
        d_extended[K - 1 :] + jnp.pad(returned, ((length - (K - 1), 0), (0, 0)))
    ).astype(BF16)
    packed = jnp.concatenate(
        [g_taps, g_shift[None], g_bias[None], g_skip[None], g_log, g_proj], axis=0
    )
    g_inx, g_inz, g_out = input_sum(d_inner), input_sum(d_gate), output_sum(gated)
    d_normed = tp_scatter(contract_last(d_inner, w_inx) + contract_last(d_gate, w_inz))
    g_gain = jnp.sum(d_normed * own_hat, axis=0)
    d_hat = d_normed * gain_full
    d_rows = own_grad + own_rms * (
        d_hat - own_hat * jnp.mean(d_hat * own_hat, axis=1, keepdims=True)
    )
    grad_natural = whole_rows(d_rows.astype(BF16))
    g_gain = turned(lax.psum(g_gain, ("ctx", "tp")), 0)
    g_gain = lax.psum_scatter(g_gain, "dp", scatter_dimension=0, tiled=True)
    packed = lax.psum(lax.psum_scatter(packed, "dp", scatter_dimension=1, tiled=True), "ctx")
    g_step = lax.psum(lax.psum_scatter(g_step, "dp", scatter_dimension=0, tiled=True), "ctx")
    return (
        out_natural,
        grad_natural,
        g_gain,
        g_inx,
        g_inz,
        packed[:K],
        packed[K],
        packed[K + 3 + N :].T,
        g_step,
        packed[K + 1],
        packed[K + 3 : K + 3 + N].T,
        packed[K + 2],
        g_out,
    )


def solution(mesh):
    in_specs = (
        P(("dp", "ctx"), None),
        P("dp", None),
        P("dp", None),
        P("dp"),
        P("dp", "tp"),
        P("dp", "tp"),
        P(None, ("tp", "dp")),
        P(("tp", "dp")),
        P(("tp", "dp"), None),
        P("dp", "tp"),
        P(("tp", "dp")),
        P(("tp", "dp"), None),
        P(("tp", "dp")),
        P("tp", "dp"),
        P(("dp", "ctx"), None),
    )
    out_specs = (
        P(("dp", "ctx"), None),
        P(("dp", "ctx"), None),
        P("dp"),
        P("dp", "tp"),
        P("dp", "tp"),
        P(None, ("tp", "dp")),
        P(("tp", "dp")),
        P(("tp", "dp"), None),
        P("dp", "tp"),
        P(("tp", "dp")),
        P(("tp", "dp"), None),
        P(("tp", "dp")),
        P("tp", "dp"),
    )
    return jax.shard_map(
        per_device, mesh=mesh, in_specs=in_specs, out_specs=out_specs, check_vma=False
    )
```

```python
import jax
import jax.numpy as jnp
from jax import lax
from jax.experimental import pallas as pl
from jax.experimental.pallas import tpu as pltpu
from jax.sharding import PartitionSpec as P

N = 16
R = 128
K = 4
ROW = 2048
MICRO = 2
EPSILON = 1e-05

LANES = 128
SEGS = 8
FAR = 1e30
LOG2E = 1.4426950408889634
LN2 = 0.6931471805599453
F32 = jnp.float32
BF16 = jnp.bfloat16


def contract_last(left, right):
    return lax.dot_general(left, right, (((1,), (1,)), ((), ())), preferred_element_type=F32)


def contract_first(left, right):
    return lax.dot_general(left, right, (((0,), (0,)), ((), ())), preferred_element_type=F32)


def shifted(value, axis, steps):
    count = lax.axis_size(axis)
    leading, last = (max(0, -steps), min(count, count - steps))
    return lax.ppermute(value, axis, [(source, source + steps) for source in range(leading, last)])


def piece_starts(lengths, arrangement):
    count = lengths.shape[0]
    ids = jnp.arange(count, dtype=jnp.int32)
    ordered = jnp.sum(jnp.where(arrangement[:, None] == ids[None, :], lengths[None, :], 0), axis=1)
    nat_start = jnp.cumsum(lengths) - lengths
    pack_start = jnp.cumsum(ordered) - ordered
    rows = jnp.arange(1, MICRO, dtype=jnp.int32) * ROW
    slot = jnp.sum((rows[:, None] >= pack_start[None, 1:]).astype(jnp.int32), axis=1)
    in_slot = slot[:, None] == ids[None, :]
    sequence = jnp.sum(jnp.where(in_slot, arrangement[None, :], 0), axis=1)
    begun = jnp.sum(jnp.where(in_slot, pack_start[None, :], 0), axis=1)
    source = (
        jnp.sum(jnp.where(sequence[:, None] == ids[None, :], nat_start[None, :], 0), axis=1)
        + rows
        - begun
    )
    return jnp.concatenate([nat_start, source])


def exact_parts(value):
    high = value.astype(BF16)
    rest = value - high.astype(F32)
    mid = rest.astype(BF16)
    return high, mid, (rest - mid.astype(F32)).astype(BF16)


def spread_columns(table_ref, out_ref, extra_ref, turned_ref, groups, steps):
    rows_of = SEGS * steps
    row = lax.broadcasted_iota(jnp.int32, (2 * LANES, 2 * LANES), 0) % LANES
    side = lax.broadcasted_iota(jnp.int32, (2 * LANES, 2 * LANES), 1) // LANES
    for g in range(groups):

        def one(i, _):
            turned_ref[pl.ds(pl.multiple_of(i * SEGS, SEGS), SEGS), :] = table_ref[
                pl.ds(g * rows_of + i, SEGS, stride=steps), :
            ]
            return 0

        lax.fori_loop(0, steps, one, 0, unroll=8)
        high, mid, low = exact_parts(turned_ref[0:rows_of, :])
        most = jnp.concatenate([high, mid], axis=1)
        for n in range(0, 2 * N + 1, 2):
            pick = (row == n + side).astype(F32).astype(BF16)
            value = jnp.dot(most, pick, preferred_element_type=F32)
            value = value + jnp.dot(low, pick[:LANES], preferred_element_type=F32)
            first = value[:, :LANES].reshape(steps, SEGS, LANES)
            if n < 2 * N:
                out_ref[g * steps : (g + 1) * steps, n] = first
                out_ref[g * steps : (g + 1) * steps, n + 1] = value[:, LANES:].reshape(
                    steps, SEGS, LANES
                )
            else:
                extra_ref[g * steps : (g + 1) * steps] = first


def silu_rows(left_ref, gate_ref, out_ref):
    strip = 128

    def one(r, _):
        at = pl.ds(pl.multiple_of(r * strip, strip), strip)
        gate = gate_ref[at, :]
        out_ref[at, :] = left_ref[at, :] * gate * jax.nn.sigmoid(gate)
        return 0

    lax.fori_loop(0, out_ref.shape[0] // strip, one, 0)


def totals_kernel(
    groups,
    steps,
    step_ref,
    act_ref,
    d_gated_ref,
    gate_ref,
    rate_ref,
    table_ref,
    seg_s_ref,
    seg_h_ref,
    seg_c_ref,
    whole_ref,
    bc_s,
    keep_s,
    act_s,
    dy_s,
):
    rows_of = SEGS * steps

    @pl.when(pl.program_id(0) == 0)
    def _():
        spread_columns(table_ref, bc_s, keep_s, act_s, groups, steps)

    act_s[...] = act_ref[...].astype(F32)
    silu_rows(d_gated_ref, gate_ref, dy_s)
    half = N
    zero = jnp.zeros((SEGS, LANES), F32)
    for g in range(groups):
        for lo in range(0, N, half):
            rates = [
                jnp.broadcast_to(rate_ref[lo + n : lo + n + 1, :], (SEGS, LANES))
                for n in range(half)
            ]

            def one(i, carry):
                total, state, reach, back = carry
                state, reach, back = list(state), list(reach), list(back)
                at = pl.ds(g * rows_of + i, SEGS, stride=steps)
                step, act, dy = step_ref[at, :], act_s[at, :], dy_s[at, :]
                gone = step + keep_s[g * steps + i]
                push = step * act
                for n in range(half):
                    decay = jnp.exp2(gone * rates[n])
                    state[n] = decay * state[n] + push * bc_s[g * steps + i, lo + n]
                    reach[n] = reach[n] * decay
                    back[n] = back[n] + reach[n] * (dy * bc_s[g * steps + i, N + lo + n])
                return (total + gone, tuple(state), tuple(reach), tuple(back))

            total, state, _, back = lax.fori_loop(
                0,
                steps,
                one,
                (zero, (zero,) * half, (jnp.ones((SEGS, LANES), F32),) * half, (zero,) * half),
                unroll=8,
            )
            if lo == 0:
                seg_s_ref[g * SEGS : (g + 1) * SEGS, :] = total
            for n in range(half):
                first = (g * N + lo + n) * SEGS
                seg_h_ref[first : first + SEGS, :] = state[n]
                seg_c_ref[first : first + SEGS, :] = back[n]
    rate = rate_ref[...]
    h = jnp.zeros((N, LANES), F32)
    c = jnp.zeros((N, LANES), F32)
    order = [(g, s) for g in range(groups) for s in range(SEGS)]
    gone = jnp.zeros((1, LANES), F32)
    for g, s in order:
        at = pl.ds(g * N * SEGS + s, N, stride=SEGS)
        spent = seg_s_ref[g * SEGS + s : g * SEGS + s + 1, :]
        h = jnp.exp2(rate * spent) * h + seg_h_ref[at, :]
        gone = gone + spent
    for g, s in order[::-1]:
        at = pl.ds(g * N * SEGS + s, N, stride=SEGS)
        spent = seg_s_ref[g * SEGS + s : g * SEGS + s + 1, :]
        c = jnp.exp2(rate * spent) * c + seg_c_ref[at, :]
    whole_ref[0:N, :] = h
    whole_ref[N : 2 * N, :] = c
    whole_ref[2 * N : 2 * N + SEGS, :] = jnp.broadcast_to(gone, (SEGS, LANES))


def grads_kernel(
    groups,
    steps,
    blocks,
    step_ref,
    pre_ref,
    act_ref,
    d_gated_ref,
    gate_ref,
    skip_ref,
    rate_ref,
    table_ref,
    seg_s_ref,
    seg_h_ref,
    seg_c_ref,
    h_in_ref,
    c_in_ref,
    gated_t_ref,
    gated_ref,
    d_gate_ref,
    d_pre_ref,
    drive_ref,
    d_rate_ref,
    d_bc_ref,
    bc_s,
    keep_s,
    act_s,
    enter_h,
    enter_c,
    decay_s,
    prior_s,
    sum_b,
    sum_c,
    dy_s,
    y_s,
    d_step_s,
    d_act_s,
):
    g, j = pl.program_id(0), pl.program_id(1)

    @pl.when(j == 0)
    def _():
        spread_columns(table_ref, bc_s, keep_s, act_s, 1, steps)
        sum_b[...] = jnp.zeros_like(sum_b)
        sum_c[...] = jnp.zeros_like(sum_c)

    rate = rate_ref[...]

    @pl.when(g == 0)
    def _():
        h = h_in_ref[...]
        c = c_in_ref[...]
        order = [(a, s) for a in range(groups) for s in range(SEGS)]
        for a, s in order:
            at = pl.ds(a * N * SEGS + s, N, stride=SEGS)
            spent = seg_s_ref[a * SEGS + s : a * SEGS + s + 1, :]
            enter_h.at[j][at, :] = h
            h = jnp.exp2(rate * spent) * h + seg_h_ref[at, :]
        for a, s in order[::-1]:
            at = pl.ds(a * N * SEGS + s, N, stride=SEGS)
            spent = seg_s_ref[a * SEGS + s : a * SEGS + s + 1, :]
            enter_c.at[j][at, :] = c
            c = jnp.exp2(rate * spent) * c + seg_c_ref[at, :]

    act_s[...] = act_ref[...].astype(F32)
    silu_rows(d_gated_ref, gate_ref, dy_s)
    first = g * N * SEGS

    def rate_row(n):
        return jnp.broadcast_to(rate_ref[n : n + 1, :], (SEGS, LANES))

    def ahead(i, state):
        state = list(state)
        at = pl.ds(i, SEGS, stride=steps)
        step, act, dy = step_ref[at, :], act_s[at, :], dy_s[at, :]
        gone = step + keep_s[i]
        push = step * act
        y = jnp.zeros((SEGS, LANES), F32)
        for n in range(N):
            decay = jnp.exp2(gone * rate_row(n))
            prior = decay * state[n]
            state[n] = prior + push * bc_s[i, n]
            decay_s[i, n] = decay
            prior_s[i, n] = prior
            y = y + state[n] * bc_s[i, N + n]
            sum_c[i, n] += state[n] * dy
        y_s[at, :] = y
        return tuple(state)

    def enter(ref, n):
        return ref[j, pl.ds(pl.multiple_of(first + n * SEGS, SEGS), SEGS), :]

    lax.fori_loop(0, steps, ahead, tuple(enter(enter_h, n) for n in range(N)), unroll=8)

    def back(k, carry):
        i = steps - 1 - k
        carried, d_rate = list(carry[0]), list(carry[1])
        at = pl.ds(i, SEGS, stride=steps)
        step, act, dy = step_ref[at, :], act_s[at, :], dy_s[at, :]
        push = step * act
        along = jnp.zeros((SEGS, LANES), F32)
        d_step = jnp.zeros((SEGS, LANES), F32)
        for n in range(N):
            grad = dy * bc_s[i, N + n] + carried[n]
            along = along + grad * bc_s[i, n]
            log_grad = grad * prior_s[i, n]
            d_step = d_step + log_grad * rate_row(n)
            d_rate[n] = d_rate[n] + log_grad * step
            carried[n] = grad * decay_s[i, n]
            sum_b[i, n] += grad * push
        d_step_s[at, :] = d_step * LN2 + along * act
        d_act_s[at, :] = along * step
        return (tuple(carried), tuple(d_rate))

    zero = jnp.zeros((SEGS, LANES), F32)
    _, d_rate = lax.fori_loop(
        0, steps, back, (tuple(enter(enter_c, n) for n in range(N)), (zero,) * N), unroll=8
    )
    for n in range(N):
        d_rate_ref[0, n : n + 1, :] = jnp.sum(d_rate[n], axis=0, keepdims=True)

    strip = 64

    def close(r, sums):
        at = pl.ds(pl.multiple_of(r * strip, strip), strip)
        gate, d_gated, act, dy = gate_ref[at, :], d_gated_ref[at, :], act_s[at, :], dy_s[at, :]
        skip = skip_ref[...]
        sig = jax.nn.sigmoid(gate)
        scan_out = y_s[at, :] + skip * act
        gated = scan_out * gate * sig
        y_s[at, :] = gated
        gated_ref[at, :] = gated.astype(BF16)
        d_gate_ref[at, :] = (d_gated * scan_out * sig * (1.0 + gate * (1.0 - sig))).astype(BF16)
        d_pre = (d_step_s[at, :] * jax.nn.sigmoid(pre_ref[at, :])).astype(BF16)
        d_pre_ref[at, :] = d_pre
        drive_ref[at, :] = d_act_s[at, :] + dy * skip

        def fold(value):
            return jnp.sum(value.reshape(strip // SEGS, SEGS, LANES), axis=0)

        return sums[0] + fold(dy * act), sums[1] + fold(d_pre.astype(F32))

    g_skip, g_bias = lax.fori_loop(0, y_s.shape[0] // strip, close, (zero, zero))
    d_rate_ref[0, N : N + 1, :] = jnp.sum(g_skip, axis=0, keepdims=True)
    d_rate_ref[0, N + 1 : N + 2, :] = jnp.sum(g_bias, axis=0, keepdims=True)
    gated_t_ref[...] = y_s[...].T.astype(BF16)

    @pl.when(j == blocks - 1)
    def _():
        column = lax.broadcasted_iota(jnp.int32, (2 * LANES, LANES), 1)
        total = jnp.zeros((steps * SEGS, LANES), F32)
        for n in range(N):
            for ref, at in ((sum_b, n), (sum_c, N + n)):
                pick = (column == at).astype(F32).astype(BF16)
                value = exact_parts(ref[:, n].reshape(steps * SEGS, LANES))
                total = total + jnp.dot(
                    jnp.concatenate(value[:2], axis=1), pick, preferred_element_type=F32
                )
        act_s[...] = total

        def put(i, _):
            d_bc_ref[pl.ds(i, SEGS, stride=steps), :] = act_s[
                pl.ds(pl.multiple_of(i * SEGS, SEGS), SEGS), :
            ]
            return 0

        lax.fori_loop(0, steps, put, 0, unroll=8)


def scan_totals(step_size, activated, d_gated, gate_z, rate2, table, groups):
    length, channels = step_size.shape
    steps = length // (groups * SEGS)
    blocks = channels // LANES
    tall = pl.BlockSpec((length, LANES), lambda j: (0, j))
    rows = groups * N * SEGS
    return pl.pallas_call(
        lambda *refs: totals_kernel(groups, steps, *refs),
        grid=(blocks,),
        in_specs=[
            tall,
            tall,
            tall,
            tall,
            pl.BlockSpec((N, LANES), lambda j: (0, j)),
            pl.BlockSpec((length, LANES), lambda j: (0, 0)),
        ],
        out_specs=[
            pl.BlockSpec((groups * SEGS, LANES), lambda j: (0, j)),
            pl.BlockSpec((rows, LANES), lambda j: (0, j)),
            pl.BlockSpec((rows, LANES), lambda j: (0, j)),
            pl.BlockSpec((2 * N + SEGS, LANES), lambda j: (0, j)),
        ],
        out_shape=[
            jax.ShapeDtypeStruct((groups * SEGS, channels), F32),
            jax.ShapeDtypeStruct((rows, channels), F32),
            jax.ShapeDtypeStruct((rows, channels), F32),
            jax.ShapeDtypeStruct((2 * N + SEGS, channels), F32),
        ],
        scratch_shapes=[
            pltpu.VMEM((groups * steps, 2 * N, SEGS, LANES), F32),
            pltpu.VMEM((groups * steps, SEGS, LANES), F32),
            pltpu.VMEM((length, LANES), F32),
            pltpu.VMEM((length, LANES), F32),
        ],
        compiler_params=pltpu.CompilerParams(
            dimension_semantics=("arbitrary",), vmem_limit_bytes=40 << 20
        ),
        cost_estimate=pl.CostEstimate(
            flops=length * channels * N * 3000,
            bytes_accessed=length * channels * 14,
            transcendentals=length * channels * N,
        ),
        name="scan_totals",
    )(step_size, activated, d_gated, gate_z, rate2, table)


def scan_grads(
    step_size, step_pre, activated, d_gated, gate_z, skip, rate2, table, segs, enter, groups
):
    length, channels = step_size.shape
    steps = length // (groups * SEGS)
    blocks = channels // LANES
    share = length // groups
    tall = pl.BlockSpec((share, LANES), lambda g, j: (g, j))
    one = pl.BlockSpec((share, LANES), lambda g, j: (g, 0))
    rows = groups * N * SEGS

    def wide(height):
        return pl.BlockSpec((height, LANES), lambda g, j: (0, j))

    def shape(dtype, *dims):
        return jax.ShapeDtypeStruct(dims, dtype)

    grid_spec = pl.GridSpec(
        grid=(groups, blocks),
        in_specs=[tall] * 5
        + [wide(1), wide(N), one]
        + [wide(groups * SEGS), wide(rows), wide(rows), wide(N), wide(N)],
        out_specs=[pl.BlockSpec((LANES, share), lambda g, j: (j, g))]
        + [tall] * 4
        + [pl.BlockSpec((1, 3 * SEGS, LANES), lambda g, j: (g, 0, j)), one],
        scratch_shapes=[
            pltpu.VMEM((steps, 2 * N, SEGS, LANES), F32),
            pltpu.VMEM((steps, SEGS, LANES), F32),
            pltpu.VMEM((share, LANES), F32),
            pltpu.VMEM((blocks, rows, LANES), F32),
            pltpu.VMEM((blocks, rows, LANES), F32),
            pltpu.VMEM((steps, N, SEGS, LANES), F32),
            pltpu.VMEM((steps, N, SEGS, LANES), F32),
            pltpu.VMEM((steps, N, SEGS, LANES), F32),
            pltpu.VMEM((steps, N, SEGS, LANES), F32),
            pltpu.VMEM((share, LANES), F32),
            pltpu.VMEM((share, LANES), F32),
            pltpu.VMEM((share, LANES), F32),
            pltpu.VMEM((share, LANES), F32),
        ],
    )
    return pl.pallas_call(
        lambda *refs: grads_kernel(groups, steps, blocks, *refs),
        grid_spec=grid_spec,
        out_shape=[
            shape(BF16, channels, length),
            shape(BF16, length, channels),
            shape(BF16, length, channels),
            shape(BF16, length, channels),
            shape(F32, length, channels),
            shape(F32, groups, 3 * SEGS, channels),
            shape(F32, length, LANES),
        ],
        compiler_params=pltpu.CompilerParams(
            dimension_semantics=("arbitrary", "arbitrary"), vmem_limit_bytes=48 << 20
        ),
        cost_estimate=pl.CostEstimate(
            flops=length * channels * N * 6000,
            bytes_accessed=length * channels * 30,
            transcendentals=length * channels * N,
        ),
        name="scan_grads",
    )(step_size, step_pre, activated, d_gated, gate_z, skip, rate2, table, *segs, *enter)


MESH = pl.DeviceIdType.MESH
CHUNK = 128
AHEAD = 2
LATE = 2
WIDE = 256


def finish_kernel(
    parts,
    gated_t_hbm,
    gated_hbm,
    normed_hbm,
    d_gate_hbm,
    d_pre_hbm,
    drive_hbm,
    inner_hbm,
    halo_hbm,
    w_inx_hbm,
    w_inz_hbm,
    w_out_hbm,
    x_hbm,
    dy_hbm,
    rms_ref,
    gain_ref,
    masks_ref,
    taps_ref,
    w_step_ref,
    w_proj_ref,
    d_bc_ref,
    misc_ref,
    g_step_ref,
    sums_out,
    sums_z,
    sums_x,
    small_ref,
    out_hbm,
    grad_hbm,
    left,
    right,
    w_x,
    w_z,
    x_cols,
    y_out,
    y_in,
    a_in,
    b_in,
    line,
    first,
    held,
    total,
    core_out,
    core_in,
    kept,
    x_out,
    x_in,
    rows_x,
    rows_dy,
    final,
    passed,
    gain_sum,
    gain_core,
    gain_x,
    gain_out,
    s_out,
    s_in,
    s_a,
    s_b,
    s_line,
    p_out,
    p_in,
    q_out,
    q_in,
    turned_p,
    drive,
    inner_low,
    inner,
    active,
    pack,
    tail,
    halo_out,
    halo_in,
    load_sem,
    w_sem,
    y_sem,
    a_sem,
    b_sem,
    c_sem,
    out_sem,
    tp_sem,
    gain_sem,
    final_sem,
    small_sem,
    chain_sem,
    proj_sem,
    halo_sem,
):
    rows, width = x_hbm.shape
    half = width // 2
    dp, z, tp = lax.axis_index("dp"), lax.axis_index("ctx"), lax.axis_index("tp")
    core, x_bit = tp % 2, tp // 2
    near, across = tp + 1 - 2 * core, (tp + 2) % 4
    ends = (z == 0) | (z == 3)
    middle = (z == 1) | (z == 2)
    inward, twin, outward = z // 2 + 1, 3 - z, (z // 2) * 3

    def load(source, target, at):
        copy = pltpu.make_async_copy(source, target, load_sem.at[at])
        copy.start()
        return copy

    quarter = rows // 4
    own_row = pl.multiple_of(core * (rows // 2) + x_bit * quarter, quarter)
    got_left = load(gated_t_hbm, left.at[0], 1)
    mine = pl.multiple_of(dp * half, half)
    away = pl.multiple_of((1 - dp) * half, half)
    got_other = load(dy_hbm.at[:, pl.ds(away, half)], right.at[1], 2)
    got_pre = load(d_pre_hbm, right.at[3], 0)
    others = [
        load(dy_hbm.at[:, pl.ds(mine, half)], right.at[0], 3),
        load(normed_hbm.at[pl.ds(0, half), :], left.at[1], 4),
        load(normed_hbm.at[pl.ds(half, half), :], left.at[2], 5),
        load(d_gate_hbm, right.at[2], 6),
        load(x_hbm.at[pl.ds(own_row, quarter), pl.ds(mine, half)], rows_x.at[:, pl.ds(0, half)], 7),
        load(dy_hbm.at[pl.ds(own_row, quarter), pl.ds(mine, half)], rows_dy.at[:, pl.ds(0, half)], 8),
        load(
            x_hbm.at[pl.ds(own_row, quarter), pl.ds(away, half)],
            rows_x.at[:, pl.ds(half, half)],
            16,
        ),
        load(
            dy_hbm.at[pl.ds(own_row, quarter), pl.ds(away, half)],
            rows_dy.at[:, pl.ds(half, half)],
            17,
        ),
    ]

    barrier = pltpu.get_barrier_semaphore()
    for peer in ({"tp": near}, {"tp": across}, {"dp": 1 - dp}):
        pl.semaphore_signal(barrier, inc=1, device_id=peer, device_id_type=MESH)

    @pl.when(ends)
    def _():
        pl.semaphore_signal(barrier, inc=1, device_id={"ctx": inward}, device_id_type=MESH)
        pl.semaphore_wait(barrier, 4)

    @pl.when(middle)
    def _():
        pl.semaphore_signal(barrier, inc=1, device_id={"ctx": twin}, device_id_type=MESH)
        pl.semaphore_signal(barrier, inc=1, device_id={"ctx": outward}, device_id_type=MESH)
        pl.semaphore_wait(barrier, 5)

    def remote(source, target, sems, at, peer):
        return pltpu.make_async_remote_copy(
            src_ref=source,
            dst_ref=target,
            send_sem=sems.at[0, at],
            recv_sem=sems.at[1, at],
            device_id=peer,
            device_id_type=MESH,
        )

    per_weight, pairs = parts // 3, parts // 2

    def chunk(k):
        return k // per_weight, pl.multiple_of(k % per_weight * CHUNK, CHUNK)

    def product(slot_l, slot_r, column):
        return jnp.dot(
            left[slot_l], right[slot_r, :, pl.ds(column, 2 * CHUNK)], preferred_element_type=F32
        )

    def y_copy(k):
        return remote(y_out.at[k % 6], y_in.at[k % 8], y_sem, k, {"dp": 1 - dp})

    def a_copy(k):
        return remote(line.at[k % 4], a_in.at[k % 12], a_sem, k, {"ctx": inward})

    def b_copy(k):
        return remote(line.at[k % 4], b_in.at[k % 4], b_sem, k, {"ctx": twin})

    sums = (sums_out, sums_z, sums_x)

    def far_copy(k, ref):
        spot = ref.at[:, pl.ds(chunk(k)[1], CHUNK)]
        return remote(total.at[k % 4], spot, c_sem, k, {"ctx": outward})

    def own_copy(k, ref):
        spot = ref.at[:, pl.ds(chunk(k)[1], CHUNK)]
        return pltpu.make_async_copy(total.at[k % 4], spot, out_sem.at[k])

    def give_c(k, start):
        for w, ref in enumerate(sums):

            @pl.when(k // per_weight == w)
            def _():
                far, own = far_copy(k, ref), own_copy(k, ref)
                if start:
                    far.start()
                    own.start()
                else:
                    far.wait_send()
                    own.wait()

    def wait_c(k):
        far_copy(k, sums_out).wait_recv()

    def pair(p):
        w, column = chunk(2 * p)
        return w, pl.multiple_of(column, 2 * CHUNK)

    def send_y(k):
        @pl.when(k % 2 == 0)
        def _():
            w, column = pair(k // 2)
            up = (w + 1) // 2

            @pl.when(k >= 6)
            def _():
                y_copy(k - 6).wait_send()
                y_copy(k - 5).wait_send()

            value = product(2 * up, w + 1, column).astype(BF16)
            y_out[k % 6] = value[:, :CHUNK]
            y_out[(k + 1) % 6] = value[:, CHUNK:]

        y_copy(k).start()

    def take_y(k):
        @pl.when(k % 2 == 0)
        def _():
            w, column = pair(k // 2)
            up = (w + 1) // 2
            value = product(up, w + up, column)
            held[0] = value[:, :CHUNK]
            held[1] = value[:, CHUNK:]

        y_copy(k).wait_recv()
        value = held[k % 2] + y_in[k % 8].astype(F32)

        @pl.when(ends)
        def _():
            @pl.when(k >= 4)
            def _():
                a_copy(k - 4).wait_send()

            @pl.when(k >= 12)
            def _():
                wait_c(k - 12)

            line[k % 4] = value.astype(BF16)
            a_copy(k).start()

        @pl.when(middle)
        def _():
            first[k % 2] = value

    def take_a(k):
        @pl.when(middle)
        def _():
            @pl.when(k >= 4)
            def _():
                b_copy(k - 4).wait_send()

            a_copy(k).wait_recv()
            line[k % 4] = (first[k % 2] + a_in[k % 12].astype(F32)).astype(BF16)
            b_copy(k).start()

    def take_b(k):
        @pl.when(middle)
        def _():
            @pl.when(k >= 4)
            def _():
                give_c(k - 4, False)

            b_copy(k).wait_recv()
            total[k % 4] = (line[k % 4].astype(F32) + b_in[k % 4].astype(F32)).astype(BF16)
            give_c(k, True)

    def tick(k, _):
        @pl.when((k >= 2 * LATE) & (k < parts + 2 * LATE))
        def _():
            take_b(k - 2 * LATE)

        @pl.when((k >= LATE) & (k < parts + LATE))
        def _():
            take_a(k - LATE)

        @pl.when(k < parts)
        def _():
            take_y(k)

        @pl.when(k + AHEAD < parts)
        def _():
            send_y(k + AHEAD)

        return 0

    def ticks(begin, end):
        lax.fori_loop(begin, end, tick, 0)

    got_left.wait()
    got_other.wait()
    for k in range(AHEAD):
        send_y(jnp.int32(k))
    got_pre.wait()
    p_out[:, :LANES] = contract_last(right[3], w_step_ref[...]).astype(BF16)
    p_out[:, LANES:] = d_bc_ref[...].astype(BF16)
    p_copy = remote(p_out, p_in, proj_sem, 0, {"tp": near})
    p_copy.start()
    got_gated = load(gated_hbm, right.at[3], 0)
    p_copy.wait_recv()
    q_out[...] = (p_out[...].astype(F32) + p_in[...].astype(F32)).astype(BF16)
    q_copy = remote(q_out, q_in, proj_sem, 1, {"tp": across})
    q_copy.start()

    block = w_x.shape[0]
    send_row = pl.multiple_of((1 - core) * (rows // 2), rows // 2)
    keep_row = pl.multiple_of(core * (rows // 2), rows // 2)
    give = pl.multiple_of((1 - x_bit) * quarter, quarter)
    have = pl.multiple_of(x_bit * quarter, quarter)

    got_gated.wait()

    def out_columns(d, _):
        at = pl.multiple_of(d * block, block)
        copy = pltpu.make_async_copy(w_out_hbm.at[:, pl.ds(at, block)], x_cols, w_sem.at[0])
        copy.start()
        copy.wait()
        core_out[:, pl.ds(at, block)] = jnp.dot(
            right[3, pl.ds(send_row, rows // 2), :], x_cols[...], preferred_element_type=F32
        ).astype(BF16)
        kept[:, pl.ds(at, block)] = jnp.dot(
            right[3, pl.ds(keep_row, rows // 2), :], x_cols[...], preferred_element_type=F32
        ).astype(BF16)
        return 0

    lax.fori_loop(0, width // block, out_columns, 0)
    core_copy = remote(core_out, core_in, tp_sem, 0, {"tp": near})
    core_copy.start()

    def chain_loads(q):
        at = pl.ds(q * WIDE, WIDE)
        return (
            pltpu.make_async_copy(
                drive_hbm.at[:, at], drive.at[pl.ds(SEGS, rows), :], chain_sem.at[0]
            ),
            pltpu.make_async_copy(
                inner_hbm.at[:, at], inner_low.at[pl.ds(2 * SEGS, rows), :], chain_sem.at[1]
            ),
            pltpu.make_async_copy(
                halo_hbm.at[:, at], inner_low.at[pl.ds(0, 2 * SEGS), :], chain_sem.at[2]
            ),
        )

    for copy in chain_loads(0):
        copy.start()
    for copy in others:
        copy.wait()

    ticks(0, 2)

    core_copy.wait_recv()

    def to_across():
        x_out[...] = (
            kept[pl.ds(give, quarter), :].astype(F32) + core_in[pl.ds(give, quarter), :].astype(F32)
        ).astype(BF16)

    to_across()
    x_copy = remote(x_out, x_in, tp_sem, 1, {"tp": across})
    x_copy.start()

    q_copy.wait_recv()
    projected = q_out[...].astype(F32) + q_in[...].astype(F32)
    p_copy.wait_send()
    p_out[...] = projected.astype(BF16)
    turned_p[...] = projected.T.astype(BF16)

    zeros = jnp.zeros((SEGS, WIDE), F32)
    strip = 64
    pad = 2 * SEGS
    drive[0:SEGS, :] = zeros
    drive[rows + SEGS :, :] = zeros

    def chain(q):
        cut = slice(q * WIDE, (q + 1) * WIDE)
        for copy in chain_loads(q):
            copy.wait()
        inner[...] = inner_low[...].astype(F32)
        taps = [taps_ref[i : i + 1, cut] for i in range(K + 1)]

        def down(r, sums):
            at = pl.multiple_of(r * strip, strip)
            mask = masks_ref[pl.ds(at + SEGS, strip), :]
            valid = [mask[:, i : i + 1] for i in range(K - 1)]
            near_rows = inner[pl.ds(at, strip + pad), :]
            moved = [near_rows[pad - (K - 1) + i :][:strip] for i in range(K)]
            moved = [moved[i] * valid[i] for i in range(K - 1)] + moved[K - 1 :]
            pre = taps[K] + taps[K - 1] * moved[K - 1]
            for i in range(K - 1):
                pre = pre + taps[i] * moved[i]
            sig = jax.nn.sigmoid(pre)
            active[pl.ds(at, strip), :] = (pre * sig).astype(BF16)
            whole = drive[pl.ds(at + SEGS, strip), :] + contract_last(
                p_out[pl.ds(at, strip), :], w_proj_ref[cut, :]
            )
            grad = whole * sig * (1.0 + pre * (1.0 - sig))
            drive[pl.ds(at + SEGS, strip), :] = grad

            def fold(value):
                return jnp.sum(value.reshape(strip // SEGS, SEGS, WIDE), axis=0)

            terms = [grad * m for m in moved] + [grad]
            return tuple(s + fold(t) for s, t in zip(sums, terms))

        sums_q = lax.fori_loop(0, rows // strip, down, (zeros,) * (K + 1))
        for i in range(K + 1):
            pack[i : i + 1, cut] = jnp.sum(sums_q[i], axis=0, keepdims=True)

        def spread(base, size):
            grads = drive[pl.ds(base + SEGS, size + SEGS), :]
            mask = masks_ref[pl.ds(base + SEGS, size + SEGS), :]
            value = grads[:size] * taps[K - 1]
            for back in range(1, K):
                valid = grads * mask[:, K - 1 - back : K - back]
                value = value + valid[back : back + size] * taps[K - 1 - back]
            return value

        def up(r, _):
            at = pl.multiple_of(r * strip, strip)
            right[3, pl.ds(at, strip), cut] = spread(at, strip).astype(BF16)
            return 0

        lax.fori_loop(0, rows // strip, up, 0)
        tail[:, cut] = spread(rows - pad, pad)
        halo_out[:, cut] = spread(-SEGS, SEGS)
        pack[4 * SEGS : 4 * SEGS + R + 2 * N, cut] = jnp.dot(
            turned_p[...], active[...], preferred_element_type=F32
        )[: R + 2 * N]

    for q in range(rows // WIDE):
        chain(q)
        if q + 1 < rows // WIDE:
            for copy in chain_loads(q + 1):
                copy.start()
            ticks(2 * q + 2, 2 * q + 4)
    halo_copy = remote(halo_out, halo_in, halo_sem, 0, {"ctx": jnp.maximum(z - 1, 0)})

    @pl.when(z > 0)
    def _():
        halo_copy.start()

    ticks(8, 10)

    def gather(ref, source, base):
        copies = []
        for side in range(2):
            place = pl.multiple_of((dp + side - 2 * dp * side) * half, half)
            spot = ref.at[pl.ds(own_row, quarter), pl.ds(place, half)]
            piece = source.at[:, pl.ds(side * half, half)]
            for p, peer in enumerate((across, near)):
                copies.append(remote(piece, spot, final_sem, base + 2 * p + side, {"tp": peer}))
            copies.append(pltpu.make_async_copy(piece, spot, load_sem.at[9 + base // 2 + side]))
        for copy in copies:
            copy.start()
        return copies

    def forward(ref, copies, base):
        copies[0].wait_recv()
        copies[3].wait_recv()
        row = pl.multiple_of(core * (rows // 2) + (1 - x_bit) * quarter, quarter)
        spot = ref.at[pl.ds(row, quarter), :]
        fetch = pltpu.make_async_copy(spot, passed, load_sem.at[15])
        fetch.start()
        fetch.wait()
        copy = remote(passed, spot, final_sem, base + 4, {"tp": near})
        copy.start()
        return copy

    def finished(copies, last):
        for k, copy in enumerate(copies):
            if k in (0, 3):
                copy.wait_send()
            else:
                copy.wait()
        last.wait()

    x_copy.wait_recv()

    def summed_rows():
        return (
            kept[pl.ds(have, quarter), :].astype(F32)
            + core_in[pl.ds(have, quarter), :].astype(F32)
            + x_in[...].astype(F32)
        )

    final[...] = (rows_x[...].astype(F32) + summed_rows()).astype(BF16)
    out_copies = gather(out_hbm, final, 0)

    @pl.when(z < 3)
    def _():
        halo_copy.wait_recv()
        tail[SEGS:, :] = tail[SEGS:, :] + halo_in[...]

    right[3, rows - pad :, :] = tail[...].astype(BF16)

    ticks(10, 12)

    core_copy.wait_send()
    x_copy.wait_send()

    def columns(d, _):
        at = pl.multiple_of(d * block, block)
        copies = [
            pltpu.make_async_copy(w_inx_hbm.at[pl.ds(at, block), :], w_x, w_sem.at[0]),
            pltpu.make_async_copy(w_inz_hbm.at[pl.ds(at, block), :], w_z, w_sem.at[1]),
            pltpu.make_async_copy(
                x_hbm.at[:, pl.ds(pl.multiple_of((at + dp * half) % width, block), block)],
                x_cols,
                w_sem.at[2],
            ),
        ]
        for copy in copies:
            copy.start()
        for copy in copies:
            copy.wait()
        sums_d = jnp.zeros((SEGS, block), F32)
        for row, keep in ((send_row, False), (keep_row, True)):
            span = pl.ds(row, rows // 2)
            value = contract_last(right[3, span, :], w_x[...])
            value = value + contract_last(right[2, span, :], w_z[...])
            hat = x_cols[span, :].astype(F32) * rms_ref[span, :]
            sums_d = sums_d + jnp.sum(
                (value * hat).reshape(rows // 2 // SEGS, SEGS, block), axis=0
            )
            target = kept if keep else core_out
            target[:, pl.ds(at, block)] = value.astype(BF16)
        gain_sum[:, pl.ds(at, block)] = sums_d
        return 0

    for d in range(width // block):
        columns(d, 0)
        ticks(12 + d, 13 + d)
    gain_copy = remote(gain_sum, gain_core, gain_sem, 0, {"tp": near})
    gain_copy.start()
    gain_copy.wait_recv()
    core_again = remote(core_out, core_in, tp_sem, 2, {"tp": near})
    core_again.start()
    gain_out[...] = gain_sum[...] + gain_core[...]
    gain_across = remote(gain_out, gain_x, gain_sem, 1, {"tp": across})
    gain_across.start()

    ticks(16, 17)

    core_again.wait_recv()
    to_across()
    gain_across.wait_recv()
    x_again = remote(x_out, x_in, tp_sem, 3, {"tp": across})
    x_again.start()

    ticks(17, 18)

    both = gain_out[...] + gain_x[...]
    fine = half // 2
    steps_half = g_step_ref.shape[0] // 2
    base = 4 * SEGS + R + 2 * N
    pack[K + 1 : SEGS, :] = jnp.zeros((SEGS - K - 1, 2 * fine), F32)
    pack[SEGS : 4 * SEGS, :] = misc_ref[...]

    def small_rows(index, lanes):
        column = pl.multiple_of(index * fine, fine)
        row = pl.multiple_of(index * steps_half, steps_half)
        return jnp.concatenate(
            [
                pack[:, pl.ds(column, fine)],
                g_step_ref[pl.ds(row, steps_half), :fine],
                g_step_ref[pl.ds(row, steps_half), fine:],
                both[:, lanes : lanes + fine],
                both[:, lanes + fine : lanes + 2 * fine],
            ],
            axis=0,
        )

    s_out[...] = small_rows(1 - dp, half).astype(BF16)
    small_y = remote(s_out, s_in, small_sem, 0, {"dp": 1 - dp})
    small_y.start()
    out_last = forward(out_hbm, out_copies, 0)

    ticks(18, 20)

    x_again.wait_recv()
    r_own = rms_ref[pl.ds(own_row, quarter), :]
    d_normed = summed_rows()
    hat = rows_x[...].astype(F32) * r_own
    d_hat = d_normed * gain_ref[...]
    mean = jnp.sum(d_hat * hat, axis=1, keepdims=True) * (1.0 / width)
    rows_dy[...] = (rows_dy[...].astype(F32) + r_own * (d_hat - hat * mean)).astype(BF16)
    grad_copies = gather(grad_hbm, rows_dy, 6)

    ticks(20, 21)

    small_y.wait_recv()
    s_keep = small_rows(dp, 0) + s_in[...].astype(F32)
    small_a = remote(s_line, s_a, small_sem, 1, {"ctx": inward})
    small_b = remote(s_line, s_b, small_sem, 2, {"ctx": twin})
    small_c = remote(small_ref, small_ref, small_sem, 3, {"ctx": outward})

    @pl.when(ends)
    def _():
        s_line[...] = s_keep.astype(BF16)
        small_a.start()

    @pl.when(middle)
    def _():
        small_a.wait_recv()
        s_line[...] = (s_keep + s_a[...].astype(F32)).astype(BF16)
        small_b.start()

    ticks(21, 22)

    finished(out_copies, out_last)
    grad_last = forward(grad_hbm, grad_copies, 6)

    @pl.when(middle)
    def _():
        small_b.wait_recv()
        small_ref[...] = (s_line[...].astype(F32) + s_b[...].astype(F32)).astype(BF16)
        small_c.start()

    ticks(22, parts + 2 * LATE)

    for k in range(parts - 6, parts):
        y_copy(k).wait_send()

    @pl.when(ends)
    def _():
        for k in range(parts - 4, parts):
            a_copy(k).wait_send()
        for k in range(parts - 12, parts):
            wait_c(k)
        small_a.wait_send()
        small_c.wait_recv()

    @pl.when(middle)
    def _():
        for k in range(parts - 4, parts):
            b_copy(k).wait_send()
            far_copy(k, sums_x).wait_send()
            own_copy(k, sums_x).wait()
        small_b.wait_send()
        small_c.wait_send()

    @pl.when(z > 0)
    def _():
        halo_copy.wait_send()

    q_copy.wait_send()
    core_again.wait_send()
    x_again.wait_send()
    gain_copy.wait_send()
    gain_across.wait_send()
    small_y.wait_send()
    finished(grad_copies, grad_last)


def finish(
    gated_t, gated, normed_t, d_gate, d_pre, drive, inner, halo, w_inx, w_inz, w_out, x_all, dy_all,
    rms, gain, masks, taps, w_step, w_proj, d_bc, misc, g_step,
):
    rows, width = x_all.shape
    channels = w_inx.shape[1]
    parts = 3 * (channels // CHUNK)
    half = width // 2
    small = 4 * SEGS + R + 2 * N + g_step.shape[0] + 2 * SEGS
    fine = half // 2
    block = 512
    hbm = pl.BlockSpec(memory_space=pl.ANY)
    vmem = pl.BlockSpec(memory_space=pltpu.VMEM)
    dma = pltpu.SemaphoreType.DMA
    piece = (half, CHUNK)
    quarter = rows // 4

    def low(*shape):
        return pltpu.VMEM(shape, BF16)

    def full(*shape):
        return pltpu.VMEM(shape, F32)

    return pl.pallas_call(
        lambda *refs: finish_kernel(parts, *refs),
        in_specs=[hbm] * 13 + [vmem] * 9,
        out_specs=[hbm, hbm, hbm, vmem, hbm, hbm],
        out_shape=[jax.ShapeDtypeStruct((half, channels), BF16)] * 3
        + [
            jax.ShapeDtypeStruct((small, fine), BF16),
            jax.ShapeDtypeStruct((rows, width), BF16),
            jax.ShapeDtypeStruct((rows, width), BF16),
        ],
        scratch_shapes=[
            low(3, half, rows),
            low(4, rows, channels),
            low(block, channels),
            low(block, channels),
            low(rows, block),
            low(6, *piece),
            low(8, *piece),
            low(12, *piece),
            low(4, *piece),
            low(4, *piece),
            full(2, *piece),
            full(2, *piece),
            low(4, *piece),
            low(rows // 2, width),
            low(rows // 2, width),
            low(rows // 2, width),
            low(quarter, width),
            low(quarter, width),
            low(quarter, width),
            low(quarter, width),
            low(quarter, width),
            low(quarter, width),
            full(SEGS, width),
            full(SEGS, width),
            full(SEGS, width),
            full(SEGS, width),
            low(small, fine),
            low(small, fine),
            low(small, fine),
            low(small, fine),
            low(small, fine),
            low(rows, 2 * LANES),
            low(rows, 2 * LANES),
            low(rows, 2 * LANES),
            low(rows, 2 * LANES),
            low(2 * LANES, rows),
            full(rows + 2 * SEGS, WIDE),
            low(rows + 2 * SEGS, WIDE),
            full(rows + 2 * SEGS, WIDE),
            low(rows, WIDE),
            full(4 * SEGS + R + 2 * N, channels),
            full(2 * SEGS, channels),
            full(SEGS, channels),
            full(SEGS, channels),
            dma((18,)),
            dma((3,)),
            dma((2, parts)),
            dma((2, parts)),
            dma((2, parts)),
            dma((2, parts)),
            dma((parts,)),
            dma((2, 4)),
            dma((2, 2)),
            dma((2, 11)),
            dma((2, 4)),
            dma((3,)),
            dma((2, 2)),
            dma((2, 1)),
        ],
        compiler_params=pltpu.CompilerParams(
            collective_id=0, has_side_effects=True, vmem_limit_bytes=63900 << 10
        ),
        cost_estimate=pl.CostEstimate(
            flops=200_000_000_000, bytes_accessed=60_000_000, transcendentals=0
        ),
        name="finish",
    )(
        gated_t, gated, normed_t, d_gate, d_pre, drive, inner, halo, w_inx, w_inz, w_out, x_all, dy_all,
        rms, gain, masks, taps, w_step, w_proj, d_bc, misc, g_step,
    )


def swap_pairs(value, axis, distance):
    count = lax.axis_size(axis)
    return lax.ppermute(value, axis, [(i, i ^ distance) for i in range(count)])


def ordered(mine, other, bit, axis=0):
    return jnp.where(
        bit == 0,
        jnp.concatenate([mine, other], axis=axis),
        jnp.concatenate([other, mine], axis=axis),
    )


def half_of(value, index, axis=0):
    size = value.shape[axis] // 2
    return lax.dynamic_slice_in_dim(value, index * size, size, axis)


def tp_sum(value):
    distance = 1
    while distance < lax.axis_size("tp"):
        value = value + swap_pairs(value, "tp", distance)
        distance *= 2
    return value


def tp_scatter(value):
    index, distance = lax.axis_index("tp"), 1
    while distance < lax.axis_size("tp"):
        mine = (index // distance) % 2
        got = swap_pairs(half_of(value, 1 - mine).astype(BF16), "tp", distance)
        value = half_of(value, mine).astype(F32) + got.astype(F32)
        distance *= 2
    return value


def tp_rows():
    index, distance, at, size = lax.axis_index("tp"), 1, 0, lax.axis_size("tp")
    while distance < lax.axis_size("tp"):
        size //= 2
        at = at + (index // distance) % 2 * size
        distance *= 2
    return at


def per_device(
    hidden_in,
    seq_lengths,
    pack_order,
    norm_gain,
    in_x_weight,
    in_z_weight,
    conv_weight,
    conv_bias,
    x_weight,
    dt_weight,
    dt_bias,
    a_log,
    skip_weight,
    out_weight,
    out_grad,
):
    length, width = hidden_in.shape
    channels = in_x_weight.shape[1]
    tp_count, dp_count, ctx_count = (lax.axis_size(a) for a in ("tp", "dp", "ctx"))
    dp_index, ctx_index, tp_index = (lax.axis_index(a) for a in ("dp", "ctx", "tp"))
    paired = dp_count == 2
    half = width // dp_count
    groups = 2
    fused = paired and ctx_count == 4 and tp_count == 4 and half == channels == length

    def turned(value, axis):
        if not paired:
            return value
        return jnp.concatenate(
            [half_of(value, dp_index, axis), half_of(value, 1 - dp_index, axis)], axis=axis
        )

    def joined(value, axis):
        if not paired:
            return lax.all_gather(value, "dp", axis=axis, tiled=True)
        other = swap_pairs(value, "dp", 1)
        return jnp.where(
            dp_index == 0,
            jnp.concatenate([value, other], axis=axis),
            jnp.concatenate([other, value], axis=axis),
        )

    def weight(own, axis, after):
        if not paired:
            return lax.all_gather(own, "dp", axis=axis, tiled=True), None
        bit = ctx_index % 2
        piece = half_of(own, bit)
        if after is not None:
            piece, _ = lax.optimization_barrier((piece, after))
        near = swap_pairs(piece, "dp", 1)
        far = swap_pairs(near, "ctx", 1)
        return jnp.concatenate([own, ordered(near, far, bit)], axis=axis), near

    small = jnp.concatenate(
        [conv_weight, conv_bias[None], dt_bias[None], skip_weight[None], a_log.T], axis=0
    )
    small = joined(small, 1).astype(F32)
    gain_full = joined(norm_gain, 0).astype(F32)
    w_proj = joined(x_weight, 0)
    w_step = joined(dt_weight, 0)
    w_inx, sent = weight(in_x_weight, 0, None)
    w_inz, sent = weight(in_z_weight, 0, sent)
    w_out, sent = weight(out_weight, 1, sent)
    gain_full = turned(gain_full, 0)
    taps_full = small[:K]
    conv_shift, step_bias, skip_full = small[K], small[K + 1], small[K + 2]
    decay_rate = -jnp.exp(small[K + 3 :])

    starts = piece_starts(seq_lengths[0], pack_order[0])
    positions = ctx_index * length + jnp.arange(length, dtype=jnp.int32)

    def piece(at):
        return jnp.sum((at[:, None] >= starts[None, :]).astype(jnp.int32), axis=1)

    piece_now = piece(positions)
    masks = [(piece(positions - back) == piece_now).astype(F32) for back in (3, 2, 1)]
    blocked = (1.0 - masks[2]) * FAR

    rows_all = turned(hidden_in, 1)
    grad_all = turned(out_grad, 1)
    rows_in = rows_all.astype(F32)
    inv_rms = lax.rsqrt(jnp.mean(rows_in * rows_in, axis=1, keepdims=True) + EPSILON)
    normed = (rows_in * inv_rms * gain_full).astype(BF16)
    inner_x = jnp.dot(normed, w_inx, preferred_element_type=F32).astype(BF16)
    halo = shifted(inner_x[length - (K - 1) :], "ctx", 1)
    extended = jnp.concatenate([halo, inner_x], axis=0).astype(F32)
    conv_pre = conv_shift[None, :] + taps_full[K - 1] * extended[K - 1 :]
    for tap in range(K - 1):
        conv_pre = conv_pre + taps_full[tap] * extended[tap : tap + length] * masks[tap][:, None]
    activated = jax.nn.silu(conv_pre).astype(BF16)
    projected = tp_sum(jnp.dot(activated, w_proj, preferred_element_type=F32))
    gate_z = jnp.dot(normed, w_inz, preferred_element_type=F32)
    d_gated = contract_last(grad_all, w_out)

    step_low = projected[:, :R].astype(BF16)
    step_pre = jnp.dot(step_low, w_step, preferred_element_type=F32) + step_bias
    step_size = jax.nn.softplus(step_pre)
    table = jnp.concatenate(
        [
            projected[:, R:],
            blocked[:, None],
            jnp.zeros((length, LANES - 2 * N - 1), F32),
        ],
        axis=1,
    )
    rate2 = decay_rate * LOG2E

    def entering(whole, rate):
        state, back, spent = whole[:N], whole[N : 2 * N], whole[2 * N : 2 * N + 1]
        h_in = jnp.zeros_like(state)
        c_in = jnp.zeros_like(back)
        below = jnp.zeros_like(spent)
        above = jnp.zeros_like(spent)
        distance = 1
        while distance < ctx_count:
            got = swap_pairs(jnp.concatenate([state, back, jnp.broadcast_to(spent, (8,) + spent.shape[1:])], axis=0), "ctx", distance)
            o_state, o_back, o_spent = got[:N], got[N : 2 * N], got[2 * N : 2 * N + 1]
            upper = (ctx_index // distance) % 2 == 1
            h_in = jnp.where(upper, jnp.exp2(rate * below) * o_state + h_in, h_in)
            c_in = jnp.where(upper, c_in, jnp.exp2(rate * above) * o_back + c_in)
            below = jnp.where(upper, below + o_spent, below)
            above = jnp.where(upper, above, above + o_spent)
            mine, other = jnp.exp2(rate * spent), jnp.exp2(rate * o_spent)
            state, back = (
                jnp.where(upper, mine * o_state + state, other * state + o_state),
                jnp.where(upper, o_back + other * back, back + mine * o_back),
            )
            spent = spent + o_spent
            distance *= 2
        return h_in, c_in

    *segs, whole = scan_totals(step_size, activated, d_gated, gate_z, rate2, table, groups)
    gated_t, gated, d_gate, d_pre, d_drive, rates_d, d_bc = scan_grads(
        step_size,
        step_pre,
        activated,
        d_gated,
        gate_z,
        skip_full[None],
        rate2,
        table,
        segs,
        entering(whole, rate2),
        groups,
    )
    rates_d = jnp.sum(rates_d, axis=0)
    g_log, g_skip, g_bias = rates_d[:N] * decay_rate, rates_d[N], rates_d[N + 1]
    g_step = contract_first(step_low, d_pre)

    def input_sum(cotangent):
        value = contract_first(normed, cotangent)
        if paired:
            value = turned(value, 0)
        value = lax.psum_scatter(value.astype(BF16), "dp", scatter_dimension=0, tiled=True)
        return lax.psum(value, "ctx").astype(F32)

    def output_sum(gated):
        value = contract_first(gated, grad_all)
        if paired:
            value = turned(value, 1)
        value = lax.psum_scatter(value.astype(BF16), "dp", scatter_dimension=1, tiled=True)
        return lax.psum(value, "ctx").astype(F32)

    if fused:
        padded = jnp.pad(jnp.stack(masks, axis=1), ((SEGS, SEGS), (0, 1)))
        before = jnp.pad(halo, ((2 * SEGS - (K - 1), 0), (0, 0)))
        taps = jnp.pad(jnp.concatenate([taps_full, conv_shift[None]]), ((0, SEGS - K - 1), (0, 0)))
        misc = jnp.pad(
            jnp.concatenate([g_bias[None], g_skip[None], g_log]), ((0, 3 * SEGS - N - 2), (0, 0))
        )
        s_out, s_z, s_x, small_sum, out_natural, grad_natural = finish(
            gated_t,
            gated,
            normed.T,
            d_gate,
            d_pre,
            d_drive,
            inner_x,
            before,
            w_inx,
            w_inz,
            w_out,
            hidden_in,
            out_grad,
            inv_rms,
            gain_full[None],
            padded,
            taps,
            w_step,
            jnp.pad(w_proj, ((0, 0), (0, 2 * LANES - R - 2 * N))),
            d_bc,
            misc,
            g_step,
        )
        small_sum = small_sum.astype(F32)
        steps_half = g_step.shape[0] // 2
        at = 4 * SEGS + R + 2 * N
        end = at + 2 * steps_half
        return (
            out_natural,
            grad_natural,
            jnp.concatenate(
                [
                    jnp.sum(small_sum[end : end + SEGS], axis=0),
                    jnp.sum(small_sum[end + SEGS :], axis=0),
                ]
            ),
            s_x.astype(F32),
            s_z.astype(F32),
            small_sum[:K],
            small_sum[K],
            small_sum[4 * SEGS : at].T,
            jnp.concatenate(
                [small_sum[at : at + steps_half], small_sum[at + steps_half : end]], axis=1
            ),
            small_sum[SEGS],
            small_sum[SEGS + 2 : SEGS + 2 + N].T,
            small_sum[SEGS + 1],
            s_out.astype(F32),
        )

    branch = jnp.dot(gated, w_out, preferred_element_type=F32)
    d_proj = tp_sum(
        jnp.concatenate([contract_last(d_pre, w_step), d_bc[:, : 2 * N]], axis=1)
    ).astype(BF16)

    quarter = length // tp_count
    own_row = tp_rows() * quarter
    own_in = lax.dynamic_slice_in_dim(rows_all, own_row, quarter, 0).astype(F32)
    own_grad = lax.dynamic_slice_in_dim(grad_all, own_row, quarter, 0).astype(F32)
    own_rms = lax.rsqrt(jnp.mean(own_in * own_in, axis=1, keepdims=True) + EPSILON)
    own_hat = own_in * own_rms

    def whole_rows(value):
        distance = tp_count // 2
        while distance >= 1:
            value = ordered(value, swap_pairs(value, "tp", distance), (tp_index // distance) % 2)
            distance //= 2
        if not paired:
            return value
        return ordered(value[:, :half], value[:, half:], dp_index, axis=1)

    out_natural = whole_rows((own_in + tp_scatter(branch)).astype(BF16))

    g_proj = contract_first(d_proj, activated)
    d_total = d_drive + contract_last(d_proj, w_proj)
    conv_sig = jax.nn.sigmoid(conv_pre)
    d_conv = d_total * conv_sig * (1.0 + conv_pre * (1.0 - conv_sig))
    g_shift = jnp.sum(d_conv, axis=0)
    g_taps = jnp.stack(
        [
            jnp.sum(d_conv * masks[tap][:, None] * extended[tap : tap + length], axis=0)
            for tap in range(K - 1)
        ]
        + [jnp.sum(d_conv * extended[K - 1 :], axis=0)],
        axis=0,
    )
    d_extended = jnp.pad(d_conv * taps_full[K - 1], ((K - 1, 0), (0, 0)))
    for tap in range(K - 1):
        d_extended = d_extended + jnp.pad(
            d_conv * masks[tap][:, None] * taps_full[tap], ((tap, K - 1 - tap), (0, 0))
        )
    returned = shifted(d_extended[: K - 1], "ctx", -1)
    d_inner = (
        d_extended[K - 1 :] + jnp.pad(returned, ((length - (K - 1), 0), (0, 0)))
    ).astype(BF16)
    packed = jnp.concatenate(
        [g_taps, g_shift[None], g_bias[None], g_skip[None], g_log, g_proj], axis=0
    )
    g_inx, g_inz, g_out = input_sum(d_inner), input_sum(d_gate), output_sum(gated)
    d_normed = tp_scatter(contract_last(d_inner, w_inx) + contract_last(d_gate, w_inz))
    g_gain = jnp.sum(d_normed * own_hat, axis=0)
    d_hat = d_normed * gain_full
    d_rows = own_grad + own_rms * (
        d_hat - own_hat * jnp.mean(d_hat * own_hat, axis=1, keepdims=True)
    )
    grad_natural = whole_rows(d_rows.astype(BF16))
    g_gain = turned(lax.psum(g_gain, ("ctx", "tp")), 0)
    g_gain = lax.psum_scatter(g_gain, "dp", scatter_dimension=0, tiled=True)
    packed = lax.psum(lax.psum_scatter(packed, "dp", scatter_dimension=1, tiled=True), "ctx")
    g_step = lax.psum(lax.psum_scatter(g_step, "dp", scatter_dimension=0, tiled=True), "ctx")
    return (
        out_natural,
        grad_natural,
        g_gain,
        g_inx,
        g_inz,
        packed[:K],
        packed[K],
        packed[K + 3 + N :].T,
        g_step,
        packed[K + 1],
        packed[K + 3 : K + 3 + N].T,
        packed[K + 2],
        g_out,
    )


def solution(mesh):
    in_specs = (
        P(("dp", "ctx"), None),
        P("dp", None),
        P("dp", None),
        P("dp"),
        P("dp", "tp"),
        P("dp", "tp"),
        P(None, ("tp", "dp")),
        P(("tp", "dp")),
        P(("tp", "dp"), None),
        P("dp", "tp"),
        P(("tp", "dp")),
        P(("tp", "dp"), None),
        P(("tp", "dp")),
        P("tp", "dp"),
        P(("dp", "ctx"), None),
    )
    out_specs = (
        P(("dp", "ctx"), None),
        P(("dp", "ctx"), None),
        P("dp"),
        P("dp", "tp"),
        P("dp", "tp"),
        P(None, ("tp", "dp")),
        P(("tp", "dp")),
        P(("tp", "dp"), None),
        P("dp", "tp"),
        P(("tp", "dp")),
        P(("tp", "dp"), None),
        P(("tp", "dp")),
        P("tp", "dp"),
    )
    return jax.shard_map(
        per_device, mesh=mesh, in_specs=in_specs, out_specs=out_specs, check_vma=False
    )
```

```python
import jax
import jax.numpy as jnp
from jax import lax
from jax.experimental import pallas as pl
from jax.experimental.pallas import tpu as pltpu
from jax.sharding import PartitionSpec as P

N = 16
R = 128
K = 4
ROW = 2048
MICRO = 2
EPSILON = 1e-05

LANES = 128
SEGS = 8
FAR = 1e30
LOG2E = 1.4426950408889634
LN2 = 0.6931471805599453
F32 = jnp.float32
BF16 = jnp.bfloat16


def contract_last(left, right):
    return lax.dot_general(left, right, (((1,), (1,)), ((), ())), preferred_element_type=F32)


def contract_first(left, right):
    return lax.dot_general(left, right, (((0,), (0,)), ((), ())), preferred_element_type=F32)


def shifted(value, axis, steps):
    count = lax.axis_size(axis)
    leading, last = (max(0, -steps), min(count, count - steps))
    return lax.ppermute(value, axis, [(source, source + steps) for source in range(leading, last)])


def piece_starts(lengths, arrangement):
    count = lengths.shape[0]
    ids = jnp.arange(count, dtype=jnp.int32)
    ordered = jnp.sum(jnp.where(arrangement[:, None] == ids[None, :], lengths[None, :], 0), axis=1)
    nat_start = jnp.cumsum(lengths) - lengths
    pack_start = jnp.cumsum(ordered) - ordered
    rows = jnp.arange(1, MICRO, dtype=jnp.int32) * ROW
    slot = jnp.sum((rows[:, None] >= pack_start[None, 1:]).astype(jnp.int32), axis=1)
    in_slot = slot[:, None] == ids[None, :]
    sequence = jnp.sum(jnp.where(in_slot, arrangement[None, :], 0), axis=1)
    begun = jnp.sum(jnp.where(in_slot, pack_start[None, :], 0), axis=1)
    source = (
        jnp.sum(jnp.where(sequence[:, None] == ids[None, :], nat_start[None, :], 0), axis=1)
        + rows
        - begun
    )
    return jnp.concatenate([nat_start, source])


def exact_parts(value):
    high = value.astype(BF16)
    rest = value - high.astype(F32)
    mid = rest.astype(BF16)
    return high, mid, (rest - mid.astype(F32)).astype(BF16)


def spread_columns(table_ref, out_ref, extra_ref, turned_ref, groups, steps):
    rows_of = SEGS * steps
    row = lax.broadcasted_iota(jnp.int32, (2 * LANES, 2 * LANES), 0) % LANES
    side = lax.broadcasted_iota(jnp.int32, (2 * LANES, 2 * LANES), 1) // LANES
    for g in range(groups):

        def one(i, _):
            turned_ref[pl.ds(pl.multiple_of(i * SEGS, SEGS), SEGS), :] = table_ref[
                pl.ds(g * rows_of + i, SEGS, stride=steps), :
            ]
            return 0

        lax.fori_loop(0, steps, one, 0, unroll=8)
        high, mid, low = exact_parts(turned_ref[0:rows_of, :])
        most = jnp.concatenate([high, mid], axis=1)
        for n in range(0, 2 * N + 1, 2):
            pick = (row == n + side).astype(F32).astype(BF16)
            value = jnp.dot(most, pick, preferred_element_type=F32)
            value = value + jnp.dot(low, pick[:LANES], preferred_element_type=F32)
            first = value[:, :LANES].reshape(steps, SEGS, LANES)
            if n < 2 * N:
                out_ref[g * steps : (g + 1) * steps, n] = first
                out_ref[g * steps : (g + 1) * steps, n + 1] = value[:, LANES:].reshape(
                    steps, SEGS, LANES
                )
            else:
                extra_ref[g * steps : (g + 1) * steps] = first


def silu_rows(left_ref, gate_ref, out_ref):
    strip = 128

    def one(r, _):
        at = pl.ds(pl.multiple_of(r * strip, strip), strip)
        gate = gate_ref[at, :]
        out_ref[at, :] = left_ref[at, :] * gate * jax.nn.sigmoid(gate)
        return 0

    lax.fori_loop(0, out_ref.shape[0] // strip, one, 0)


def totals_kernel(
    groups,
    steps,
    step_ref,
    act_ref,
    d_gated_ref,
    gate_ref,
    rate_ref,
    table_ref,
    seg_s_ref,
    seg_h_ref,
    seg_c_ref,
    whole_ref,
    bc_s,
    keep_s,
    act_s,
    dy_s,
):
    rows_of = SEGS * steps

    @pl.when(pl.program_id(0) == 0)
    def _():
        spread_columns(table_ref, bc_s, keep_s, act_s, groups, steps)

    act_s[...] = act_ref[...].astype(F32)
    silu_rows(d_gated_ref, gate_ref, dy_s)
    half = N
    zero = jnp.zeros((SEGS, LANES), F32)
    for g in range(groups):
        for lo in range(0, N, half):
            rates = [
                jnp.broadcast_to(rate_ref[lo + n : lo + n + 1, :], (SEGS, LANES))
                for n in range(half)
            ]

            def one(i, carry):
                total, state, reach, back = carry
                state, reach, back = list(state), list(reach), list(back)
                at = pl.ds(g * rows_of + i, SEGS, stride=steps)
                step, act, dy = step_ref[at, :], act_s[at, :], dy_s[at, :]
                gone = step + keep_s[g * steps + i]
                push = step * act
                for n in range(half):
                    decay = jnp.exp2(gone * rates[n])
                    state[n] = decay * state[n] + push * bc_s[g * steps + i, lo + n]
                    reach[n] = reach[n] * decay
                    back[n] = back[n] + reach[n] * (dy * bc_s[g * steps + i, N + lo + n])
                return (total + gone, tuple(state), tuple(reach), tuple(back))

            total, state, _, back = lax.fori_loop(
                0,
                steps,
                one,
                (zero, (zero,) * half, (jnp.ones((SEGS, LANES), F32),) * half, (zero,) * half),
                unroll=8,
            )
            if lo == 0:
                seg_s_ref[g * SEGS : (g + 1) * SEGS, :] = total
            for n in range(half):
                first = (g * N + lo + n) * SEGS
                seg_h_ref[first : first + SEGS, :] = state[n]
                seg_c_ref[first : first + SEGS, :] = back[n]
    rate = rate_ref[...]
    h = jnp.zeros((N, LANES), F32)
    c = jnp.zeros((N, LANES), F32)
    order = [(g, s) for g in range(groups) for s in range(SEGS)]
    gone = jnp.zeros((1, LANES), F32)
    for g, s in order:
        at = pl.ds(g * N * SEGS + s, N, stride=SEGS)
        spent = seg_s_ref[g * SEGS + s : g * SEGS + s + 1, :]
        h = jnp.exp2(rate * spent) * h + seg_h_ref[at, :]
        gone = gone + spent
    for g, s in order[::-1]:
        at = pl.ds(g * N * SEGS + s, N, stride=SEGS)
        spent = seg_s_ref[g * SEGS + s : g * SEGS + s + 1, :]
        c = jnp.exp2(rate * spent) * c + seg_c_ref[at, :]
    whole_ref[0:N, :] = h
    whole_ref[N : 2 * N, :] = c
    whole_ref[2 * N : 2 * N + SEGS, :] = jnp.broadcast_to(gone, (SEGS, LANES))


def grads_kernel(
    groups,
    steps,
    blocks,
    step_ref,
    pre_ref,
    act_ref,
    d_gated_ref,
    gate_ref,
    skip_ref,
    rate_ref,
    table_ref,
    seg_s_ref,
    seg_h_ref,
    seg_c_ref,
    h_in_ref,
    c_in_ref,
    gated_t_ref,
    gated_ref,
    d_gate_ref,
    d_pre_ref,
    drive_ref,
    d_rate_ref,
    d_bc_ref,
    bc_s,
    keep_s,
    act_s,
    enter_h,
    enter_c,
    decay_s,
    prior_s,
    sum_b,
    sum_c,
    dy_s,
    y_s,
    d_step_s,
    d_act_s,
):
    g, j = pl.program_id(0), pl.program_id(1)

    @pl.when(j == 0)
    def _():
        spread_columns(table_ref, bc_s, keep_s, act_s, 1, steps)
        sum_b[...] = jnp.zeros_like(sum_b)
        sum_c[...] = jnp.zeros_like(sum_c)

    rate = rate_ref[...]

    @pl.when(g == 0)
    def _():
        h = h_in_ref[...]
        c = c_in_ref[...]
        order = [(a, s) for a in range(groups) for s in range(SEGS)]
        for a, s in order:
            at = pl.ds(a * N * SEGS + s, N, stride=SEGS)
            spent = seg_s_ref[a * SEGS + s : a * SEGS + s + 1, :]
            enter_h.at[j][at, :] = h
            h = jnp.exp2(rate * spent) * h + seg_h_ref[at, :]
        for a, s in order[::-1]:
            at = pl.ds(a * N * SEGS + s, N, stride=SEGS)
            spent = seg_s_ref[a * SEGS + s : a * SEGS + s + 1, :]
            enter_c.at[j][at, :] = c
            c = jnp.exp2(rate * spent) * c + seg_c_ref[at, :]

    act_s[...] = act_ref[...].astype(F32)
    silu_rows(d_gated_ref, gate_ref, dy_s)
    first = g * N * SEGS

    def rate_row(n):
        return jnp.broadcast_to(rate_ref[n : n + 1, :], (SEGS, LANES))

    def ahead(i, state):
        state = list(state)
        at = pl.ds(i, SEGS, stride=steps)
        step, act, dy = step_ref[at, :], act_s[at, :], dy_s[at, :]
        gone = step + keep_s[i]
        push = step * act
        y = jnp.zeros((SEGS, LANES), F32)
        for n in range(N):
            decay = jnp.exp2(gone * rate_row(n))
            prior = decay * state[n]
            state[n] = prior + push * bc_s[i, n]
            decay_s[i, n] = decay
            prior_s[i, n] = prior
            y = y + state[n] * bc_s[i, N + n]
            sum_c[i, n] += state[n] * dy
        y_s[at, :] = y
        return tuple(state)

    def enter(ref, n):
        return ref[j, pl.ds(pl.multiple_of(first + n * SEGS, SEGS), SEGS), :]

    lax.fori_loop(0, steps, ahead, tuple(enter(enter_h, n) for n in range(N)), unroll=8)

    def back(k, carry):
        i = steps - 1 - k
        carried, d_rate = list(carry[0]), list(carry[1])
        at = pl.ds(i, SEGS, stride=steps)
        step, act, dy = step_ref[at, :], act_s[at, :], dy_s[at, :]
        push = step * act
        along = jnp.zeros((SEGS, LANES), F32)
        d_step = jnp.zeros((SEGS, LANES), F32)
        for n in range(N):
            grad = dy * bc_s[i, N + n] + carried[n]
            along = along + grad * bc_s[i, n]
            log_grad = grad * prior_s[i, n]
            d_step = d_step + log_grad * rate_row(n)
            d_rate[n] = d_rate[n] + log_grad * step
            carried[n] = grad * decay_s[i, n]
            sum_b[i, n] += grad * push
        d_step_s[at, :] = d_step * LN2 + along * act
        d_act_s[at, :] = along * step
        return (tuple(carried), tuple(d_rate))

    zero = jnp.zeros((SEGS, LANES), F32)
    _, d_rate = lax.fori_loop(
        0, steps, back, (tuple(enter(enter_c, n) for n in range(N)), (zero,) * N), unroll=8
    )
    for n in range(N):
        d_rate_ref[0, n : n + 1, :] = jnp.sum(d_rate[n], axis=0, keepdims=True)

    strip = 64

    def close(r, sums):
        at = pl.ds(pl.multiple_of(r * strip, strip), strip)
        gate, d_gated, act, dy = gate_ref[at, :], d_gated_ref[at, :], act_s[at, :], dy_s[at, :]
        skip = skip_ref[...]
        sig = jax.nn.sigmoid(gate)
        scan_out = y_s[at, :] + skip * act
        gated = scan_out * gate * sig
        y_s[at, :] = gated
        gated_ref[at, :] = gated.astype(BF16)
        d_gate_ref[at, :] = (d_gated * scan_out * sig * (1.0 + gate * (1.0 - sig))).astype(BF16)
        d_pre = (d_step_s[at, :] * jax.nn.sigmoid(pre_ref[at, :])).astype(BF16)
        d_pre_ref[at, :] = d_pre
        drive_ref[at, :] = d_act_s[at, :] + dy * skip

        def fold(value):
            return jnp.sum(value.reshape(strip // SEGS, SEGS, LANES), axis=0)

        return sums[0] + fold(dy * act), sums[1] + fold(d_pre.astype(F32))

    g_skip, g_bias = lax.fori_loop(0, y_s.shape[0] // strip, close, (zero, zero))
    d_rate_ref[0, N : N + 1, :] = jnp.sum(g_skip, axis=0, keepdims=True)
    d_rate_ref[0, N + 1 : N + 2, :] = jnp.sum(g_bias, axis=0, keepdims=True)
    gated_t_ref[...] = y_s[...].T.astype(BF16)

    @pl.when(j == blocks - 1)
    def _():
        column = lax.broadcasted_iota(jnp.int32, (2 * LANES, LANES), 1)
        total = jnp.zeros((steps * SEGS, LANES), F32)
        for n in range(N):
            for ref, at in ((sum_b, n), (sum_c, N + n)):
                pick = (column == at).astype(F32).astype(BF16)
                value = exact_parts(ref[:, n].reshape(steps * SEGS, LANES))
                total = total + jnp.dot(
                    jnp.concatenate(value[:2], axis=1), pick, preferred_element_type=F32
                )
        act_s[...] = total

        def put(i, _):
            d_bc_ref[pl.ds(i, SEGS, stride=steps), :] = act_s[
                pl.ds(pl.multiple_of(i * SEGS, SEGS), SEGS), :
            ]
            return 0

        lax.fori_loop(0, steps, put, 0, unroll=8)


def scan_totals(step_size, activated, d_gated, gate_z, rate2, table, groups):
    length, channels = step_size.shape
    steps = length // (groups * SEGS)
    blocks = channels // LANES
    tall = pl.BlockSpec((length, LANES), lambda j: (0, j))
    rows = groups * N * SEGS
    return pl.pallas_call(
        lambda *refs: totals_kernel(groups, steps, *refs),
        grid=(blocks,),
        in_specs=[
            tall,
            tall,
            tall,
            tall,
            pl.BlockSpec((N, LANES), lambda j: (0, j)),
            pl.BlockSpec((length, LANES), lambda j: (0, 0)),
        ],
        out_specs=[
            pl.BlockSpec((groups * SEGS, LANES), lambda j: (0, j)),
            pl.BlockSpec((rows, LANES), lambda j: (0, j)),
            pl.BlockSpec((rows, LANES), lambda j: (0, j)),
            pl.BlockSpec((2 * N + SEGS, LANES), lambda j: (0, j)),
        ],
        out_shape=[
            jax.ShapeDtypeStruct((groups * SEGS, channels), F32),
            jax.ShapeDtypeStruct((rows, channels), F32),
            jax.ShapeDtypeStruct((rows, channels), F32),
            jax.ShapeDtypeStruct((2 * N + SEGS, channels), F32),
        ],
        scratch_shapes=[
            pltpu.VMEM((groups * steps, 2 * N, SEGS, LANES), F32),
            pltpu.VMEM((groups * steps, SEGS, LANES), F32),
            pltpu.VMEM((length, LANES), F32),
            pltpu.VMEM((length, LANES), F32),
        ],
        compiler_params=pltpu.CompilerParams(
            dimension_semantics=("arbitrary",), vmem_limit_bytes=40 << 20
        ),
        cost_estimate=pl.CostEstimate(
            flops=length * channels * N * 3000,
            bytes_accessed=length * channels * 14,
            transcendentals=length * channels * N,
        ),
        name="scan_totals",
    )(step_size, activated, d_gated, gate_z, rate2, table)


def scan_grads(
    step_size, step_pre, activated, d_gated, gate_z, skip, rate2, table, segs, enter, groups
):
    length, channels = step_size.shape
    steps = length // (groups * SEGS)
    blocks = channels // LANES
    share = length // groups
    tall = pl.BlockSpec((share, LANES), lambda g, j: (g, j))
    one = pl.BlockSpec((share, LANES), lambda g, j: (g, 0))
    rows = groups * N * SEGS

    def wide(height):
        return pl.BlockSpec((height, LANES), lambda g, j: (0, j))

    def shape(dtype, *dims):
        return jax.ShapeDtypeStruct(dims, dtype)

    grid_spec = pl.GridSpec(
        grid=(groups, blocks),
        in_specs=[tall] * 5
        + [wide(1), wide(N), one]
        + [wide(groups * SEGS), wide(rows), wide(rows), wide(N), wide(N)],
        out_specs=[pl.BlockSpec((LANES, share), lambda g, j: (j, g))]
        + [tall] * 4
        + [pl.BlockSpec((1, 3 * SEGS, LANES), lambda g, j: (g, 0, j)), one],
        scratch_shapes=[
            pltpu.VMEM((steps, 2 * N, SEGS, LANES), F32),
            pltpu.VMEM((steps, SEGS, LANES), F32),
            pltpu.VMEM((share, LANES), F32),
            pltpu.VMEM((blocks, rows, LANES), F32),
            pltpu.VMEM((blocks, rows, LANES), F32),
            pltpu.VMEM((steps, N, SEGS, LANES), F32),
            pltpu.VMEM((steps, N, SEGS, LANES), F32),
            pltpu.VMEM((steps, N, SEGS, LANES), F32),
            pltpu.VMEM((steps, N, SEGS, LANES), F32),
            pltpu.VMEM((share, LANES), F32),
            pltpu.VMEM((share, LANES), F32),
            pltpu.VMEM((share, LANES), F32),
            pltpu.VMEM((share, LANES), F32),
        ],
    )
    return pl.pallas_call(
        lambda *refs: grads_kernel(groups, steps, blocks, *refs),
        grid_spec=grid_spec,
        out_shape=[
            shape(BF16, channels, length),
            shape(BF16, length, channels),
            shape(BF16, length, channels),
            shape(BF16, length, channels),
            shape(F32, length, channels),
            shape(F32, groups, 3 * SEGS, channels),
            shape(F32, length, LANES),
        ],
        compiler_params=pltpu.CompilerParams(
            dimension_semantics=("arbitrary", "arbitrary"), vmem_limit_bytes=48 << 20
        ),
        cost_estimate=pl.CostEstimate(
            flops=length * channels * N * 6000,
            bytes_accessed=length * channels * 30,
            transcendentals=length * channels * N,
        ),
        name="scan_grads",
    )(step_size, step_pre, activated, d_gated, gate_z, skip, rate2, table, *segs, *enter)


MESH = pl.DeviceIdType.MESH
CHUNK = 128
AHEAD = 2
LATE = 2
WIDE = 256


def finish_kernel(
    parts,
    gated_t_hbm,
    gated_hbm,
    normed_hbm,
    d_gate_hbm,
    d_pre_hbm,
    drive_hbm,
    inner_hbm,
    halo_hbm,
    w_inx_hbm,
    w_inz_hbm,
    w_out_hbm,
    x_hbm,
    dy_hbm,
    rms_ref,
    gain_ref,
    masks_ref,
    taps_ref,
    w_step_ref,
    w_proj_ref,
    d_bc_ref,
    misc_ref,
    g_step_ref,
    sums_out,
    sums_z,
    sums_x,
    small_ref,
    out_hbm,
    grad_hbm,
    left,
    right,
    w_x,
    w_z,
    x_cols,
    y_out,
    y_in,
    a_in,
    b_in,
    line,
    first,
    held,
    total,
    core_out,
    core_in,
    kept,
    x_out,
    x_in,
    rows_x,
    rows_dy,
    final,
    passed,
    gain_sum,
    gain_core,
    gain_x,
    gain_out,
    s_out,
    s_in,
    s_a,
    s_b,
    s_line,
    p_out,
    p_in,
    q_out,
    q_in,
    turned_p,
    drive,
    inner_low,
    inner,
    active,
    pack,
    tail,
    halo_out,
    halo_in,
    load_sem,
    w_sem,
    y_sem,
    a_sem,
    b_sem,
    c_sem,
    out_sem,
    tp_sem,
    gain_sem,
    final_sem,
    small_sem,
    chain_sem,
    proj_sem,
    halo_sem,
):
    rows, width = x_hbm.shape
    half = width // 2
    dp, z, tp = lax.axis_index("dp"), lax.axis_index("ctx"), lax.axis_index("tp")
    core, x_bit = tp % 2, tp // 2
    near, across = tp + 1 - 2 * core, (tp + 2) % 4
    ends = (z == 0) | (z == 3)
    middle = (z == 1) | (z == 2)
    inward, twin, outward = z // 2 + 1, 3 - z, (z // 2) * 3

    def load(source, target, at):
        copy = pltpu.make_async_copy(source, target, load_sem.at[at])
        copy.start()
        return copy

    quarter = rows // 4
    own_row = pl.multiple_of(core * (rows // 2) + x_bit * quarter, quarter)
    got_left = load(gated_t_hbm, left.at[0], 1)
    mine = pl.multiple_of(dp * half, half)
    away = pl.multiple_of((1 - dp) * half, half)
    got_other = load(dy_hbm.at[:, pl.ds(away, half)], right.at[1], 2)
    got_pre = load(d_pre_hbm, right.at[3], 0)
    others = [
        load(dy_hbm.at[:, pl.ds(mine, half)], right.at[0], 3),
        load(normed_hbm.at[pl.ds(0, half), :], left.at[1], 4),
        load(normed_hbm.at[pl.ds(half, half), :], left.at[2], 5),
        load(d_gate_hbm, right.at[2], 6),
        load(x_hbm.at[pl.ds(own_row, quarter), pl.ds(mine, half)], rows_x.at[:, pl.ds(0, half)], 7),
        load(dy_hbm.at[pl.ds(own_row, quarter), pl.ds(mine, half)], rows_dy.at[:, pl.ds(0, half)], 8),
        load(
            x_hbm.at[pl.ds(own_row, quarter), pl.ds(away, half)],
            rows_x.at[:, pl.ds(half, half)],
            16,
        ),
        load(
            dy_hbm.at[pl.ds(own_row, quarter), pl.ds(away, half)],
            rows_dy.at[:, pl.ds(half, half)],
            17,
        ),
    ]

    barrier = pltpu.get_barrier_semaphore()
    for peer in ({"tp": near}, {"tp": across}, {"dp": 1 - dp}):
        pl.semaphore_signal(barrier, inc=1, device_id=peer, device_id_type=MESH)

    @pl.when(ends)
    def _():
        pl.semaphore_signal(barrier, inc=1, device_id={"ctx": inward}, device_id_type=MESH)
        pl.semaphore_wait(barrier, 4)

    @pl.when(middle)
    def _():
        pl.semaphore_signal(barrier, inc=1, device_id={"ctx": twin}, device_id_type=MESH)
        pl.semaphore_signal(barrier, inc=1, device_id={"ctx": outward}, device_id_type=MESH)
        pl.semaphore_wait(barrier, 5)

    def remote(source, target, sems, at, peer):
        return pltpu.make_async_remote_copy(
            src_ref=source,
            dst_ref=target,
            send_sem=sems.at[0, at],
            recv_sem=sems.at[1, at],
            device_id=peer,
            device_id_type=MESH,
        )

    per_weight, pairs = parts // 3, parts // 2

    def chunk(k):
        return k // per_weight, pl.multiple_of(k % per_weight * CHUNK, CHUNK)

    def product(slot_l, slot_r, column):
        return jnp.dot(
            left[slot_l], right[slot_r, :, pl.ds(column, 2 * CHUNK)], preferred_element_type=F32
        )

    def y_copy(k):
        return remote(y_out.at[k % 6], y_in.at[k % 8], y_sem, k, {"dp": 1 - dp})

    def a_copy(k):
        return remote(line.at[k % 4], a_in.at[k % 12], a_sem, k, {"ctx": inward})

    def b_copy(k):
        return remote(line.at[k % 4], b_in.at[k % 4], b_sem, k, {"ctx": twin})

    sums = (sums_out, sums_z, sums_x)

    def far_copy(k, ref):
        spot = ref.at[:, pl.ds(chunk(k)[1], CHUNK)]
        return remote(total.at[k % 4], spot, c_sem, k, {"ctx": outward})

    def own_copy(k, ref):
        spot = ref.at[:, pl.ds(chunk(k)[1], CHUNK)]
        return pltpu.make_async_copy(total.at[k % 4], spot, out_sem.at[k])

    def give_c(k, start):
        for w, ref in enumerate(sums):

            @pl.when(k // per_weight == w)
            def _():
                far, own = far_copy(k, ref), own_copy(k, ref)
                if start:
                    far.start()
                    own.start()
                else:
                    far.wait_send()
                    own.wait()

    def wait_c(k):
        far_copy(k, sums_out).wait_recv()

    def pair(p):
        w, column = chunk(2 * p)
        return w, pl.multiple_of(column, 2 * CHUNK)

    def send_y(k):
        @pl.when(k % 2 == 0)
        def _():
            w, column = pair(k // 2)
            up = (w + 1) // 2

            @pl.when(k >= 6)
            def _():
                y_copy(k - 6).wait_send()
                y_copy(k - 5).wait_send()

            value = product(2 * up, w + 1, column).astype(BF16)
            y_out[k % 6] = value[:, :CHUNK]
            y_out[(k + 1) % 6] = value[:, CHUNK:]

        y_copy(k).start()

    def take_y(k):
        @pl.when(k % 2 == 0)
        def _():
            w, column = pair(k // 2)
            up = (w + 1) // 2
            value = product(up, w + up, column)
            held[0] = value[:, :CHUNK]
            held[1] = value[:, CHUNK:]

        y_copy(k).wait_recv()
        value = held[k % 2] + y_in[k % 8].astype(F32)

        @pl.when(ends)
        def _():
            @pl.when(k >= 4)
            def _():
                a_copy(k - 4).wait_send()

            @pl.when(k >= 12)
            def _():
                wait_c(k - 12)

            line[k % 4] = value.astype(BF16)
            a_copy(k).start()

        @pl.when(middle)
        def _():
            first[k % 2] = value

    def take_a(k):
        @pl.when(middle)
        def _():
            @pl.when(k >= 4)
            def _():
                b_copy(k - 4).wait_send()

            a_copy(k).wait_recv()
            line[k % 4] = (first[k % 2] + a_in[k % 12].astype(F32)).astype(BF16)
            b_copy(k).start()

    def take_b(k):
        @pl.when(middle)
        def _():
            @pl.when(k >= 4)
            def _():
                give_c(k - 4, False)

            b_copy(k).wait_recv()
            total[k % 4] = (line[k % 4].astype(F32) + b_in[k % 4].astype(F32)).astype(BF16)
            give_c(k, True)

    def tick(k, _):
        @pl.when((k >= 2 * LATE) & (k < parts + 2 * LATE))
        def _():
            take_b(k - 2 * LATE)

        @pl.when((k >= LATE) & (k < parts + LATE))
        def _():
            take_a(k - LATE)

        @pl.when(k < parts)
        def _():
            take_y(k)

        @pl.when(k + AHEAD < parts)
        def _():
            send_y(k + AHEAD)

        return 0

    def ticks(begin, end):
        lax.fori_loop(begin, end, tick, 0)

    got_left.wait()
    got_other.wait()
    for k in range(AHEAD):
        send_y(jnp.int32(k))
    got_pre.wait()
    p_out[:, :LANES] = contract_last(right[3], w_step_ref[...]).astype(BF16)
    p_out[:, LANES:] = d_bc_ref[...].astype(BF16)
    p_copy = remote(p_out, p_in, proj_sem, 0, {"tp": near})
    p_copy.start()
    got_gated = load(gated_hbm, right.at[3], 0)
    p_copy.wait_recv()
    q_out[...] = (p_out[...].astype(F32) + p_in[...].astype(F32)).astype(BF16)
    q_copy = remote(q_out, q_in, proj_sem, 1, {"tp": across})
    q_copy.start()

    block = w_x.shape[0]
    send_row = pl.multiple_of((1 - core) * (rows // 2), rows // 2)
    keep_row = pl.multiple_of(core * (rows // 2), rows // 2)
    give = pl.multiple_of((1 - x_bit) * quarter, quarter)
    have = pl.multiple_of(x_bit * quarter, quarter)

    got_gated.wait()

    def out_columns(d, _):
        at = pl.multiple_of(d * block, block)
        copy = pltpu.make_async_copy(w_out_hbm.at[:, pl.ds(at, block)], x_cols, w_sem.at[0])
        copy.start()
        copy.wait()
        core_out[:, pl.ds(at, block)] = jnp.dot(
            right[3, pl.ds(send_row, rows // 2), :], x_cols[...], preferred_element_type=F32
        ).astype(BF16)
        kept[:, pl.ds(at, block)] = jnp.dot(
            right[3, pl.ds(keep_row, rows // 2), :], x_cols[...], preferred_element_type=F32
        ).astype(BF16)
        return 0

    lax.fori_loop(0, width // block, out_columns, 0)
    core_copy = remote(core_out, core_in, tp_sem, 0, {"tp": near})
    core_copy.start()

    def chain_loads(q):
        at = pl.ds(q * WIDE, WIDE)
        return (
            pltpu.make_async_copy(
                drive_hbm.at[:, at], drive.at[pl.ds(SEGS, rows), :], chain_sem.at[0]
            ),
            pltpu.make_async_copy(
                inner_hbm.at[:, at], inner_low.at[pl.ds(2 * SEGS, rows), :], chain_sem.at[1]
            ),
            pltpu.make_async_copy(
                halo_hbm.at[:, at], inner_low.at[pl.ds(0, 2 * SEGS), :], chain_sem.at[2]
            ),
        )

    for copy in chain_loads(0):
        copy.start()
    for copy in others:
        copy.wait()

    ticks(0, 2)

    core_copy.wait_recv()

    def to_across():
        x_out[...] = (
            kept[pl.ds(give, quarter), :].astype(F32) + core_in[pl.ds(give, quarter), :].astype(F32)
        ).astype(BF16)

    to_across()
    x_copy = remote(x_out, x_in, tp_sem, 1, {"tp": across})
    x_copy.start()

    q_copy.wait_recv()
    projected = q_out[...].astype(F32) + q_in[...].astype(F32)
    p_copy.wait_send()
    p_out[...] = projected.astype(BF16)
    turned_p[...] = projected.T.astype(BF16)

    zeros = jnp.zeros((SEGS, WIDE), F32)
    strip = 64
    pad = 2 * SEGS
    drive[0:SEGS, :] = zeros
    drive[rows + SEGS :, :] = zeros

    def chain(q):
        cut = slice(q * WIDE, (q + 1) * WIDE)
        for copy in chain_loads(q):
            copy.wait()
        inner[...] = inner_low[...].astype(F32)
        taps = [taps_ref[i : i + 1, cut] for i in range(K + 1)]

        def down(r, sums):
            at = pl.multiple_of(r * strip, strip)
            mask = masks_ref[pl.ds(at + SEGS, strip), :]
            valid = [mask[:, i : i + 1] for i in range(K - 1)]
            near_rows = inner[pl.ds(at, strip + pad), :]
            moved = [near_rows[pad - (K - 1) + i :][:strip] for i in range(K)]
            moved = [moved[i] * valid[i] for i in range(K - 1)] + moved[K - 1 :]
            pre = taps[K] + taps[K - 1] * moved[K - 1]
            for i in range(K - 1):
                pre = pre + taps[i] * moved[i]
            sig = jax.nn.sigmoid(pre)
            active[pl.ds(at, strip), :] = (pre * sig).astype(BF16)
            whole = drive[pl.ds(at + SEGS, strip), :] + contract_last(
                p_out[pl.ds(at, strip), :], w_proj_ref[cut, :]
            )
            grad = whole * sig * (1.0 + pre * (1.0 - sig))
            drive[pl.ds(at + SEGS, strip), :] = grad

            def fold(value):
                return jnp.sum(value.reshape(strip // SEGS, SEGS, WIDE), axis=0)

            terms = [grad * m for m in moved] + [grad]
            return tuple(s + fold(t) for s, t in zip(sums, terms))

        sums_q = lax.fori_loop(0, rows // strip, down, (zeros,) * (K + 1))
        for i in range(K + 1):
            pack[i : i + 1, cut] = jnp.sum(sums_q[i], axis=0, keepdims=True)

        def spread(base, size):
            grads = drive[pl.ds(base + SEGS, size + SEGS), :]
            mask = masks_ref[pl.ds(base + SEGS, size + SEGS), :]
            value = grads[:size] * taps[K - 1]
            for back in range(1, K):
                valid = grads * mask[:, K - 1 - back : K - back]
                value = value + valid[back : back + size] * taps[K - 1 - back]
            return value

        def up(r, _):
            at = pl.multiple_of(r * strip, strip)
            right[3, pl.ds(at, strip), cut] = spread(at, strip).astype(BF16)
            return 0

        lax.fori_loop(0, rows // strip, up, 0)
        tail[:, cut] = spread(rows - pad, pad)
        halo_out[:, cut] = spread(-SEGS, SEGS)
        pack[4 * SEGS : 4 * SEGS + R + 2 * N, cut] = jnp.dot(
            turned_p[...], active[...], preferred_element_type=F32
        )[: R + 2 * N]

    for q in range(rows // WIDE):
        chain(q)
        if q + 1 < rows // WIDE:
            for copy in chain_loads(q + 1):
                copy.start()
            ticks(2 * q + 2, 2 * q + 4)
    halo_copy = remote(halo_out, halo_in, halo_sem, 0, {"ctx": jnp.maximum(z - 1, 0)})

    @pl.when(z > 0)
    def _():
        halo_copy.start()

    ticks(8, 10)

    def gather(ref, source, base):
        copies = []
        for side in range(2):
            place = pl.multiple_of((dp + side - 2 * dp * side) * half, half)
            spot = ref.at[pl.ds(own_row, quarter), pl.ds(place, half)]
            piece = source.at[:, pl.ds(side * half, half)]
            for p, peer in enumerate((across, near)):
                copies.append(remote(piece, spot, final_sem, base + 2 * p + side, {"tp": peer}))
            copies.append(pltpu.make_async_copy(piece, spot, load_sem.at[9 + base // 2 + side]))
        for copy in copies:
            copy.start()
        return copies

    def forward(ref, copies, base):
        copies[0].wait_recv()
        copies[3].wait_recv()
        row = pl.multiple_of(core * (rows // 2) + (1 - x_bit) * quarter, quarter)
        spot = ref.at[pl.ds(row, quarter), :]
        fetch = pltpu.make_async_copy(spot, passed, load_sem.at[15])
        fetch.start()
        fetch.wait()
        copy = remote(passed, spot, final_sem, base + 4, {"tp": near})
        copy.start()
        return copy

    def finished(copies, last):
        for k, copy in enumerate(copies):
            if k in (0, 3):
                copy.wait_send()
            else:
                copy.wait()
        last.wait()

    x_copy.wait_recv()

    def summed_rows():
        return (
            kept[pl.ds(have, quarter), :].astype(F32)
            + core_in[pl.ds(have, quarter), :].astype(F32)
            + x_in[...].astype(F32)
        )

    final[...] = (rows_x[...].astype(F32) + summed_rows()).astype(BF16)
    out_copies = gather(out_hbm, final, 0)

    @pl.when(z < 3)
    def _():
        halo_copy.wait_recv()
        tail[SEGS:, :] = tail[SEGS:, :] + halo_in[...]

    right[3, rows - pad :, :] = tail[...].astype(BF16)

    ticks(10, 12)

    core_copy.wait_send()
    x_copy.wait_send()

    def columns(d, _):
        at = pl.multiple_of(d * block, block)
        copies = [
            pltpu.make_async_copy(w_inx_hbm.at[pl.ds(at, block), :], w_x, w_sem.at[0]),
            pltpu.make_async_copy(w_inz_hbm.at[pl.ds(at, block), :], w_z, w_sem.at[1]),
            pltpu.make_async_copy(
                x_hbm.at[:, pl.ds(pl.multiple_of((at + dp * half) % width, block), block)],
                x_cols,
                w_sem.at[2],
            ),
        ]
        for copy in copies:
            copy.start()
        for copy in copies:
            copy.wait()
        sums_d = jnp.zeros((SEGS, block), F32)
        for row, keep in ((send_row, False), (keep_row, True)):
            span = pl.ds(row, rows // 2)
            value = contract_last(right[3, span, :], w_x[...])
            value = value + contract_last(right[2, span, :], w_z[...])
            hat = x_cols[span, :].astype(F32) * rms_ref[span, :]
            sums_d = sums_d + jnp.sum(
                (value * hat).reshape(rows // 2 // SEGS, SEGS, block), axis=0
            )
            target = kept if keep else core_out
            target[:, pl.ds(at, block)] = value.astype(BF16)
        gain_sum[:, pl.ds(at, block)] = sums_d
        return 0

    for d in range(width // block):
        columns(d, 0)
        ticks(12 + d, 13 + d)
    gain_copy = remote(gain_sum, gain_core, gain_sem, 0, {"tp": near})
    gain_copy.start()
    gain_copy.wait_recv()
    core_again = remote(core_out, core_in, tp_sem, 2, {"tp": near})
    core_again.start()
    gain_out[...] = gain_sum[...] + gain_core[...]
    gain_across = remote(gain_out, gain_x, gain_sem, 1, {"tp": across})
    gain_across.start()

    ticks(16, 17)

    core_again.wait_recv()
    to_across()
    gain_across.wait_recv()
    x_again = remote(x_out, x_in, tp_sem, 3, {"tp": across})
    x_again.start()

    ticks(17, 18)

    both = gain_out[...] + gain_x[...]
    fine = half // 2
    steps_half = g_step_ref.shape[0] // 2
    base = 4 * SEGS + R + 2 * N
    pack[K + 1 : SEGS, :] = jnp.zeros((SEGS - K - 1, 2 * fine), F32)
    pack[SEGS : 4 * SEGS, :] = misc_ref[...]

    def small_rows(index, lanes):
        column = pl.multiple_of(index * fine, fine)
        row = pl.multiple_of(index * steps_half, steps_half)
        return jnp.concatenate(
            [
                pack[:, pl.ds(column, fine)],
                g_step_ref[pl.ds(row, steps_half), :fine],
                g_step_ref[pl.ds(row, steps_half), fine:],
                both[:, lanes : lanes + fine],
                both[:, lanes + fine : lanes + 2 * fine],
            ],
            axis=0,
        )

    s_out[...] = small_rows(1 - dp, half).astype(BF16)
    small_y = remote(s_out, s_in, small_sem, 0, {"dp": 1 - dp})
    small_y.start()
    out_last = forward(out_hbm, out_copies, 0)

    ticks(18, 20)

    x_again.wait_recv()
    r_own = rms_ref[pl.ds(own_row, quarter), :]
    d_normed = summed_rows()
    hat = rows_x[...].astype(F32) * r_own
    d_hat = d_normed * gain_ref[...]
    mean = jnp.sum(d_hat * hat, axis=1, keepdims=True) * (1.0 / width)
    rows_dy[...] = (rows_dy[...].astype(F32) + r_own * (d_hat - hat * mean)).astype(BF16)
    grad_copies = gather(grad_hbm, rows_dy, 6)

    ticks(20, 21)

    small_y.wait_recv()
    s_keep = small_rows(dp, 0) + s_in[...].astype(F32)
    small_a = remote(s_line, s_a, small_sem, 1, {"ctx": inward})
    small_b = remote(s_line, s_b, small_sem, 2, {"ctx": twin})
    small_c = remote(small_ref, small_ref, small_sem, 3, {"ctx": outward})

    @pl.when(ends)
    def _():
        s_line[...] = s_keep.astype(BF16)
        small_a.start()

    @pl.when(middle)
    def _():
        small_a.wait_recv()
        s_line[...] = (s_keep + s_a[...].astype(F32)).astype(BF16)
        small_b.start()

    ticks(21, 22)

    finished(out_copies, out_last)
    grad_last = forward(grad_hbm, grad_copies, 6)

    @pl.when(middle)
    def _():
        small_b.wait_recv()
        small_ref[...] = (s_line[...].astype(F32) + s_b[...].astype(F32)).astype(BF16)
        small_c.start()

    ticks(22, parts + 2 * LATE)

    for k in range(parts - 6, parts):
        y_copy(k).wait_send()

    @pl.when(ends)
    def _():
        for k in range(parts - 4, parts):
            a_copy(k).wait_send()
        for k in range(parts - 12, parts):
            wait_c(k)
        small_a.wait_send()
        small_c.wait_recv()

    @pl.when(middle)
    def _():
        for k in range(parts - 4, parts):
            b_copy(k).wait_send()
            far_copy(k, sums_x).wait_send()
            own_copy(k, sums_x).wait()
        small_b.wait_send()
        small_c.wait_send()

    @pl.when(z > 0)
    def _():
        halo_copy.wait_send()

    q_copy.wait_send()
    core_again.wait_send()
    x_again.wait_send()
    gain_copy.wait_send()
    gain_across.wait_send()
    small_y.wait_send()
    finished(grad_copies, grad_last)


def finish(
    gated_t, gated, normed_t, d_gate, d_pre, drive, inner, halo, w_inx, w_inz, w_out, x_all, dy_all,
    rms, gain, masks, taps, w_step, w_proj, d_bc, misc, g_step,
):
    rows, width = x_all.shape
    channels = w_inx.shape[1]
    parts = 3 * (channels // CHUNK)
    half = width // 2
    small = 4 * SEGS + R + 2 * N + g_step.shape[0] + 2 * SEGS
    fine = half // 2
    block = 512
    hbm = pl.BlockSpec(memory_space=pl.ANY)
    vmem = pl.BlockSpec(memory_space=pltpu.VMEM)
    dma = pltpu.SemaphoreType.DMA
    piece = (half, CHUNK)
    quarter = rows // 4

    def low(*shape):
        return pltpu.VMEM(shape, BF16)

    def full(*shape):
        return pltpu.VMEM(shape, F32)

    return pl.pallas_call(
        lambda *refs: finish_kernel(parts, *refs),
        in_specs=[hbm] * 13 + [vmem] * 9,
        out_specs=[hbm, hbm, hbm, vmem, hbm, hbm],
        out_shape=[jax.ShapeDtypeStruct((half, channels), BF16)] * 3
        + [
            jax.ShapeDtypeStruct((small, fine), BF16),
            jax.ShapeDtypeStruct((rows, width), BF16),
            jax.ShapeDtypeStruct((rows, width), BF16),
        ],
        scratch_shapes=[
            low(3, half, rows),
            low(4, rows, channels),
            low(block, channels),
            low(block, channels),
            low(rows, block),
            low(6, *piece),
            low(8, *piece),
            low(12, *piece),
            low(4, *piece),
            low(4, *piece),
            full(2, *piece),
            full(2, *piece),
            low(4, *piece),
            low(rows // 2, width),
            low(rows // 2, width),
            low(rows // 2, width),
            low(quarter, width),
            low(quarter, width),
            low(quarter, width),
            low(quarter, width),
            low(quarter, width),
            low(quarter, width),
            full(SEGS, width),
            full(SEGS, width),
            full(SEGS, width),
            full(SEGS, width),
            low(small, fine),
            low(small, fine),
            low(small, fine),
            low(small, fine),
            low(small, fine),
            low(rows, 2 * LANES),
            low(rows, 2 * LANES),
            low(rows, 2 * LANES),
            low(rows, 2 * LANES),
            low(2 * LANES, rows),
            full(rows + 2 * SEGS, WIDE),
            low(rows + 2 * SEGS, WIDE),
            full(rows + 2 * SEGS, WIDE),
            low(rows, WIDE),
            full(4 * SEGS + R + 2 * N, channels),
            full(2 * SEGS, channels),
            full(SEGS, channels),
            full(SEGS, channels),
            dma((18,)),
            dma((3,)),
            dma((2, parts)),
            dma((2, parts)),
            dma((2, parts)),
            dma((2, parts)),
            dma((parts,)),
            dma((2, 4)),
            dma((2, 2)),
            dma((2, 11)),
            dma((2, 4)),
            dma((3,)),
            dma((2, 2)),
            dma((2, 1)),
        ],
        compiler_params=pltpu.CompilerParams(
            collective_id=0, has_side_effects=True, vmem_limit_bytes=63900 << 10
        ),
        cost_estimate=pl.CostEstimate(
            flops=200_000_000_000, bytes_accessed=60_000_000, transcendentals=0
        ),
        name="finish",
    )(
        gated_t, gated, normed_t, d_gate, d_pre, drive, inner, halo, w_inx, w_inz, w_out, x_all, dy_all,
        rms, gain, masks, taps, w_step, w_proj, d_bc, misc, g_step,
    )


def swap_pairs(value, axis, distance):
    count = lax.axis_size(axis)
    return lax.ppermute(value, axis, [(i, i ^ distance) for i in range(count)])


def ordered(mine, other, bit, axis=0):
    return jnp.where(
        bit == 0,
        jnp.concatenate([mine, other], axis=axis),
        jnp.concatenate([other, mine], axis=axis),
    )


def half_of(value, index, axis=0):
    size = value.shape[axis] // 2
    return lax.dynamic_slice_in_dim(value, index * size, size, axis)


def tp_sum(value):
    distance = 1
    while distance < lax.axis_size("tp"):
        value = value + swap_pairs(value, "tp", distance)
        distance *= 2
    return value


def tp_scatter(value):
    index, distance = lax.axis_index("tp"), 1
    while distance < lax.axis_size("tp"):
        mine = (index // distance) % 2
        got = swap_pairs(half_of(value, 1 - mine).astype(BF16), "tp", distance)
        value = half_of(value, mine).astype(F32) + got.astype(F32)
        distance *= 2
    return value


def tp_rows():
    index, distance, at, size = lax.axis_index("tp"), 1, 0, lax.axis_size("tp")
    while distance < lax.axis_size("tp"):
        size //= 2
        at = at + (index // distance) % 2 * size
        distance *= 2
    return at


def per_device(
    hidden_in,
    seq_lengths,
    pack_order,
    norm_gain,
    in_x_weight,
    in_z_weight,
    conv_weight,
    conv_bias,
    x_weight,
    dt_weight,
    dt_bias,
    a_log,
    skip_weight,
    out_weight,
    out_grad,
):
    length, width = hidden_in.shape
    channels = in_x_weight.shape[1]
    tp_count, dp_count, ctx_count = (lax.axis_size(a) for a in ("tp", "dp", "ctx"))
    dp_index, ctx_index, tp_index = (lax.axis_index(a) for a in ("dp", "ctx", "tp"))
    paired = dp_count == 2
    half = width // dp_count
    groups = 2
    fused = paired and ctx_count == 4 and tp_count == 4 and half == channels == length

    def turned(value, axis):
        if not paired:
            return value
        return jnp.concatenate(
            [half_of(value, dp_index, axis), half_of(value, 1 - dp_index, axis)], axis=axis
        )

    def joined(value, axis):
        if not paired:
            return lax.all_gather(value, "dp", axis=axis, tiled=True)
        other = swap_pairs(value, "dp", 1)
        return jnp.where(
            dp_index == 0,
            jnp.concatenate([value, other], axis=axis),
            jnp.concatenate([other, value], axis=axis),
        )

    def weight(own, axis, after):
        if not paired:
            return lax.all_gather(own, "dp", axis=axis, tiled=True), None
        bit = ctx_index % 2
        piece = half_of(own, bit)
        if after is not None:
            piece, _ = lax.optimization_barrier((piece, after))
        near = swap_pairs(piece, "dp", 1)
        far = swap_pairs(near, "ctx", 1)
        return jnp.concatenate([own, ordered(near, far, bit)], axis=axis), near

    small = jnp.concatenate(
        [conv_weight, conv_bias[None], dt_bias[None], skip_weight[None], a_log.T], axis=0
    )
    small = joined(small, 1).astype(F32)
    gain_full = joined(norm_gain, 0).astype(F32)
    w_proj = joined(x_weight, 0)
    w_step = joined(dt_weight, 0)
    w_inx, first = weight(in_x_weight, 0, None)
    w_inz, sent = weight(in_z_weight, 0, first)
    w_out, sent = weight(out_weight, 1, sent)
    gain_full = turned(gain_full, 0)
    taps_full = small[:K]
    conv_shift, step_bias, skip_full = small[K], small[K + 1], small[K + 2]
    decay_rate = -jnp.exp(small[K + 3 :])

    starts = piece_starts(seq_lengths[0], pack_order[0])
    positions = ctx_index * length + jnp.arange(length, dtype=jnp.int32)

    def piece(at):
        return jnp.sum((at[:, None] >= starts[None, :]).astype(jnp.int32), axis=1)

    piece_now = piece(positions)
    masks = [(piece(positions - back) == piece_now).astype(F32) for back in (3, 2, 1)]
    blocked = (1.0 - masks[2]) * FAR

    rows_all = turned(hidden_in, 1)
    grad_later = lax.optimization_barrier((out_grad, first))[0] if paired else out_grad
    grad_all = turned(grad_later, 1)
    rows_in = rows_all.astype(F32)
    inv_rms = lax.rsqrt(jnp.mean(rows_in * rows_in, axis=1, keepdims=True) + EPSILON)
    normed = (rows_in * inv_rms * gain_full).astype(BF16)
    inner_x = jnp.dot(normed, w_inx, preferred_element_type=F32).astype(BF16)
    halo = shifted(inner_x[length - (K - 1) :], "ctx", 1)
    extended = jnp.concatenate([halo, inner_x], axis=0).astype(F32)
    conv_pre = conv_shift[None, :] + taps_full[K - 1] * extended[K - 1 :]
    for tap in range(K - 1):
        conv_pre = conv_pre + taps_full[tap] * extended[tap : tap + length] * masks[tap][:, None]
    activated = jax.nn.silu(conv_pre).astype(BF16)
    projected = tp_sum(jnp.dot(activated, w_proj, preferred_element_type=F32))
    gate_z = jnp.dot(normed, w_inz, preferred_element_type=F32)
    d_gated = contract_last(grad_all, w_out)

    step_low = projected[:, :R].astype(BF16)
    step_pre = jnp.dot(step_low, w_step, preferred_element_type=F32) + step_bias
    step_size = jax.nn.softplus(step_pre)
    table = jnp.concatenate(
        [
            projected[:, R:],
            blocked[:, None],
            jnp.zeros((length, LANES - 2 * N - 1), F32),
        ],
        axis=1,
    )
    rate2 = decay_rate * LOG2E

    def entering(whole, rate):
        state, back, spent = whole[:N], whole[N : 2 * N], whole[2 * N : 2 * N + 1]
        h_in = jnp.zeros_like(state)
        c_in = jnp.zeros_like(back)
        below = jnp.zeros_like(spent)
        above = jnp.zeros_like(spent)
        distance = 1
        while distance < ctx_count:
            got = swap_pairs(jnp.concatenate([state, back, jnp.broadcast_to(spent, (8,) + spent.shape[1:])], axis=0), "ctx", distance)
            o_state, o_back, o_spent = got[:N], got[N : 2 * N], got[2 * N : 2 * N + 1]
            upper = (ctx_index // distance) % 2 == 1
            h_in = jnp.where(upper, jnp.exp2(rate * below) * o_state + h_in, h_in)
            c_in = jnp.where(upper, c_in, jnp.exp2(rate * above) * o_back + c_in)
            below = jnp.where(upper, below + o_spent, below)
            above = jnp.where(upper, above, above + o_spent)
            mine, other = jnp.exp2(rate * spent), jnp.exp2(rate * o_spent)
            state, back = (
                jnp.where(upper, mine * o_state + state, other * state + o_state),
                jnp.where(upper, o_back + other * back, back + mine * o_back),
            )
            spent = spent + o_spent
            distance *= 2
        return h_in, c_in

    *segs, whole = scan_totals(step_size, activated, d_gated, gate_z, rate2, table, groups)
    gated_t, gated, d_gate, d_pre, d_drive, rates_d, d_bc = scan_grads(
        step_size,
        step_pre,
        activated,
        d_gated,
        gate_z,
        skip_full[None],
        rate2,
        table,
        segs,
        entering(whole, rate2),
        groups,
    )
    rates_d = jnp.sum(rates_d, axis=0)
    g_log, g_skip, g_bias = rates_d[:N] * decay_rate, rates_d[N], rates_d[N + 1]
    g_step = contract_first(step_low, d_pre)

    def input_sum(cotangent):
        value = contract_first(normed, cotangent)
        if paired:
            value = turned(value, 0)
        value = lax.psum_scatter(value.astype(BF16), "dp", scatter_dimension=0, tiled=True)
        return lax.psum(value, "ctx").astype(F32)

    def output_sum(gated):
        value = contract_first(gated, grad_all)
        if paired:
            value = turned(value, 1)
        value = lax.psum_scatter(value.astype(BF16), "dp", scatter_dimension=1, tiled=True)
        return lax.psum(value, "ctx").astype(F32)

    if fused:
        padded = jnp.pad(jnp.stack(masks, axis=1), ((SEGS, SEGS), (0, 1)))
        before = jnp.pad(halo, ((2 * SEGS - (K - 1), 0), (0, 0)))
        taps = jnp.pad(jnp.concatenate([taps_full, conv_shift[None]]), ((0, SEGS - K - 1), (0, 0)))
        misc = jnp.pad(
            jnp.concatenate([g_bias[None], g_skip[None], g_log]), ((0, 3 * SEGS - N - 2), (0, 0))
        )
        s_out, s_z, s_x, small_sum, out_natural, grad_natural = finish(
            gated_t,
            gated,
            normed.T,
            d_gate,
            d_pre,
            d_drive,
            inner_x,
            before,
            w_inx,
            w_inz,
            w_out,
            hidden_in,
            out_grad,
            inv_rms,
            gain_full[None],
            padded,
            taps,
            w_step,
            jnp.pad(w_proj, ((0, 0), (0, 2 * LANES - R - 2 * N))),
            d_bc,
            misc,
            g_step,
        )
        small_sum = small_sum.astype(F32)
        steps_half = g_step.shape[0] // 2
        at = 4 * SEGS + R + 2 * N
        end = at + 2 * steps_half
        return (
            out_natural,
            grad_natural,
            jnp.concatenate(
                [
                    jnp.sum(small_sum[end : end + SEGS], axis=0),
                    jnp.sum(small_sum[end + SEGS :], axis=0),
                ]
            ),
            s_x.astype(F32),
            s_z.astype(F32),
            small_sum[:K],
            small_sum[K],
            small_sum[4 * SEGS : at].T,
            jnp.concatenate(
                [small_sum[at : at + steps_half], small_sum[at + steps_half : end]], axis=1
            ),
            small_sum[SEGS],
            small_sum[SEGS + 2 : SEGS + 2 + N].T,
            small_sum[SEGS + 1],
            s_out.astype(F32),
        )

    branch = jnp.dot(gated, w_out, preferred_element_type=F32)
    d_proj = tp_sum(
        jnp.concatenate([contract_last(d_pre, w_step), d_bc[:, : 2 * N]], axis=1)
    ).astype(BF16)

    quarter = length // tp_count
    own_row = tp_rows() * quarter
    own_in = lax.dynamic_slice_in_dim(rows_all, own_row, quarter, 0).astype(F32)
    own_grad = lax.dynamic_slice_in_dim(grad_all, own_row, quarter, 0).astype(F32)
    own_rms = lax.rsqrt(jnp.mean(own_in * own_in, axis=1, keepdims=True) + EPSILON)
    own_hat = own_in * own_rms

    def whole_rows(value):
        distance = tp_count // 2
        while distance >= 1:
            value = ordered(value, swap_pairs(value, "tp", distance), (tp_index // distance) % 2)
            distance //= 2
        if not paired:
            return value
        return ordered(value[:, :half], value[:, half:], dp_index, axis=1)

    out_natural = whole_rows((own_in + tp_scatter(branch)).astype(BF16))

    g_proj = contract_first(d_proj, activated)
    d_total = d_drive + contract_last(d_proj, w_proj)
    conv_sig = jax.nn.sigmoid(conv_pre)
    d_conv = d_total * conv_sig * (1.0 + conv_pre * (1.0 - conv_sig))
    g_shift = jnp.sum(d_conv, axis=0)
    g_taps = jnp.stack(
        [
            jnp.sum(d_conv * masks[tap][:, None] * extended[tap : tap + length], axis=0)
            for tap in range(K - 1)
        ]
        + [jnp.sum(d_conv * extended[K - 1 :], axis=0)],
        axis=0,
    )
    d_extended = jnp.pad(d_conv * taps_full[K - 1], ((K - 1, 0), (0, 0)))
    for tap in range(K - 1):
        d_extended = d_extended + jnp.pad(
            d_conv * masks[tap][:, None] * taps_full[tap], ((tap, K - 1 - tap), (0, 0))
        )
    returned = shifted(d_extended[: K - 1], "ctx", -1)
    d_inner = (
        d_extended[K - 1 :] + jnp.pad(returned, ((length - (K - 1), 0), (0, 0)))
    ).astype(BF16)
    packed = jnp.concatenate(
        [g_taps, g_shift[None], g_bias[None], g_skip[None], g_log, g_proj], axis=0
    )
    g_inx, g_inz, g_out = input_sum(d_inner), input_sum(d_gate), output_sum(gated)
    d_normed = tp_scatter(contract_last(d_inner, w_inx) + contract_last(d_gate, w_inz))
    g_gain = jnp.sum(d_normed * own_hat, axis=0)
    d_hat = d_normed * gain_full
    d_rows = own_grad + own_rms * (
        d_hat - own_hat * jnp.mean(d_hat * own_hat, axis=1, keepdims=True)
    )
    grad_natural = whole_rows(d_rows.astype(BF16))
    g_gain = turned(lax.psum(g_gain, ("ctx", "tp")), 0)
    g_gain = lax.psum_scatter(g_gain, "dp", scatter_dimension=0, tiled=True)
    packed = lax.psum(lax.psum_scatter(packed, "dp", scatter_dimension=1, tiled=True), "ctx")
    g_step = lax.psum(lax.psum_scatter(g_step, "dp", scatter_dimension=0, tiled=True), "ctx")
    return (
        out_natural,
        grad_natural,
        g_gain,
        g_inx,
        g_inz,
        packed[:K],
        packed[K],
        packed[K + 3 + N :].T,
        g_step,
        packed[K + 1],
        packed[K + 3 : K + 3 + N].T,
        packed[K + 2],
        g_out,
    )


def solution(mesh):
    in_specs = (
        P(("dp", "ctx"), None),
        P("dp", None),
        P("dp", None),
        P("dp"),
        P("dp", "tp"),
        P("dp", "tp"),
        P(None, ("tp", "dp")),
        P(("tp", "dp")),
        P(("tp", "dp"), None),
        P("dp", "tp"),
        P(("tp", "dp")),
        P(("tp", "dp"), None),
        P(("tp", "dp")),
        P("tp", "dp"),
        P(("dp", "ctx"), None),
    )
    out_specs = (
        P(("dp", "ctx"), None),
        P(("dp", "ctx"), None),
        P("dp"),
        P("dp", "tp"),
        P("dp", "tp"),
        P(None, ("tp", "dp")),
        P(("tp", "dp")),
        P(("tp", "dp"), None),
        P("dp", "tp"),
        P(("tp", "dp")),
        P(("tp", "dp"), None),
        P(("tp", "dp")),
        P("tp", "dp"),
    )
    return jax.shard_map(
        per_device, mesh=mesh, in_specs=in_specs, out_specs=out_specs, check_vma=False
    )
```

```python
import jax
import jax.numpy as jnp
from jax import lax
from jax.experimental import pallas as pl
from jax.experimental.pallas import tpu as pltpu
from jax.sharding import PartitionSpec as P

N = 16
R = 128
K = 4
ROW = 2048
MICRO = 2
EPSILON = 1e-05

LANES = 128
SEGS = 8
FAR = 1e30
LOG2E = 1.4426950408889634
LN2 = 0.6931471805599453
F32 = jnp.float32
BF16 = jnp.bfloat16


def contract_last(left, right):
    return lax.dot_general(left, right, (((1,), (1,)), ((), ())), preferred_element_type=F32)


def contract_first(left, right):
    return lax.dot_general(left, right, (((0,), (0,)), ((), ())), preferred_element_type=F32)


def shifted(value, axis, steps):
    count = lax.axis_size(axis)
    leading, last = (max(0, -steps), min(count, count - steps))
    return lax.ppermute(value, axis, [(source, source + steps) for source in range(leading, last)])


def piece_starts(lengths, arrangement):
    count = lengths.shape[0]
    ids = jnp.arange(count, dtype=jnp.int32)
    ordered = jnp.sum(jnp.where(arrangement[:, None] == ids[None, :], lengths[None, :], 0), axis=1)
    nat_start = jnp.cumsum(lengths) - lengths
    pack_start = jnp.cumsum(ordered) - ordered
    rows = jnp.arange(1, MICRO, dtype=jnp.int32) * ROW
    slot = jnp.sum((rows[:, None] >= pack_start[None, 1:]).astype(jnp.int32), axis=1)
    in_slot = slot[:, None] == ids[None, :]
    sequence = jnp.sum(jnp.where(in_slot, arrangement[None, :], 0), axis=1)
    begun = jnp.sum(jnp.where(in_slot, pack_start[None, :], 0), axis=1)
    source = (
        jnp.sum(jnp.where(sequence[:, None] == ids[None, :], nat_start[None, :], 0), axis=1)
        + rows
        - begun
    )
    return jnp.concatenate([nat_start, source])


def exact_parts(value):
    high = value.astype(BF16)
    rest = value - high.astype(F32)
    mid = rest.astype(BF16)
    return high, mid, (rest - mid.astype(F32)).astype(BF16)


def spread_columns(table_ref, out_ref, extra_ref, turned_ref, groups, steps):
    rows_of = SEGS * steps
    row = lax.broadcasted_iota(jnp.int32, (2 * LANES, 2 * LANES), 0) % LANES
    side = lax.broadcasted_iota(jnp.int32, (2 * LANES, 2 * LANES), 1) // LANES
    for g in range(groups):

        def one(i, _):
            turned_ref[pl.ds(pl.multiple_of(i * SEGS, SEGS), SEGS), :] = table_ref[
                pl.ds(g * rows_of + i, SEGS, stride=steps), :
            ]
            return 0

        lax.fori_loop(0, steps, one, 0, unroll=8)
        high, mid, low = exact_parts(turned_ref[0:rows_of, :])
        most = jnp.concatenate([high, mid], axis=1)
        for n in range(0, 2 * N + 1, 2):
            pick = (row == n + side).astype(F32).astype(BF16)
            value = jnp.dot(most, pick, preferred_element_type=F32)
            value = value + jnp.dot(low, pick[:LANES], preferred_element_type=F32)
            first = value[:, :LANES].reshape(steps, SEGS, LANES)
            if n < 2 * N:
                out_ref[g * steps : (g + 1) * steps, n] = first
                out_ref[g * steps : (g + 1) * steps, n + 1] = value[:, LANES:].reshape(
                    steps, SEGS, LANES
                )
            else:
                extra_ref[g * steps : (g + 1) * steps] = first


def silu_rows(left_ref, gate_ref, out_ref):
    strip = 128

    def one(r, _):
        at = pl.ds(pl.multiple_of(r * strip, strip), strip)
        gate = gate_ref[at, :]
        out_ref[at, :] = left_ref[at, :] * gate * jax.nn.sigmoid(gate)
        return 0

    lax.fori_loop(0, out_ref.shape[0] // strip, one, 0)


def totals_kernel(
    groups,
    steps,
    step_ref,
    act_ref,
    d_gated_ref,
    gate_ref,
    rate_ref,
    table_ref,
    seg_s_ref,
    seg_h_ref,
    seg_c_ref,
    whole_ref,
    bc_s,
    keep_s,
    act_s,
    dy_s,
):
    rows_of = SEGS * steps

    @pl.when(pl.program_id(0) == 0)
    def _():
        spread_columns(table_ref, bc_s, keep_s, act_s, groups, steps)

    act_s[...] = act_ref[...].astype(F32)
    silu_rows(d_gated_ref, gate_ref, dy_s)
    half = N
    zero = jnp.zeros((SEGS, LANES), F32)
    for g in range(groups):
        for lo in range(0, N, half):
            rates = [
                jnp.broadcast_to(rate_ref[lo + n : lo + n + 1, :], (SEGS, LANES))
                for n in range(half)
            ]

            def one(i, carry):
                total, state, reach, back = carry
                state, reach, back = list(state), list(reach), list(back)
                at = pl.ds(g * rows_of + i, SEGS, stride=steps)
                step, act, dy = step_ref[at, :], act_s[at, :], dy_s[at, :]
                gone = step + keep_s[g * steps + i]
                push = step * act
                for n in range(half):
                    decay = jnp.exp2(gone * rates[n])
                    state[n] = decay * state[n] + push * bc_s[g * steps + i, lo + n]
                    reach[n] = reach[n] * decay
                    back[n] = back[n] + reach[n] * (dy * bc_s[g * steps + i, N + lo + n])
                return (total + gone, tuple(state), tuple(reach), tuple(back))

            total, state, _, back = lax.fori_loop(
                0,
                steps,
                one,
                (zero, (zero,) * half, (jnp.ones((SEGS, LANES), F32),) * half, (zero,) * half),
                unroll=8,
            )
            if lo == 0:
                seg_s_ref[g * SEGS : (g + 1) * SEGS, :] = total
            for n in range(half):
                first = (g * N + lo + n) * SEGS
                seg_h_ref[first : first + SEGS, :] = state[n]
                seg_c_ref[first : first + SEGS, :] = back[n]
    rate = rate_ref[...]
    h = jnp.zeros((N, LANES), F32)
    c = jnp.zeros((N, LANES), F32)
    order = [(g, s) for g in range(groups) for s in range(SEGS)]
    gone = jnp.zeros((1, LANES), F32)
    for g, s in order:
        at = pl.ds(g * N * SEGS + s, N, stride=SEGS)
        spent = seg_s_ref[g * SEGS + s : g * SEGS + s + 1, :]
        h = jnp.exp2(rate * spent) * h + seg_h_ref[at, :]
        gone = gone + spent
    for g, s in order[::-1]:
        at = pl.ds(g * N * SEGS + s, N, stride=SEGS)
        spent = seg_s_ref[g * SEGS + s : g * SEGS + s + 1, :]
        c = jnp.exp2(rate * spent) * c + seg_c_ref[at, :]
    whole_ref[0:N, :] = h
    whole_ref[N : 2 * N, :] = c
    whole_ref[2 * N : 2 * N + SEGS, :] = jnp.broadcast_to(gone, (SEGS, LANES))


def grads_kernel(
    groups,
    steps,
    blocks,
    step_ref,
    pre_ref,
    act_ref,
    d_gated_ref,
    gate_ref,
    skip_ref,
    rate_ref,
    table_ref,
    seg_s_ref,
    seg_h_ref,
    seg_c_ref,
    h_in_ref,
    c_in_ref,
    gated_t_ref,
    gated_ref,
    d_gate_ref,
    d_pre_ref,
    drive_ref,
    d_rate_ref,
    d_bc_ref,
    bc_s,
    keep_s,
    act_s,
    enter_h,
    enter_c,
    decay_s,
    prior_s,
    sum_b,
    sum_c,
    dy_s,
    y_s,
    d_step_s,
    d_act_s,
):
    g, j = pl.program_id(0), pl.program_id(1)

    @pl.when(j == 0)
    def _():
        spread_columns(table_ref, bc_s, keep_s, act_s, 1, steps)
        sum_b[...] = jnp.zeros_like(sum_b)
        sum_c[...] = jnp.zeros_like(sum_c)

    rate = rate_ref[...]

    @pl.when(g == 0)
    def _():
        h = h_in_ref[...]
        c = c_in_ref[...]
        order = [(a, s) for a in range(groups) for s in range(SEGS)]
        for a, s in order:
            at = pl.ds(a * N * SEGS + s, N, stride=SEGS)
            spent = seg_s_ref[a * SEGS + s : a * SEGS + s + 1, :]
            enter_h.at[j][at, :] = h
            h = jnp.exp2(rate * spent) * h + seg_h_ref[at, :]
        for a, s in order[::-1]:
            at = pl.ds(a * N * SEGS + s, N, stride=SEGS)
            spent = seg_s_ref[a * SEGS + s : a * SEGS + s + 1, :]
            enter_c.at[j][at, :] = c
            c = jnp.exp2(rate * spent) * c + seg_c_ref[at, :]

    act_s[...] = act_ref[...].astype(F32)
    silu_rows(d_gated_ref, gate_ref, dy_s)
    first = g * N * SEGS

    def rate_row(n):
        return jnp.broadcast_to(rate_ref[n : n + 1, :], (SEGS, LANES))

    def ahead(i, state):
        state = list(state)
        at = pl.ds(i, SEGS, stride=steps)
        step, act, dy = step_ref[at, :], act_s[at, :], dy_s[at, :]
        gone = step + keep_s[i]
        push = step * act
        y = jnp.zeros((SEGS, LANES), F32)
        for n in range(N):
            decay = jnp.exp2(gone * rate_row(n))
            prior = decay * state[n]
            state[n] = prior + push * bc_s[i, n]
            decay_s[i, n] = decay
            prior_s[i, n] = prior
            y = y + state[n] * bc_s[i, N + n]
            sum_c[i, n] += state[n] * dy
        y_s[at, :] = y
        return tuple(state)

    def enter(ref, n):
        return ref[j, pl.ds(pl.multiple_of(first + n * SEGS, SEGS), SEGS), :]

    lax.fori_loop(0, steps, ahead, tuple(enter(enter_h, n) for n in range(N)), unroll=8)

    def back(k, carry):
        i = steps - 1 - k
        carried, d_rate = list(carry[0]), list(carry[1])
        at = pl.ds(i, SEGS, stride=steps)
        step, act, dy = step_ref[at, :], act_s[at, :], dy_s[at, :]
        push = step * act
        along = jnp.zeros((SEGS, LANES), F32)
        d_step = jnp.zeros((SEGS, LANES), F32)
        for n in range(N):
            grad = dy * bc_s[i, N + n] + carried[n]
            along = along + grad * bc_s[i, n]
            log_grad = grad * prior_s[i, n]
            d_step = d_step + log_grad * rate_row(n)
            d_rate[n] = d_rate[n] + log_grad * step
            carried[n] = grad * decay_s[i, n]
            sum_b[i, n] += grad * push
        d_step_s[at, :] = d_step * LN2 + along * act
        d_act_s[at, :] = along * step
        return (tuple(carried), tuple(d_rate))

    zero = jnp.zeros((SEGS, LANES), F32)
    _, d_rate = lax.fori_loop(
        0, steps, back, (tuple(enter(enter_c, n) for n in range(N)), (zero,) * N), unroll=8
    )
    for n in range(N):
        d_rate_ref[0, n : n + 1, :] = jnp.sum(d_rate[n], axis=0, keepdims=True)

    strip = 64

    def close(r, sums):
        at = pl.ds(pl.multiple_of(r * strip, strip), strip)
        gate, d_gated, act, dy = gate_ref[at, :], d_gated_ref[at, :], act_s[at, :], dy_s[at, :]
        skip = skip_ref[...]
        sig = jax.nn.sigmoid(gate)
        scan_out = y_s[at, :] + skip * act
        gated = scan_out * gate * sig
        y_s[at, :] = gated
        gated_ref[at, :] = gated.astype(BF16)
        d_gate_ref[at, :] = (d_gated * scan_out * sig * (1.0 + gate * (1.0 - sig))).astype(BF16)
        d_pre = (d_step_s[at, :] * jax.nn.sigmoid(pre_ref[at, :])).astype(BF16)
        d_pre_ref[at, :] = d_pre
        drive_ref[at, :] = d_act_s[at, :] + dy * skip

        def fold(value):
            return jnp.sum(value.reshape(strip // SEGS, SEGS, LANES), axis=0)

        return sums[0] + fold(dy * act), sums[1] + fold(d_pre.astype(F32))

    g_skip, g_bias = lax.fori_loop(0, y_s.shape[0] // strip, close, (zero, zero))
    d_rate_ref[0, N : N + 1, :] = jnp.sum(g_skip, axis=0, keepdims=True)
    d_rate_ref[0, N + 1 : N + 2, :] = jnp.sum(g_bias, axis=0, keepdims=True)
    gated_t_ref[...] = y_s[...].T.astype(BF16)

    @pl.when(j == blocks - 1)
    def _():
        column = lax.broadcasted_iota(jnp.int32, (2 * LANES, LANES), 1)
        total = jnp.zeros((steps * SEGS, LANES), F32)
        for n in range(N):
            for ref, at in ((sum_b, n), (sum_c, N + n)):
                pick = (column == at).astype(F32).astype(BF16)
                value = exact_parts(ref[:, n].reshape(steps * SEGS, LANES))
                total = total + jnp.dot(
                    jnp.concatenate(value[:2], axis=1), pick, preferred_element_type=F32
                )
        act_s[...] = total

        def put(i, _):
            d_bc_ref[pl.ds(i, SEGS, stride=steps), :] = act_s[
                pl.ds(pl.multiple_of(i * SEGS, SEGS), SEGS), :
            ]
            return 0

        lax.fori_loop(0, steps, put, 0, unroll=8)


def scan_totals(step_size, activated, d_gated, gate_z, rate2, table, groups):
    length, channels = step_size.shape
    steps = length // (groups * SEGS)
    blocks = channels // LANES
    tall = pl.BlockSpec((length, LANES), lambda j: (0, j))
    rows = groups * N * SEGS
    return pl.pallas_call(
        lambda *refs: totals_kernel(groups, steps, *refs),
        grid=(blocks,),
        in_specs=[
            tall,
            tall,
            tall,
            tall,
            pl.BlockSpec((N, LANES), lambda j: (0, j)),
            pl.BlockSpec((length, LANES), lambda j: (0, 0)),
        ],
        out_specs=[
            pl.BlockSpec((groups * SEGS, LANES), lambda j: (0, j)),
            pl.BlockSpec((rows, LANES), lambda j: (0, j)),
            pl.BlockSpec((rows, LANES), lambda j: (0, j)),
            pl.BlockSpec((2 * N + SEGS, LANES), lambda j: (0, j)),
        ],
        out_shape=[
            jax.ShapeDtypeStruct((groups * SEGS, channels), F32),
            jax.ShapeDtypeStruct((rows, channels), F32),
            jax.ShapeDtypeStruct((rows, channels), F32),
            jax.ShapeDtypeStruct((2 * N + SEGS, channels), F32),
        ],
        scratch_shapes=[
            pltpu.VMEM((groups * steps, 2 * N, SEGS, LANES), F32),
            pltpu.VMEM((groups * steps, SEGS, LANES), F32),
            pltpu.VMEM((length, LANES), F32),
            pltpu.VMEM((length, LANES), F32),
        ],
        compiler_params=pltpu.CompilerParams(
            dimension_semantics=("arbitrary",), vmem_limit_bytes=40 << 20
        ),
        cost_estimate=pl.CostEstimate(
            flops=length * channels * N * 3000,
            bytes_accessed=length * channels * 14,
            transcendentals=length * channels * N,
        ),
        name="scan_totals",
    )(step_size, activated, d_gated, gate_z, rate2, table)


def scan_grads(
    step_size, step_pre, activated, d_gated, gate_z, skip, rate2, table, segs, enter, groups
):
    length, channels = step_size.shape
    steps = length // (groups * SEGS)
    blocks = channels // LANES
    share = length // groups
    tall = pl.BlockSpec((share, LANES), lambda g, j: (g, j))
    one = pl.BlockSpec((share, LANES), lambda g, j: (g, 0))
    rows = groups * N * SEGS

    def wide(height):
        return pl.BlockSpec((height, LANES), lambda g, j: (0, j))

    def shape(dtype, *dims):
        return jax.ShapeDtypeStruct(dims, dtype)

    grid_spec = pl.GridSpec(
        grid=(groups, blocks),
        in_specs=[tall] * 5
        + [wide(1), wide(N), one]
        + [wide(groups * SEGS), wide(rows), wide(rows), wide(N), wide(N)],
        out_specs=[pl.BlockSpec((LANES, share), lambda g, j: (j, g))]
        + [tall] * 4
        + [pl.BlockSpec((1, 3 * SEGS, LANES), lambda g, j: (g, 0, j)), one],
        scratch_shapes=[
            pltpu.VMEM((steps, 2 * N, SEGS, LANES), F32),
            pltpu.VMEM((steps, SEGS, LANES), F32),
            pltpu.VMEM((share, LANES), F32),
            pltpu.VMEM((blocks, rows, LANES), F32),
            pltpu.VMEM((blocks, rows, LANES), F32),
            pltpu.VMEM((steps, N, SEGS, LANES), F32),
            pltpu.VMEM((steps, N, SEGS, LANES), F32),
            pltpu.VMEM((steps, N, SEGS, LANES), F32),
            pltpu.VMEM((steps, N, SEGS, LANES), F32),
            pltpu.VMEM((share, LANES), F32),
            pltpu.VMEM((share, LANES), F32),
            pltpu.VMEM((share, LANES), F32),
            pltpu.VMEM((share, LANES), F32),
        ],
    )
    return pl.pallas_call(
        lambda *refs: grads_kernel(groups, steps, blocks, *refs),
        grid_spec=grid_spec,
        out_shape=[
            shape(BF16, channels, length),
            shape(BF16, length, channels),
            shape(BF16, length, channels),
            shape(BF16, length, channels),
            shape(F32, length, channels),
            shape(F32, groups, 3 * SEGS, channels),
            shape(F32, length, LANES),
        ],
        compiler_params=pltpu.CompilerParams(
            dimension_semantics=("arbitrary", "arbitrary"), vmem_limit_bytes=48 << 20
        ),
        cost_estimate=pl.CostEstimate(
            flops=length * channels * N * 6000,
            bytes_accessed=length * channels * 30,
            transcendentals=length * channels * N,
        ),
        name="scan_grads",
    )(step_size, step_pre, activated, d_gated, gate_z, skip, rate2, table, *segs, *enter)


MESH = pl.DeviceIdType.MESH
CHUNK = 128
AHEAD = 2
LATE = 2
WIDE = 256


def finish_kernel(
    parts,
    gated_t_hbm,
    gated_hbm,
    normed_hbm,
    d_gate_hbm,
    d_pre_hbm,
    drive_hbm,
    inner_hbm,
    halo_hbm,
    w_inx_hbm,
    w_inz_hbm,
    w_out_hbm,
    x_hbm,
    dy_hbm,
    rms_ref,
    gain_ref,
    masks_ref,
    taps_ref,
    w_step_ref,
    w_proj_ref,
    d_bc_ref,
    misc_ref,
    g_step_ref,
    sums_out,
    sums_z,
    sums_x,
    small_ref,
    out_hbm,
    grad_hbm,
    left,
    right,
    w_x,
    w_z,
    x_cols,
    y_out,
    y_in,
    a_in,
    b_in,
    line,
    first,
    held,
    total,
    core_out,
    core_in,
    kept,
    x_out,
    x_in,
    rows_x,
    rows_dy,
    final,
    passed,
    gain_sum,
    gain_core,
    gain_x,
    gain_out,
    s_out,
    s_in,
    s_a,
    s_b,
    s_line,
    p_out,
    p_in,
    q_out,
    q_in,
    turned_p,
    drive,
    inner_low,
    inner,
    active,
    pack,
    tail,
    halo_out,
    halo_in,
    load_sem,
    w_sem,
    y_sem,
    a_sem,
    b_sem,
    c_sem,
    out_sem,
    tp_sem,
    gain_sem,
    final_sem,
    small_sem,
    chain_sem,
    proj_sem,
    halo_sem,
):
    rows, width = x_hbm.shape
    half = width // 2
    dp, z, tp = lax.axis_index("dp"), lax.axis_index("ctx"), lax.axis_index("tp")
    core, x_bit = tp % 2, tp // 2
    near, across = tp + 1 - 2 * core, (tp + 2) % 4
    ends = (z == 0) | (z == 3)
    middle = (z == 1) | (z == 2)
    inward, twin, outward = z // 2 + 1, 3 - z, (z // 2) * 3

    def load(source, target, at):
        copy = pltpu.make_async_copy(source, target, load_sem.at[at])
        copy.start()
        return copy

    quarter = rows // 4
    own_row = pl.multiple_of(core * (rows // 2) + x_bit * quarter, quarter)
    got_left = load(gated_t_hbm, left.at[0], 1)
    mine = pl.multiple_of(dp * half, half)
    away = pl.multiple_of((1 - dp) * half, half)
    got_other = load(dy_hbm.at[:, pl.ds(away, half)], right.at[1], 2)
    got_pre = load(d_pre_hbm, right.at[3], 0)
    others = [
        load(dy_hbm.at[:, pl.ds(mine, half)], right.at[0], 3),
        load(normed_hbm.at[pl.ds(0, half), :], left.at[1], 4),
        load(normed_hbm.at[pl.ds(half, half), :], left.at[2], 5),
        load(d_gate_hbm, right.at[2], 6),
        load(x_hbm.at[pl.ds(own_row, quarter), pl.ds(mine, half)], rows_x.at[:, pl.ds(0, half)], 7),
        load(dy_hbm.at[pl.ds(own_row, quarter), pl.ds(mine, half)], rows_dy.at[:, pl.ds(0, half)], 8),
        load(
            x_hbm.at[pl.ds(own_row, quarter), pl.ds(away, half)],
            rows_x.at[:, pl.ds(half, half)],
            16,
        ),
        load(
            dy_hbm.at[pl.ds(own_row, quarter), pl.ds(away, half)],
            rows_dy.at[:, pl.ds(half, half)],
            17,
        ),
    ]

    barrier = pltpu.get_barrier_semaphore()
    for peer in ({"tp": near}, {"tp": across}, {"dp": 1 - dp}):
        pl.semaphore_signal(barrier, inc=1, device_id=peer, device_id_type=MESH)

    @pl.when(ends)
    def _():
        pl.semaphore_signal(barrier, inc=1, device_id={"ctx": inward}, device_id_type=MESH)
        pl.semaphore_wait(barrier, 4)

    @pl.when(middle)
    def _():
        pl.semaphore_signal(barrier, inc=1, device_id={"ctx": twin}, device_id_type=MESH)
        pl.semaphore_signal(barrier, inc=1, device_id={"ctx": outward}, device_id_type=MESH)
        pl.semaphore_wait(barrier, 5)

    def remote(source, target, sems, at, peer):
        return pltpu.make_async_remote_copy(
            src_ref=source,
            dst_ref=target,
            send_sem=sems.at[0, at],
            recv_sem=sems.at[1, at],
            device_id=peer,
            device_id_type=MESH,
        )

    per_weight, pairs = parts // 3, parts // 2

    def chunk(k):
        return k // per_weight, pl.multiple_of(k % per_weight * CHUNK, CHUNK)

    def product(slot_l, slot_r, column):
        return jnp.dot(
            left[slot_l], right[slot_r, :, pl.ds(column, 2 * CHUNK)], preferred_element_type=F32
        )

    def y_copy(k):
        return remote(y_out.at[k % 6], y_in.at[k % 8], y_sem, k, {"dp": 1 - dp})

    def a_copy(k):
        return remote(line.at[k % 4], a_in.at[k % 12], a_sem, k, {"ctx": inward})

    def b_copy(k):
        return remote(line.at[k % 4], b_in.at[k % 4], b_sem, k, {"ctx": twin})

    sums = (sums_out, sums_z, sums_x)

    def far_copy(k, ref):
        spot = ref.at[:, pl.ds(chunk(k)[1], CHUNK)]
        return remote(total.at[k % 4], spot, c_sem, k, {"ctx": outward})

    def own_copy(k, ref):
        spot = ref.at[:, pl.ds(chunk(k)[1], CHUNK)]
        return pltpu.make_async_copy(total.at[k % 4], spot, out_sem.at[k])

    def give_c(k, start):
        for w, ref in enumerate(sums):

            @pl.when(k // per_weight == w)
            def _():
                far, own = far_copy(k, ref), own_copy(k, ref)
                if start:
                    far.start()
                    own.start()
                else:
                    far.wait_send()
                    own.wait()

    def wait_c(k):
        far_copy(k, sums_out).wait_recv()

    def pair(p):
        w, column = chunk(2 * p)
        return w, pl.multiple_of(column, 2 * CHUNK)

    def send_y(k):
        @pl.when(k % 2 == 0)
        def _():
            w, column = pair(k // 2)
            up = (w + 1) // 2

            @pl.when(k >= 6)
            def _():
                y_copy(k - 6).wait_send()
                y_copy(k - 5).wait_send()

            value = product(2 * up, w + 1, column).astype(BF16)
            y_out[k % 6] = value[:, :CHUNK]
            y_out[(k + 1) % 6] = value[:, CHUNK:]

        y_copy(k).start()

    def take_y(k):
        @pl.when(k % 2 == 0)
        def _():
            w, column = pair(k // 2)
            up = (w + 1) // 2
            value = product(up, w + up, column)
            held[0] = value[:, :CHUNK]
            held[1] = value[:, CHUNK:]

        y_copy(k).wait_recv()
        value = held[k % 2] + y_in[k % 8].astype(F32)

        @pl.when(ends)
        def _():
            @pl.when(k >= 4)
            def _():
                a_copy(k - 4).wait_send()

            @pl.when(k >= 12)
            def _():
                wait_c(k - 12)

            line[k % 4] = value.astype(BF16)
            a_copy(k).start()

        @pl.when(middle)
        def _():
            first[k % 2] = value

    def take_a(k):
        @pl.when(middle)
        def _():
            @pl.when(k >= 4)
            def _():
                b_copy(k - 4).wait_send()

            a_copy(k).wait_recv()
            line[k % 4] = (first[k % 2] + a_in[k % 12].astype(F32)).astype(BF16)
            b_copy(k).start()

    def take_b(k):
        @pl.when(middle)
        def _():
            @pl.when(k >= 4)
            def _():
                give_c(k - 4, False)

            b_copy(k).wait_recv()
            total[k % 4] = (line[k % 4].astype(F32) + b_in[k % 4].astype(F32)).astype(BF16)
            give_c(k, True)

    def tick(k, _):
        @pl.when((k >= 2 * LATE) & (k < parts + 2 * LATE))
        def _():
            take_b(k - 2 * LATE)

        @pl.when((k >= LATE) & (k < parts + LATE))
        def _():
            take_a(k - LATE)

        @pl.when(k < parts)
        def _():
            take_y(k)

        @pl.when(k + AHEAD < parts)
        def _():
            send_y(k + AHEAD)

        return 0

    def ticks(begin, end):
        lax.fori_loop(begin, end, tick, 0)

    got_left.wait()
    got_other.wait()
    for k in range(AHEAD):
        send_y(jnp.int32(k))
    got_pre.wait()
    p_out[:, :LANES] = contract_last(right[3], w_step_ref[...]).astype(BF16)
    p_out[:, LANES:] = d_bc_ref[...].astype(BF16)
    p_copy = remote(p_out, p_in, proj_sem, 0, {"tp": near})
    p_copy.start()
    got_gated = load(gated_hbm, right.at[3], 0)
    p_copy.wait_recv()
    q_out[...] = (p_out[...].astype(F32) + p_in[...].astype(F32)).astype(BF16)
    q_copy = remote(q_out, q_in, proj_sem, 1, {"tp": across})
    q_copy.start()

    block = w_x.shape[0]
    send_row = pl.multiple_of((1 - core) * (rows // 2), rows // 2)
    keep_row = pl.multiple_of(core * (rows // 2), rows // 2)
    give = pl.multiple_of((1 - x_bit) * quarter, quarter)
    have = pl.multiple_of(x_bit * quarter, quarter)

    got_gated.wait()

    def out_columns(d, _):
        at = pl.multiple_of(d * block, block)
        copy = pltpu.make_async_copy(w_out_hbm.at[:, pl.ds(at, block)], x_cols, w_sem.at[0])
        copy.start()
        copy.wait()
        core_out[:, pl.ds(at, block)] = jnp.dot(
            right[3, pl.ds(send_row, rows // 2), :], x_cols[...], preferred_element_type=F32
        ).astype(BF16)
        kept[:, pl.ds(at, block)] = jnp.dot(
            right[3, pl.ds(keep_row, rows // 2), :], x_cols[...], preferred_element_type=F32
        ).astype(BF16)
        return 0

    lax.fori_loop(0, width // block, out_columns, 0)
    core_copy = remote(core_out, core_in, tp_sem, 0, {"tp": near})
    core_copy.start()

    def chain_loads(q):
        at = pl.ds(q * WIDE, WIDE)
        return (
            pltpu.make_async_copy(
                drive_hbm.at[:, at], drive.at[pl.ds(SEGS, rows), :], chain_sem.at[0]
            ),
            pltpu.make_async_copy(
                inner_hbm.at[:, at], inner_low.at[pl.ds(2 * SEGS, rows), :], chain_sem.at[1]
            ),
            pltpu.make_async_copy(
                halo_hbm.at[:, at], inner_low.at[pl.ds(0, 2 * SEGS), :], chain_sem.at[2]
            ),
        )

    for copy in chain_loads(0):
        copy.start()
    for copy in others:
        copy.wait()

    ticks(0, 2)

    core_copy.wait_recv()

    def to_across():
        x_out[...] = (
            kept[pl.ds(give, quarter), :].astype(F32) + core_in[pl.ds(give, quarter), :].astype(F32)
        ).astype(BF16)

    to_across()
    x_copy = remote(x_out, x_in, tp_sem, 1, {"tp": across})
    x_copy.start()

    q_copy.wait_recv()
    projected = q_out[...].astype(F32) + q_in[...].astype(F32)
    p_copy.wait_send()
    p_out[...] = projected.astype(BF16)
    turned_p[...] = projected.T.astype(BF16)

    zeros = jnp.zeros((SEGS, WIDE), F32)
    strip = 64
    pad = 2 * SEGS
    drive[0:SEGS, :] = zeros
    drive[rows + SEGS :, :] = zeros

    def chain(q):
        cut = slice(q * WIDE, (q + 1) * WIDE)
        for copy in chain_loads(q):
            copy.wait()
        inner[...] = inner_low[...].astype(F32)
        taps = [taps_ref[i : i + 1, cut] for i in range(K + 1)]

        def down(r, sums):
            at = pl.multiple_of(r * strip, strip)
            mask = masks_ref[pl.ds(at + SEGS, strip), :]
            valid = [mask[:, i : i + 1] for i in range(K - 1)]
            near_rows = inner[pl.ds(at, strip + pad), :]
            moved = [near_rows[pad - (K - 1) + i :][:strip] for i in range(K)]
            moved = [moved[i] * valid[i] for i in range(K - 1)] + moved[K - 1 :]
            pre = taps[K] + taps[K - 1] * moved[K - 1]
            for i in range(K - 1):
                pre = pre + taps[i] * moved[i]
            sig = jax.nn.sigmoid(pre)
            active[pl.ds(at, strip), :] = (pre * sig).astype(BF16)
            whole = drive[pl.ds(at + SEGS, strip), :] + contract_last(
                p_out[pl.ds(at, strip), :], w_proj_ref[cut, :]
            )
            grad = whole * sig * (1.0 + pre * (1.0 - sig))
            drive[pl.ds(at + SEGS, strip), :] = grad

            def fold(value):
                return jnp.sum(value.reshape(strip // SEGS, SEGS, WIDE), axis=0)

            terms = [grad * m for m in moved] + [grad]
            return tuple(s + fold(t) for s, t in zip(sums, terms))

        sums_q = lax.fori_loop(0, rows // strip, down, (zeros,) * (K + 1))
        for i in range(K + 1):
            pack[i : i + 1, cut] = jnp.sum(sums_q[i], axis=0, keepdims=True)

        def spread(base, size):
            grads = drive[pl.ds(base + SEGS, size + SEGS), :]
            mask = masks_ref[pl.ds(base + SEGS, size + SEGS), :]
            value = grads[:size] * taps[K - 1]
            for back in range(1, K):
                valid = grads * mask[:, K - 1 - back : K - back]
                value = value + valid[back : back + size] * taps[K - 1 - back]
            return value

        def up(r, _):
            at = pl.multiple_of(r * strip, strip)
            right[3, pl.ds(at, strip), cut] = spread(at, strip).astype(BF16)
            return 0

        lax.fori_loop(0, rows // strip, up, 0)
        tail[:, cut] = spread(rows - pad, pad)
        halo_out[:, cut] = spread(-SEGS, SEGS)
        pack[4 * SEGS : 4 * SEGS + R + 2 * N, cut] = jnp.dot(
            turned_p[...], active[...], preferred_element_type=F32
        )[: R + 2 * N]

    for q in range(rows // WIDE):
        chain(q)
        if q + 1 < rows // WIDE:
            for copy in chain_loads(q + 1):
                copy.start()
            ticks(2 * q + 2, 2 * q + 4)
    halo_copy = remote(halo_out, halo_in, halo_sem, 0, {"ctx": jnp.maximum(z - 1, 0)})

    @pl.when(z > 0)
    def _():
        halo_copy.start()

    ticks(8, 10)

    def gather(ref, source, base):
        copies = []
        for side in range(2):
            place = pl.multiple_of((dp + side - 2 * dp * side) * half, half)
            spot = ref.at[pl.ds(own_row, quarter), pl.ds(place, half)]
            piece = source.at[:, pl.ds(side * half, half)]
            for p, peer in enumerate((across, near)):
                copies.append(remote(piece, spot, final_sem, base + 2 * p + side, {"tp": peer}))
            copies.append(pltpu.make_async_copy(piece, spot, load_sem.at[9 + base // 2 + side]))
        for copy in copies:
            copy.start()
        return copies

    def forward(ref, copies, base):
        copies[0].wait_recv()
        copies[3].wait_recv()
        row = pl.multiple_of(core * (rows // 2) + (1 - x_bit) * quarter, quarter)
        spot = ref.at[pl.ds(row, quarter), :]
        fetch = pltpu.make_async_copy(spot, passed, load_sem.at[15])
        fetch.start()
        fetch.wait()
        copy = remote(passed, spot, final_sem, base + 4, {"tp": near})
        copy.start()
        return copy

    def finished(copies, last):
        for k, copy in enumerate(copies):
            if k in (0, 3):
                copy.wait_send()
            else:
                copy.wait()
        last.wait()

    x_copy.wait_recv()

    def summed_rows():
        return (
            kept[pl.ds(have, quarter), :].astype(F32)
            + core_in[pl.ds(have, quarter), :].astype(F32)
            + x_in[...].astype(F32)
        )

    final[...] = (rows_x[...].astype(F32) + summed_rows()).astype(BF16)
    out_copies = gather(out_hbm, final, 0)

    @pl.when(z < 3)
    def _():
        halo_copy.wait_recv()
        tail[SEGS:, :] = tail[SEGS:, :] + halo_in[...]

    right[3, rows - pad :, :] = tail[...].astype(BF16)

    ticks(10, 12)

    core_copy.wait_send()
    x_copy.wait_send()

    def columns(d, _):
        at = pl.multiple_of(d * block, block)
        copies = [
            pltpu.make_async_copy(w_inx_hbm.at[pl.ds(at, block), :], w_x, w_sem.at[0]),
            pltpu.make_async_copy(w_inz_hbm.at[pl.ds(at, block), :], w_z, w_sem.at[1]),
            pltpu.make_async_copy(
                x_hbm.at[:, pl.ds(pl.multiple_of((at + dp * half) % width, block), block)],
                x_cols,
                w_sem.at[2],
            ),
        ]
        for copy in copies:
            copy.start()
        for copy in copies:
            copy.wait()
        sums_d = jnp.zeros((SEGS, block), F32)
        for row, keep in ((send_row, False), (keep_row, True)):
            span = pl.ds(row, rows // 2)
            value = contract_last(right[3, span, :], w_x[...])
            value = value + contract_last(right[2, span, :], w_z[...])
            hat = x_cols[span, :].astype(F32) * rms_ref[span, :]
            sums_d = sums_d + jnp.sum(
                (value * hat).reshape(rows // 2 // SEGS, SEGS, block), axis=0
            )
            target = kept if keep else core_out
            target[:, pl.ds(at, block)] = value.astype(BF16)
        gain_sum[:, pl.ds(at, block)] = sums_d
        return 0

    for d in range(width // block):
        columns(d, 0)
        ticks(12 + d, 13 + d)
    gain_copy = remote(gain_sum, gain_core, gain_sem, 0, {"tp": near})
    gain_copy.start()
    gain_copy.wait_recv()
    core_again = remote(core_out, core_in, tp_sem, 2, {"tp": near})
    core_again.start()
    gain_out[...] = gain_sum[...] + gain_core[...]
    gain_across = remote(gain_out, gain_x, gain_sem, 1, {"tp": across})
    gain_across.start()

    ticks(16, 17)

    core_again.wait_recv()
    to_across()
    gain_across.wait_recv()
    x_again = remote(x_out, x_in, tp_sem, 3, {"tp": across})
    x_again.start()

    ticks(17, 18)

    both = gain_out[...] + gain_x[...]
    fine = half // 2
    steps_half = g_step_ref.shape[0] // 2
    base = 4 * SEGS + R + 2 * N
    pack[K + 1 : SEGS, :] = jnp.zeros((SEGS - K - 1, 2 * fine), F32)
    pack[SEGS : 4 * SEGS, :] = misc_ref[...]

    def small_rows(index, lanes):
        column = pl.multiple_of(index * fine, fine)
        row = pl.multiple_of(index * steps_half, steps_half)
        return jnp.concatenate(
            [
                pack[:, pl.ds(column, fine)],
                g_step_ref[pl.ds(row, steps_half), :fine],
                g_step_ref[pl.ds(row, steps_half), fine:],
                both[:, lanes : lanes + fine],
                both[:, lanes + fine : lanes + 2 * fine],
            ],
            axis=0,
        )

    s_out[...] = small_rows(1 - dp, half).astype(BF16)
    small_y = remote(s_out, s_in, small_sem, 0, {"dp": 1 - dp})
    small_y.start()
    out_last = forward(out_hbm, out_copies, 0)

    ticks(18, 20)

    x_again.wait_recv()
    r_own = rms_ref[pl.ds(own_row, quarter), :]
    d_normed = summed_rows()
    hat = rows_x[...].astype(F32) * r_own
    d_hat = d_normed * gain_ref[...]
    mean = jnp.sum(d_hat * hat, axis=1, keepdims=True) * (1.0 / width)
    rows_dy[...] = (rows_dy[...].astype(F32) + r_own * (d_hat - hat * mean)).astype(BF16)
    grad_copies = gather(grad_hbm, rows_dy, 6)

    ticks(20, 21)

    small_y.wait_recv()
    s_keep = small_rows(dp, 0) + s_in[...].astype(F32)
    small_a = remote(s_line, s_a, small_sem, 1, {"ctx": inward})
    small_b = remote(s_line, s_b, small_sem, 2, {"ctx": twin})
    small_c = remote(small_ref, small_ref, small_sem, 3, {"ctx": outward})

    @pl.when(ends)
    def _():
        s_line[...] = s_keep.astype(BF16)
        small_a.start()

    @pl.when(middle)
    def _():
        small_a.wait_recv()
        s_line[...] = (s_keep + s_a[...].astype(F32)).astype(BF16)
        small_b.start()

    ticks(21, 22)

    finished(out_copies, out_last)
    grad_last = forward(grad_hbm, grad_copies, 6)

    @pl.when(middle)
    def _():
        small_b.wait_recv()
        small_ref[...] = (s_line[...].astype(F32) + s_b[...].astype(F32)).astype(BF16)
        small_c.start()

    ticks(22, parts + 2 * LATE)

    for k in range(parts - 6, parts):
        y_copy(k).wait_send()

    @pl.when(ends)
    def _():
        for k in range(parts - 4, parts):
            a_copy(k).wait_send()
        for k in range(parts - 12, parts):
            wait_c(k)
        small_a.wait_send()
        small_c.wait_recv()

    @pl.when(middle)
    def _():
        for k in range(parts - 4, parts):
            b_copy(k).wait_send()
            far_copy(k, sums_x).wait_send()
            own_copy(k, sums_x).wait()
        small_b.wait_send()
        small_c.wait_send()

    @pl.when(z > 0)
    def _():
        halo_copy.wait_send()

    q_copy.wait_send()
    core_again.wait_send()
    x_again.wait_send()
    gain_copy.wait_send()
    gain_across.wait_send()
    small_y.wait_send()
    finished(grad_copies, grad_last)


def finish(
    gated_t, gated, normed_t, d_gate, d_pre, drive, inner, halo, w_inx, w_inz, w_out, x_all, dy_all,
    rms, gain, masks, taps, w_step, w_proj, d_bc, misc, g_step,
):
    rows, width = x_all.shape
    channels = w_inx.shape[1]
    parts = 3 * (channels // CHUNK)
    half = width // 2
    small = 4 * SEGS + R + 2 * N + g_step.shape[0] + 2 * SEGS
    fine = half // 2
    block = 512
    hbm = pl.BlockSpec(memory_space=pl.ANY)
    vmem = pl.BlockSpec(memory_space=pltpu.VMEM)
    dma = pltpu.SemaphoreType.DMA
    piece = (half, CHUNK)
    quarter = rows // 4

    def low(*shape):
        return pltpu.VMEM(shape, BF16)

    def full(*shape):
        return pltpu.VMEM(shape, F32)

    return pl.pallas_call(
        lambda *refs: finish_kernel(parts, *refs),
        in_specs=[hbm] * 13 + [vmem] * 9,
        out_specs=[hbm, hbm, hbm, vmem, hbm, hbm],
        out_shape=[jax.ShapeDtypeStruct((half, channels), BF16)] * 3
        + [
            jax.ShapeDtypeStruct((small, fine), BF16),
            jax.ShapeDtypeStruct((rows, width), BF16),
            jax.ShapeDtypeStruct((rows, width), BF16),
        ],
        scratch_shapes=[
            low(3, half, rows),
            low(4, rows, channels),
            low(block, channels),
            low(block, channels),
            low(rows, block),
            low(6, *piece),
            low(8, *piece),
            low(12, *piece),
            low(4, *piece),
            low(4, *piece),
            full(2, *piece),
            full(2, *piece),
            low(4, *piece),
            low(rows // 2, width),
            low(rows // 2, width),
            low(rows // 2, width),
            low(quarter, width),
            low(quarter, width),
            low(quarter, width),
            low(quarter, width),
            low(quarter, width),
            low(quarter, width),
            full(SEGS, width),
            full(SEGS, width),
            full(SEGS, width),
            full(SEGS, width),
            low(small, fine),
            low(small, fine),
            low(small, fine),
            low(small, fine),
            low(small, fine),
            low(rows, 2 * LANES),
            low(rows, 2 * LANES),
            low(rows, 2 * LANES),
            low(rows, 2 * LANES),
            low(2 * LANES, rows),
            full(rows + 2 * SEGS, WIDE),
            low(rows + 2 * SEGS, WIDE),
            full(rows + 2 * SEGS, WIDE),
            low(rows, WIDE),
            full(4 * SEGS + R + 2 * N, channels),
            full(2 * SEGS, channels),
            full(SEGS, channels),
            full(SEGS, channels),
            dma((18,)),
            dma((3,)),
            dma((2, parts)),
            dma((2, parts)),
            dma((2, parts)),
            dma((2, parts)),
            dma((parts,)),
            dma((2, 4)),
            dma((2, 2)),
            dma((2, 11)),
            dma((2, 4)),
            dma((3,)),
            dma((2, 2)),
            dma((2, 1)),
        ],
        compiler_params=pltpu.CompilerParams(
            collective_id=0, has_side_effects=True, vmem_limit_bytes=63900 << 10
        ),
        cost_estimate=pl.CostEstimate(
            flops=200_000_000_000, bytes_accessed=60_000_000, transcendentals=0
        ),
        name="finish",
    )(
        gated_t, gated, normed_t, d_gate, d_pre, drive, inner, halo, w_inx, w_inz, w_out, x_all, dy_all,
        rms, gain, masks, taps, w_step, w_proj, d_bc, misc, g_step,
    )


def swap_pairs(value, axis, distance):
    count = lax.axis_size(axis)
    return lax.ppermute(value, axis, [(i, i ^ distance) for i in range(count)])


def ordered(mine, other, bit, axis=0):
    return jnp.where(
        bit == 0,
        jnp.concatenate([mine, other], axis=axis),
        jnp.concatenate([other, mine], axis=axis),
    )


def half_of(value, index, axis=0):
    size = value.shape[axis] // 2
    return lax.dynamic_slice_in_dim(value, index * size, size, axis)


def tp_sum(value):
    distance = 1
    while distance < lax.axis_size("tp"):
        value = value + swap_pairs(value, "tp", distance)
        distance *= 2
    return value


def tp_scatter(value):
    index, distance = lax.axis_index("tp"), 1
    while distance < lax.axis_size("tp"):
        mine = (index // distance) % 2
        got = swap_pairs(half_of(value, 1 - mine).astype(BF16), "tp", distance)
        value = half_of(value, mine).astype(F32) + got.astype(F32)
        distance *= 2
    return value


def tp_rows():
    index, distance, at, size = lax.axis_index("tp"), 1, 0, lax.axis_size("tp")
    while distance < lax.axis_size("tp"):
        size //= 2
        at = at + (index // distance) % 2 * size
        distance *= 2
    return at


def per_device(
    hidden_in,
    seq_lengths,
    pack_order,
    norm_gain,
    in_x_weight,
    in_z_weight,
    conv_weight,
    conv_bias,
    x_weight,
    dt_weight,
    dt_bias,
    a_log,
    skip_weight,
    out_weight,
    out_grad,
):
    length, width = hidden_in.shape
    channels = in_x_weight.shape[1]
    tp_count, dp_count, ctx_count = (lax.axis_size(a) for a in ("tp", "dp", "ctx"))
    dp_index, ctx_index, tp_index = (lax.axis_index(a) for a in ("dp", "ctx", "tp"))
    paired = dp_count == 2
    half = width // dp_count
    groups = 2
    fused = paired and ctx_count == 4 and tp_count == 4 and half == channels == length

    def turned(value, axis):
        if not paired:
            return value
        return jnp.concatenate(
            [half_of(value, dp_index, axis), half_of(value, 1 - dp_index, axis)], axis=axis
        )

    def joined(value, axis):
        if not paired:
            return lax.all_gather(value, "dp", axis=axis, tiled=True)
        other = swap_pairs(value, "dp", 1)
        return jnp.where(
            dp_index == 0,
            jnp.concatenate([value, other], axis=axis),
            jnp.concatenate([other, value], axis=axis),
        )

    def weight(own, axis, after):
        if not paired:
            return lax.all_gather(own, "dp", axis=axis, tiled=True), None
        bit = ctx_index % 2
        piece = half_of(own, bit)
        if after is not None:
            piece, _ = lax.optimization_barrier((piece, after))
        near = swap_pairs(piece, "dp", 1)
        far = swap_pairs(near, "ctx", 1)
        return jnp.concatenate([own, ordered(near, far, bit)], axis=axis), near

    small = jnp.concatenate(
        [conv_weight, conv_bias[None], dt_bias[None], skip_weight[None], a_log.T], axis=0
    )
    small = joined(small, 1).astype(F32)
    gain_full = joined(norm_gain, 0).astype(F32)
    w_proj = joined(x_weight, 0)
    w_step = joined(dt_weight, 0)
    w_inx, first = weight(in_x_weight, 0, None)
    w_inz, sent = weight(in_z_weight, 0, first)
    w_out, sent = weight(out_weight, 1, sent)
    gain_full = turned(gain_full, 0)
    taps_full = small[:K]
    conv_shift, step_bias, skip_full = small[K], small[K + 1], small[K + 2]
    decay_rate = -jnp.exp(small[K + 3 :])

    starts = piece_starts(seq_lengths[0], pack_order[0])
    positions = ctx_index * length + jnp.arange(length, dtype=jnp.int32)

    def piece(at):
        return jnp.sum((at[:, None] >= starts[None, :]).astype(jnp.int32), axis=1)

    piece_now = piece(positions)
    masks = [(piece(positions - back) == piece_now).astype(F32) for back in (3, 2, 1)]
    blocked = (1.0 - masks[2]) * FAR

    rows_later = lax.optimization_barrier((hidden_in, first))[0] if paired else hidden_in
    rows_all = turned(rows_later, 1)
    grad_later = lax.optimization_barrier((out_grad, first))[0] if paired else out_grad
    grad_all = turned(grad_later, 1)
    rows_in = rows_all.astype(F32)
    inv_rms = lax.rsqrt(jnp.mean(rows_in * rows_in, axis=1, keepdims=True) + EPSILON)
    normed = (rows_in * inv_rms * gain_full).astype(BF16)
    inner_x = jnp.dot(normed, w_inx, preferred_element_type=F32).astype(BF16)
    halo = shifted(inner_x[length - (K - 1) :], "ctx", 1)
    extended = jnp.concatenate([halo, inner_x], axis=0).astype(F32)
    conv_pre = conv_shift[None, :] + taps_full[K - 1] * extended[K - 1 :]
    for tap in range(K - 1):
        conv_pre = conv_pre + taps_full[tap] * extended[tap : tap + length] * masks[tap][:, None]
    activated = jax.nn.silu(conv_pre).astype(BF16)
    projected = tp_sum(jnp.dot(activated, w_proj, preferred_element_type=F32))
    gate_z = jnp.dot(normed, w_inz, preferred_element_type=F32)
    d_gated = contract_last(grad_all, w_out)

    step_low = projected[:, :R].astype(BF16)
    step_pre = jnp.dot(step_low, w_step, preferred_element_type=F32) + step_bias
    step_size = jax.nn.softplus(step_pre)
    table = jnp.concatenate(
        [
            projected[:, R:],
            blocked[:, None],
            jnp.zeros((length, LANES - 2 * N - 1), F32),
        ],
        axis=1,
    )
    rate2 = decay_rate * LOG2E

    def entering(whole, rate):
        state, back, spent = whole[:N], whole[N : 2 * N], whole[2 * N : 2 * N + 1]
        h_in = jnp.zeros_like(state)
        c_in = jnp.zeros_like(back)
        below = jnp.zeros_like(spent)
        above = jnp.zeros_like(spent)
        distance = 1
        while distance < ctx_count:
            got = swap_pairs(jnp.concatenate([state, back, jnp.broadcast_to(spent, (8,) + spent.shape[1:])], axis=0), "ctx", distance)
            o_state, o_back, o_spent = got[:N], got[N : 2 * N], got[2 * N : 2 * N + 1]
            upper = (ctx_index // distance) % 2 == 1
            h_in = jnp.where(upper, jnp.exp2(rate * below) * o_state + h_in, h_in)
            c_in = jnp.where(upper, c_in, jnp.exp2(rate * above) * o_back + c_in)
            below = jnp.where(upper, below + o_spent, below)
            above = jnp.where(upper, above, above + o_spent)
            mine, other = jnp.exp2(rate * spent), jnp.exp2(rate * o_spent)
            state, back = (
                jnp.where(upper, mine * o_state + state, other * state + o_state),
                jnp.where(upper, o_back + other * back, back + mine * o_back),
            )
            spent = spent + o_spent
            distance *= 2
        return h_in, c_in

    *segs, whole = scan_totals(step_size, activated, d_gated, gate_z, rate2, table, groups)
    gated_t, gated, d_gate, d_pre, d_drive, rates_d, d_bc = scan_grads(
        step_size,
        step_pre,
        activated,
        d_gated,
        gate_z,
        skip_full[None],
        rate2,
        table,
        segs,
        entering(whole, rate2),
        groups,
    )
    rates_d = jnp.sum(rates_d, axis=0)
    g_log, g_skip, g_bias = rates_d[:N] * decay_rate, rates_d[N], rates_d[N + 1]
    g_step = contract_first(step_low, d_pre)

    def input_sum(cotangent):
        value = contract_first(normed, cotangent)
        if paired:
            value = turned(value, 0)
        value = lax.psum_scatter(value.astype(BF16), "dp", scatter_dimension=0, tiled=True)
        return lax.psum(value, "ctx").astype(F32)

    def output_sum(gated):
        value = contract_first(gated, grad_all)
        if paired:
            value = turned(value, 1)
        value = lax.psum_scatter(value.astype(BF16), "dp", scatter_dimension=1, tiled=True)
        return lax.psum(value, "ctx").astype(F32)

    if fused:
        padded = jnp.pad(jnp.stack(masks, axis=1), ((SEGS, SEGS), (0, 1)))
        before = jnp.pad(halo, ((2 * SEGS - (K - 1), 0), (0, 0)))
        taps = jnp.pad(jnp.concatenate([taps_full, conv_shift[None]]), ((0, SEGS - K - 1), (0, 0)))
        misc = jnp.pad(
            jnp.concatenate([g_bias[None], g_skip[None], g_log]), ((0, 3 * SEGS - N - 2), (0, 0))
        )
        s_out, s_z, s_x, small_sum, out_natural, grad_natural = finish(
            gated_t,
            gated,
            normed.T,
            d_gate,
            d_pre,
            d_drive,
            inner_x,
            before,
            w_inx,
            w_inz,
            w_out,
            hidden_in,
            out_grad,
            inv_rms,
            gain_full[None],
            padded,
            taps,
            w_step,
            jnp.pad(w_proj, ((0, 0), (0, 2 * LANES - R - 2 * N))),
            d_bc,
            misc,
            g_step,
        )
        small_sum = small_sum.astype(F32)
        steps_half = g_step.shape[0] // 2
        at = 4 * SEGS + R + 2 * N
        end = at + 2 * steps_half
        return (
            out_natural,
            grad_natural,
            jnp.concatenate(
                [
                    jnp.sum(small_sum[end : end + SEGS], axis=0),
                    jnp.sum(small_sum[end + SEGS :], axis=0),
                ]
            ),
            s_x.astype(F32),
            s_z.astype(F32),
            small_sum[:K],
            small_sum[K],
            small_sum[4 * SEGS : at].T,
            jnp.concatenate(
                [small_sum[at : at + steps_half], small_sum[at + steps_half : end]], axis=1
            ),
            small_sum[SEGS],
            small_sum[SEGS + 2 : SEGS + 2 + N].T,
            small_sum[SEGS + 1],
            s_out.astype(F32),
        )

    branch = jnp.dot(gated, w_out, preferred_element_type=F32)
    d_proj = tp_sum(
        jnp.concatenate([contract_last(d_pre, w_step), d_bc[:, : 2 * N]], axis=1)
    ).astype(BF16)

    quarter = length // tp_count
    own_row = tp_rows() * quarter
    own_in = lax.dynamic_slice_in_dim(rows_all, own_row, quarter, 0).astype(F32)
    own_grad = lax.dynamic_slice_in_dim(grad_all, own_row, quarter, 0).astype(F32)
    own_rms = lax.rsqrt(jnp.mean(own_in * own_in, axis=1, keepdims=True) + EPSILON)
    own_hat = own_in * own_rms

    def whole_rows(value):
        distance = tp_count // 2
        while distance >= 1:
            value = ordered(value, swap_pairs(value, "tp", distance), (tp_index // distance) % 2)
            distance //= 2
        if not paired:
            return value
        return ordered(value[:, :half], value[:, half:], dp_index, axis=1)

    out_natural = whole_rows((own_in + tp_scatter(branch)).astype(BF16))

    g_proj = contract_first(d_proj, activated)
    d_total = d_drive + contract_last(d_proj, w_proj)
    conv_sig = jax.nn.sigmoid(conv_pre)
    d_conv = d_total * conv_sig * (1.0 + conv_pre * (1.0 - conv_sig))
    g_shift = jnp.sum(d_conv, axis=0)
    g_taps = jnp.stack(
        [
            jnp.sum(d_conv * masks[tap][:, None] * extended[tap : tap + length], axis=0)
            for tap in range(K - 1)
        ]
        + [jnp.sum(d_conv * extended[K - 1 :], axis=0)],
        axis=0,
    )
    d_extended = jnp.pad(d_conv * taps_full[K - 1], ((K - 1, 0), (0, 0)))
    for tap in range(K - 1):
        d_extended = d_extended + jnp.pad(
            d_conv * masks[tap][:, None] * taps_full[tap], ((tap, K - 1 - tap), (0, 0))
        )
    returned = shifted(d_extended[: K - 1], "ctx", -1)
    d_inner = (
        d_extended[K - 1 :] + jnp.pad(returned, ((length - (K - 1), 0), (0, 0)))
    ).astype(BF16)
    packed = jnp.concatenate(
        [g_taps, g_shift[None], g_bias[None], g_skip[None], g_log, g_proj], axis=0
    )
    g_inx, g_inz, g_out = input_sum(d_inner), input_sum(d_gate), output_sum(gated)
    d_normed = tp_scatter(contract_last(d_inner, w_inx) + contract_last(d_gate, w_inz))
    g_gain = jnp.sum(d_normed * own_hat, axis=0)
    d_hat = d_normed * gain_full
    d_rows = own_grad + own_rms * (
        d_hat - own_hat * jnp.mean(d_hat * own_hat, axis=1, keepdims=True)
    )
    grad_natural = whole_rows(d_rows.astype(BF16))
    g_gain = turned(lax.psum(g_gain, ("ctx", "tp")), 0)
    g_gain = lax.psum_scatter(g_gain, "dp", scatter_dimension=0, tiled=True)
    packed = lax.psum(lax.psum_scatter(packed, "dp", scatter_dimension=1, tiled=True), "ctx")
    g_step = lax.psum(lax.psum_scatter(g_step, "dp", scatter_dimension=0, tiled=True), "ctx")
    return (
        out_natural,
        grad_natural,
        g_gain,
        g_inx,
        g_inz,
        packed[:K],
        packed[K],
        packed[K + 3 + N :].T,
        g_step,
        packed[K + 1],
        packed[K + 3 : K + 3 + N].T,
        packed[K + 2],
        g_out,
    )


def solution(mesh):
    in_specs = (
        P(("dp", "ctx"), None),
        P("dp", None),
        P("dp", None),
        P("dp"),
        P("dp", "tp"),
        P("dp", "tp"),
        P(None, ("tp", "dp")),
        P(("tp", "dp")),
        P(("tp", "dp"), None),
        P("dp", "tp"),
        P(("tp", "dp")),
        P(("tp", "dp"), None),
        P(("tp", "dp")),
        P("tp", "dp"),
        P(("dp", "ctx"), None),
    )
    out_specs = (
        P(("dp", "ctx"), None),
        P(("dp", "ctx"), None),
        P("dp"),
        P("dp", "tp"),
        P("dp", "tp"),
        P(None, ("tp", "dp")),
        P(("tp", "dp")),
        P(("tp", "dp"), None),
        P("dp", "tp"),
        P(("tp", "dp")),
        P(("tp", "dp"), None),
        P(("tp", "dp")),
        P("tp", "dp"),
    )
    return jax.shard_map(
        per_device, mesh=mesh, in_specs=in_specs, out_specs=out_specs, check_vma=False
    )
```
